32 devices in a mesh: role: 2 (over y), gx: 4 (over z), gy: 4 (over x, core).
Axes of the slice: x: 2, y: 2, z: 4, core: 2. Of those that a mesh axis runs over, the one named last changes fastest.
Arguments:
- design: float32 [64, 128, 256], P(('gx', 'gy'), None, 'role'), may hold values from 0 to 1
- force: float32 [3, 32, 64, 256], P(None, 'gx', 'gy', 'role'), may hold values from -6 to 6
- clamped_dof_mask: int32 [3, 32, 64, 256], P(None, 'gx', 'gy', 'role'), may hold values 0 or 1
- stiffness: float32 [81, 81], replicated, may hold values from -1 to 70, as said below
Outputs:
- sensitivity: float32 [64, 128, 256], P(('gx', 'gy'), None, 'role')
- displacement: float32 [3, 32, 64, 256], P(None, 'gx', 'gy', 'role')
The draws below stay inside these ranges and needn't reach their ends.
Inputs may be any that keep to these rules, and one draw needn't show every extreme that they name: `stiffness`: symmetric, and each diagonal entry exceeds the sum of the magnitudes of the other entries of its row.
All inputs are finite; a program needn't handle non-finite values. No bound on the sum of `clamped_dof_mask` on one device may be relied on, other than what follows from the above.
Results may differ from the reference program's by a relative error of at most 0.00013.
Values sent between devices are 32-bit elements; how exact they have to be, the bound alone decides.
No kernel may reach another device: no remote copies, remote signals or barrier semaphores. Data moves between devices by JAX's collectives and lax.ppermute only.
A program may use at most 64 MiB of HBM per device.

```python
import jax
import jax.numpy as jnp
from jax import lax

ITERS = 3
RADIUS = 2
ELEMENTS_X = 16
ELEMENTS_Y = 32
ELEMENTS_Z = 128
FX = 64
FY = 128
FZ = 256


def draw_stiffness(key, part):
    first_key, second_key = jax.random.split(jax.random.fold_in(key, 11))
    raw = jnp.clip(jax.random.normal(first_key, (81, 81), jnp.float32), -4.0, 4.0) / 9.0
    identity = jnp.eye(81, dtype=jnp.float32)
    symmetric = (raw + raw.T) * 0.7071
    offdiag = symmetric * (1.0 - identity)
    diagonal = 1.25 * jnp.sum(jnp.abs(offdiag), axis=1) + jax.random.uniform(second_key, (81,), jnp.float32, 0.5, 2.0)
    return offdiag + diagonal[:, None] * identity


def plant(values, key, smallest, high):
    longest = values.shape.index(max(values.shape))
    spots = []
    for shift in (0, 1):
        where = [jax.random.randint(jax.random.fold_in(key, axis), (), 0, length) for axis, length in enumerate(values.shape)]
        where[longest] = (where[longest] + shift) % values.shape[longest]
        spots.append(tuple(where))
    return values.at[spots[0]].set(smallest).at[spots[1]].set(high)


def level_of(key, shape, cuts, least, top_value):
    def one(dim, shards_of):
        heights = jax.random.uniform(jax.random.fold_in(jax.random.fold_in(key, 6), dim), (shards_of,), jnp.float32, least / len(cuts), top_value / len(cuts))
        return jnp.repeat(jnp.exp(heights), shape[dim] // shards_of).reshape((-1,) + (1,) * (len(shape) - dim - 1))

    loudness = one(*cuts[0])
    for cut in cuts[1:]:
        loudness = loudness * one(*cut)
    return loudness


def normal_values(own_key, shape, scale, bound, cuts=(), kind=jnp.bfloat16):
    drawn = jax.random.normal(own_key, shape, jnp.float32) * scale
    if len(cuts) > 0:
        drawn = level_of(own_key, shape, cuts, -0.22, 0.18) * drawn
    return jnp.clip(drawn, min=-bound, max=bound).astype(kind)


def setup_inputs(seed: int = 0) -> dict:
    arg_keys = jax.random.split(jax.random.key(seed), 5)
    design = jnp.clip(1.0 * jax.random.uniform(arg_keys[0], (FX, FY, FZ), jnp.float32) ** level_of(arg_keys[0], (FX, FY, FZ), ((0, 16), (2, 2)), -0.2, 0.2), 0.0, 1.0)
    force = normal_values(arg_keys[1], (3, 2 * ELEMENTS_X, 2 * ELEMENTS_Y, 2 * ELEMENTS_Z), 1.0, 6.0, ((1, 4), (2, 4), (3, 2)), jnp.float32)
    clamped_dof_mask = plant((jax.random.randint(arg_keys[2], (3, 2 * ELEMENTS_X, 2 * ELEMENTS_Y, 2 * ELEMENTS_Z), 0, 8) < 1).astype(jnp.int32), jax.random.fold_in(arg_keys[2], 1), 0, 1)
    stiffness = draw_stiffness(jax.random.fold_in(arg_keys[4], 71), 0)
    return {"design": design, "force": force, "clamped_dof_mask": clamped_dof_mask, "stiffness": stiffness}


sharpness = 4.0
threshold = 0.5
floor_stiff = 0.001


def hat_list():
    return [float(RADIUS + 1 - abs(shift_idx - RADIUS)) for shift_idx in range(2 * RADIUS + 1)]


def smooth_axis(padded, axis_num, length):
    result = None
    for offset_idx, weight in enumerate(hat_list()):
        portion = weight * lax.slice_in_dim(padded, offset_idx, offset_idx + length, axis=axis_num)
        result = portion if result is None else result + portion
    return result


def axis_count(start, length, extent):
    places = start + jnp.arange(length, dtype=jnp.int32)
    counted = jnp.zeros((length,), jnp.float32)
    for offset_idx, weight in enumerate(hat_list()):
        target = places + (offset_idx - RADIUS)
        inside = jnp.logical_and(target >= 0, target < extent)
        counted = counted + weight * inside.astype(jnp.float32)
    return counted


def smooth_all(field):
    extent_x, extent_y, extent_z = field.shape
    padded = jnp.pad(field, RADIUS)
    return smooth_axis(smooth_axis(smooth_axis(padded, 2, extent_z), 1, extent_y), 0, extent_x)


def heaviside_projection(values):
    scaled = jnp.tanh(sharpness * threshold) + jnp.tanh(sharpness * (1.0 - threshold))
    return (jnp.tanh(sharpness * threshold) + jnp.tanh(sharpness * (values - threshold))) / scaled


def slope(values):
    scaled = jnp.tanh(sharpness * threshold) + jnp.tanh(sharpness * (1.0 - threshold))
    bent = jnp.tanh(sharpness * (values - threshold))
    return sharpness * (1.0 - bent * bent) / scaled


def element_mean(fine):
    count_x = fine.shape[0] // 4
    count_y = fine.shape[1] // 4
    count_z = fine.shape[2] // 2
    return fine.reshape(count_x, 4, count_y, 4, count_z, 2).mean(axis=(1, 3, 5))


def spread(elements):
    count_x, count_y, count_z = elements.shape
    widened = jnp.broadcast_to(elements[:, None, :, None, :, None], (count_x, 4, count_y, 4, count_z, 2))
    return widened.reshape(4 * count_x, 4 * count_y, 2 * count_z)


def split_axis(values, axis_num):
    half_len = (values.shape[axis_num] - 1) // 2
    pieces = [lax.slice_in_dim(values, corner, corner + 2 * half_len - 1, stride=2, axis=axis_num) for corner in range(3)]
    return jnp.stack(pieces, axis=0)


def split_nodes(values):
    stacked = split_axis(values, 1)
    stacked = split_axis(stacked, 3)
    stacked = split_axis(stacked, 5)
    return stacked.reshape(81, -1)


def merge_axis(parts, axis_num):
    opening = parts[0]
    middle = parts[1]
    closing = parts[2]
    length = opening.shape[axis_num]
    before = [(0, 0)] * opening.ndim
    before[axis_num] = (0, 1)
    behind = [(0, 0)] * opening.ndim
    behind[axis_num] = (1, 0)
    evens = jnp.pad(opening, before) + jnp.pad(closing, behind)
    leading = lax.slice_in_dim(evens, 0, length, axis=axis_num)
    ending = lax.slice_in_dim(evens, length, length + 1, axis=axis_num)
    braided = jnp.stack([leading, middle], axis=axis_num + 1)
    new_shape = list(leading.shape)
    new_shape[axis_num] = 2 * length
    return jnp.concatenate([braided.reshape(new_shape), ending], axis=axis_num)


def merge_nodes(stiffness_product, element_shape):
    reshaped = stiffness_product.reshape((3, 3, 3, 3) + tuple(element_shape))
    merged = merge_axis(reshaped, 5)
    merged = merge_axis(merged, 3)
    return merge_axis(merged, 1)


def conjugate_gradient_solve(operate, inner_sum, rhs):
    solution = jnp.zeros_like(rhs)
    residual = rhs
    direction = rhs
    current = inner_sum(residual, residual)
    for sweep in range(ITERS):
        applied = operate(direction)
        step_len = current / inner_sum(direction, applied)
        solution = solution + step_len * direction
        residual = residual - step_len * applied
        updated = inner_sum(residual, residual)
        direction = residual + (updated / current) * direction
        current = updated
    return solution


def reference(design, force, clamped_dof_mask, stiffness):
    extent_x, extent_y, extent_z = design.shape
    filter_weight_grid = (axis_count(0, extent_x, extent_x)[:, None, None]
                   * axis_count(0, extent_y, extent_y)[None, :, None]
                   * axis_count(0, extent_z, extent_z)[None, None, :])
    filtered = smooth_all(design) / filter_weight_grid
    density = element_mean(heaviside_projection(filtered))
    factor = floor_stiff + (1.0 - floor_stiff) * density ** 3
    behind = ((0, 0), (0, 1), (0, 1), (0, 1))
    free = jnp.pad((1 - clamped_dof_mask).astype(jnp.float32), behind)
    rhs = free * jnp.pad(force, behind)
    scales = factor.reshape(-1)

    def operate(values):
        columns = split_nodes(free * values)
        stiffness_product = jnp.dot(stiffness, columns, precision=lax.Precision.HIGHEST,
                          preferred_element_type=jnp.float32) * scales[None, :]
        return free * merge_nodes(stiffness_product, factor.shape)

    def inner_sum(left, right):
        return jnp.sum(left * right)

    solution = conjugate_gradient_solve(operate, inner_sum, rhs)
    columns = split_nodes(solution)
    energy = jnp.sum(columns * jnp.dot(stiffness, columns, precision=lax.Precision.HIGHEST,
                                       preferred_element_type=jnp.float32), axis=0).reshape(factor.shape)
    element_grad = -3.0 * density ** 2 * (1.0 - floor_stiff) * energy / 32.0
    voxel_grad = spread(element_grad) * slope(filtered)
    sensitivity = smooth_all(voxel_grad / filter_weight_grid)
    return sensitivity, solution[:, :-1, :-1, :-1]
```

```python
import jax
import jax.numpy as jnp
import numpy as np
from jax import lax
from jax.experimental import pallas as pl
from jax.experimental.pallas import tpu as pltpu
from jax.sharding import PartitionSpec as P

SHARPNESS = 4.0
THRESHOLD = 0.5
FLOOR_STIFF = 0.001
TANH2 = float(np.tanh(2.0))
LANES = 128
HALO = 3
STRIP = 8
ROWS = 120
LINE = ("gx", "gy")
F32 = jnp.float32
BF16 = jnp.bfloat16


def iota(shape, dim):
    return lax.broadcasted_iota(jnp.int32, shape, dim)


def place_table():
    table = np.zeros((ROWS, 81), np.float32)
    for c in range(3):
        for b in range(3):
            for a in range(3):
                for q in range(3):
                    dof = ((c * 3 + b) * 3 + a) * 3 + q
                    if c < 2:
                        row = 8 * (3 * a + b) + 4 * c + q
                    else:
                        row = 72 + 8 * (2 * b + (a == 2)) + 4 * (a == 1) + q
                    table[row, dof] = 1.0
    return table


def split2(x):
    hi = x.astype(BF16)
    return hi, (x - hi.astype(F32)).astype(BF16)


def split3(x):
    hi = x.astype(BF16)
    rest = x - hi.astype(F32)
    mid = rest.astype(BF16)
    return hi, mid, (rest - mid.astype(F32)).astype(BF16)


def dot(a, b):
    return jnp.dot(a, b, preferred_element_type=F32)


def pick_right(x, table):
    hi, mid, lo = split3(x)
    return (dot(hi, table) + dot(mid, table)) + dot(lo, table)


def pick_left(table, x):
    hi, mid, lo = split3(x)
    return (dot(table, hi) + dot(table, mid)) + dot(table, lo)


def where_am_i():
    role = lax.axis_index("role")
    slab = lax.axis_index("gx") * lax.axis_size("gy") + lax.axis_index("gy")
    return role, slab


def element_lanes(shape, role, half):
    lane = iota(shape, len(shape) - 1)
    above = jnp.logical_and(lane >= half, lane < half + HALO)
    below = lane >= LANES - HALO
    roles = lax.axis_size("role")
    return (lane < half) | (above & (role < roles - 1)) | (below & (role > 0))


def hat_count(place, extent):
    low = jnp.where(place == 0, 3.0, jnp.where(place == 1, 1.0, 0.0))
    high = jnp.where(place == extent - 1, 3.0, jnp.where(place == extent - 2, 1.0, 0.0))
    return 9.0 - low - high


def smooth_z(x):
    width = x.shape[1]
    for _ in range(2):
        x = x + pltpu.roll(x, 1, 1) + pltpu.roll(x, width - 1, 1)
    return x


def smooth_y(x):
    rows = x.shape[0]
    x = jnp.concatenate([x, jnp.zeros((8, x.shape[1]), F32)], axis=0)
    for _ in range(2):
        x = x + pltpu.roll(x, 1, 0) + pltpu.roll(x, rows + 7, 0)
    return x[:rows]


def prep_kernel(force_ref, mask_ref, next_ref, stiff_ref, place_ref, pack_ref, table_ref):
    parts = pack_ref.shape[0]
    for q in range(3):
        free = 1.0 - mask_ref[q].astype(F32)
        rhs = free * force_ref[q]
        for row, val in ((q, rhs), (q + 3, free)):
            for j in range(parts):
                for a in range(3):
                    x = 2 * j + a
                    pack_ref[j, row, a] = val[x] if x < 2 * parts else next_ref[row]
    place = place_ref[...]
    half_way = jnp.dot(place, stiff_ref[...], precision=lax.Precision.HIGHEST, preferred_element_type=F32)
    spread = lax.dot_general(
        half_way, place, (((1,), (1,)), ((), ())), precision=lax.Precision.HIGHEST, preferred_element_type=F32
    )
    hi, lo = split2(spread)
    row = iota((ROWS, 2 * ROWS), 0)
    col = iota((ROWS, 2 * ROWS), 1)
    twice = jnp.where(row == 8 * (col // 16) + col % 8, 1.0, 0.0).astype(BF16)
    table_ref[:ROWS] = dot(hi, twice).astype(BF16)
    table_ref[ROWS:] = dot(lo, twice).astype(BF16)


def plane_rows(tiles):
    return tiles * 8


def shifted_tiles(nodes_ref, tiles, s):
    count = plane_rows(tiles)
    upper = (iota((count, LANES), 0) & 4) == 0
    if s == 0:
        first = nodes_ref[0:count]
        second = nodes_ref[count : 2 * count]
        x = jnp.where(upper, first, pltpu.roll(second, 4, 0))
    else:
        x = jnp.where(upper, nodes_ref[2 * count : 3 * count], 0.0)
    return pltpu.roll(x, LANES - 1, 1)


def pair_tiles(x):
    tiles = x.shape[0] // 8
    hi = x.astype(BF16).astype(F32)
    lo = x - hi
    both = jnp.concatenate([hi.reshape(tiles, 8, LANES), lo.reshape(tiles, 8, LANES)], axis=1)
    return both.astype(BF16)


def make_tiles(nodes_ref, main_ref, shift_ref, shift32_ref):
    tiles = main_ref.shape[1]
    count = plane_rows(tiles)
    for a in range(3):
        main_ref[a] = pair_tiles(nodes_ref[a * count : (a + 1) * count])
    for s in range(2):
        x = shifted_tiles(nodes_ref, tiles, s)
        if shift32_ref is not None:
            shift32_ref[s] = x
        shift_ref[s] = pair_tiles(x)


def sweep(table_ref, main_ref, shift_ref, factor_ref, out_ref, energies):
    tiles = main_ref.shape[1]
    columns = factor_ref.shape[0]
    upper = iota((8, LANES), 0) < 4

    def finish(node, parts):
        t0, t1, t2, s0, s1 = parts
        r0 = pltpu.roll(s0, 1, 1)
        r1 = pltpu.roll(s1, 1, 1)
        done = (
            t0 + jnp.where(upper, r0, 0.0),
            t1 + jnp.where(upper, pltpu.roll(r0, 4, 0), 0.0),
            t2 + jnp.where(upper, r1, 0.0),
        )
        for a in range(3):
            out_ref[pl.ds(pl.multiple_of((a * tiles + node) * 8, 8), 8), :] = done[a]

    def body(i, carry):
        cols = []
        for k in range(2):
            base = 4 * i + 2 * k
            pieces = [main_ref[a, base + b] for a in range(3) for b in range(3)]
            pieces += [shift_ref[s, base + b] for b in range(3) for s in range(2)]
            cols.append(jnp.concatenate(pieces, axis=0))
        product = dot(table_ref[...], jnp.concatenate(cols, axis=1))
        product = product[:ROWS] + product[ROWS:]
        parts = []
        for k in range(2):
            y = product[:, k * LANES : (k + 1) * LANES]
            base = 4 * i + 2 * k
            for nodes_ref, shift32_ref, e_ref in energies:
                total = None
                for a in range(3):
                    for b in range(3):
                        at = pl.multiple_of((a * tiles + base + b) * 8, 8)
                        term = nodes_ref[pl.ds(at, 8), :] * y[8 * (3 * a + b) : 8 * (3 * a + b) + 8]
                        total = term if total is None else total + term
                for b in range(3):
                    for s in range(2):
                        at = pl.multiple_of((base + b) * 8, 8)
                        lo = 72 + 8 * (2 * b + s)
                        total = total + shift32_ref[s, pl.ds(at, 8), :] * y[lo : lo + 8]
                e_ref[pl.ds(2 * i + k, 1), :] = jnp.sum(total, axis=0, keepdims=True)
            if out_ref is not None:
                z = y * factor_ref[pl.ds(2 * i + k, 1), :]
                parts.append(
                    [
                        [z[8 * (3 * a + b) : 8 * (3 * a + b) + 8] for a in range(3)]
                        + [z[72 + 8 * (2 * b + s) : 80 + 8 * (2 * b + s)] for s in range(2)]
                        for b in range(3)
                    ]
                )
        if out_ref is None:
            return carry
        left, right = parts
        finish(4 * i, [c + v for c, v in zip(carry, left[0])])
        finish(4 * i + 1, left[1])
        finish(4 * i + 2, [c + v for c, v in zip(left[2], right[0])])
        finish(4 * i + 3, right[1])
        return tuple(right[2])

    if out_ref is None:
        lax.fori_loop(0, columns // 2, lambda i, c: body(i, c), 0)
    else:
        zero = jnp.zeros((8, LANES), F32)
        lax.fori_loop(0, columns // 2, body, (zero,) * 5)
        for a in range(3):
            for node in range(2 * columns, tiles):
                at = (a * tiles + node) * 8
                out_ref[at : at + 8, :] = zero


def send_planes(local_ref, tiles, slab, to_a, to_b):
    count = plane_rows(tiles)
    low = local_ref[0:count]
    high = local_ref[2 * count : 3 * count]
    even = slab % 2 == 0
    to_a[...] = jnp.where(even, high, low)
    to_b[...] = jnp.where(even, low, high)


def gather_nodes(local_ref, from_a, from_b, free_ref, tiles, slab, nodes_ref):
    count = plane_rows(tiles)
    even = slab % 2 == 0
    a = from_a[...]
    b = from_b[...]
    nodes_ref[0:count] = free_ref[0:count] * (local_ref[0:count] + jnp.where(even, b, a))
    nodes_ref[count : 2 * count] = free_ref[count : 2 * count] * local_ref[count : 2 * count]
    nodes_ref[2 * count :] = free_ref[2 * count :] * (local_ref[2 * count :] + jnp.where(even, a, b))


def first_kernel(
    design_ref, da_ref, db_ref, strip_ref, rf_ref, table_ref,
    sw_ref, factor_ref, density_ref, nodes_ref, free_ref, local_ref, to_a, to_b, e00_ref,
    fine_ref, sum_ref, main_ref, shift_ref, shift32_ref,
):
    planes, fy, fz = design_ref.shape
    tiles = main_ref.shape[1]
    count = plane_rows(tiles)
    role, slab = where_am_i()
    slabs = lax.axis_size("gx") * lax.axis_size("gy")
    roles = lax.axis_size("role")
    half = fz // 2
    even = slab % 2 == 0

    at_lane = jnp.where(role == 0, 0, LANES - STRIP)
    put = jnp.where(iota((STRIP, LANES), 1) == iota((STRIP, LANES), 0) + at_lane, 1.0, 0.0).astype(BF16)
    for p in range(planes):
        a = da_ref[p]
        b = db_ref[p]
        fine_ref[p, :, :fz] = jnp.where(even, b, a)
        fine_ref[planes + p, :, :fz] = design_ref[p]
        fine_ref[2 * planes + p, :, :fz] = jnp.where(even, a, b)
    for p in range(planes):
        own = pick_right(strip_ref[p * fy : (p + 1) * fy], put)
        a = pick_right(strip_ref[(planes + p) * fy : (planes + p + 1) * fy], put)
        b = pick_right(strip_ref[(2 * planes + p) * fy : (2 * planes + p + 1) * fy], put)
        fine_ref[p, :, fz:] = jnp.where(even, b, a)
        fine_ref[planes + p, :, fz:] = own
        fine_ref[2 * planes + p, :, fz:] = jnp.where(even, a, b)

    width = 2 * fz
    lane = iota((1, width), 1)
    z_place = role * fz + jnp.where(lane < fz + fz // 2, lane, lane - width)
    inv_z = 1.0 / hat_count(z_place, roles * fz)
    inv_y = 1.0 / hat_count(iota((fy, 1), 0), fy)
    inv_yz = inv_y * inv_z
    sum_ref[...] = jnp.zeros((fy, width), F32)

    def filter_plane(p, _):
        x = fine_ref[p] + fine_ref[p + 4] + 2.0 * (fine_ref[p + 1] + fine_ref[p + 3]) + 3.0 * fine_ref[p + 2]
        x = smooth_y(smooth_z(x))
        place = jnp.full((1, 1), slab * planes + p - 2, jnp.int32)
        inv = inv_yz * (1.0 / hat_count(place, slabs * planes))
        bent = jnp.tanh(SHARPNESS * (x * inv - THRESHOLD))
        sw_ref[p] = (SHARPNESS / (2.0 * TANH2)) * (1.0 - bent * bent) * inv
        mine = jnp.logical_and(p >= 2, p < 2 + planes)
        sum_ref[...] += jnp.where(mine, (TANH2 + bent) * (1.0 / (2.0 * TANH2)), 0.0)
        return 0

    lax.fori_loop(0, planes + 4, filter_plane, 0)

    rows = factor_ref.shape[0]
    pool_y = jnp.where(iota((rows, fy), 1) // 4 == iota((rows, fy), 0), 1.0, 0.0).astype(BF16)
    pool_z = jnp.where(iota((width, LANES), 0) // 2 == iota((width, LANES), 1), 1.0, 0.0).astype(BF16)
    density = pick_right(pick_left(pool_y, sum_ref[...]), pool_z) * (1.0 / 32.0)
    inside = element_lanes((rows, LANES), role, half)
    density = jnp.where(inside, density, 0.0)
    density_ref[...] = density
    factor_ref[...] = jnp.where(inside, FLOOR_STIFF + (1.0 - FLOOR_STIFF) * density * density * density, 0.0)

    nodes_ref[...] = jnp.zeros(nodes_ref.shape, F32)
    free_ref[...] = jnp.zeros(free_ref.shape, F32)
    zi = iota((LANES, width), 0)
    ci = iota((LANES, width), 1)
    lane_of = ci & (LANES - 1)
    odd = ci // LANES
    own_table = jnp.where(zi == 2 * lane_of + odd, 1.0, 0.0).astype(BF16)
    si = iota((STRIP, width), 0)
    ci = iota((STRIP, width), 1)
    lane_of = ci & (LANES - 1)
    odd = ci // LANES
    first_lane = jnp.where(role == 0, half, LANES - STRIP // 2)
    strip_table = jnp.where(si == 2 * (lane_of - first_lane) + odd, 1.0, 0.0).astype(BF16)
    parts = rf_ref.shape[0]
    deep = rf_ref.shape[3]
    base = 3 * planes * fy
    for row in range(6):
        for a in range(3):
            x = jnp.concatenate([rf_ref[j, row, a] for j in range(parts)], axis=0)
            st = jnp.concatenate(
                [
                    strip_ref[base + ((j * 6 + row) * 3 + a) * deep : base + ((j * 6 + row) * 3 + a + 1) * deep]
                    for j in range(parts)
                ],
                axis=0,
            )
            if row < 3:
                y = pick_right(x, own_table) + pick_right(st, strip_table)
                dest = nodes_ref
            else:
                y = dot(x.astype(BF16), own_table) + dot(st.astype(BF16), strip_table)
                dest = free_ref
            q = row % 3
            dest[pl.ds(a * count + q, parts * deep, stride=8), :] = y[:, :LANES]
            dest[pl.ds(a * count + 4 + q, parts * deep, stride=8), :] = y[:, LANES:]

    make_tiles(nodes_ref, main_ref, shift_ref, shift32_ref)
    sweep(table_ref, main_ref, shift_ref, factor_ref, local_ref, [(nodes_ref, shift32_ref, e00_ref)])
    send_planes(local_ref, tiles, slab, to_a, to_b)


def second_kernel(
    prev_ref, free_ref, last_ref, from_a, from_b, factor_ref, table_ref,
    nodes_ref, local_ref, to_a, to_b, e01_ref, e11_ref,
    main_ref, shift_ref, shift32_ref, prev32_ref,
):
    tiles = main_ref.shape[1]
    role, slab = where_am_i()
    gather_nodes(last_ref, from_a, from_b, free_ref, tiles, slab, nodes_ref)
    for s in range(2):
        prev32_ref[s] = shifted_tiles(prev_ref, tiles, s)
    make_tiles(nodes_ref, main_ref, shift_ref, shift32_ref)
    sweep(
        table_ref, main_ref, shift_ref, factor_ref, local_ref,
        [(prev_ref, prev32_ref, e01_ref), (nodes_ref, shift32_ref, e11_ref)],
    )
    send_planes(local_ref, tiles, slab, to_a, to_b)


def third_kernel(
    v0_ref, v1_ref, free_ref, last_ref, from_a, from_b, factor_ref, table_ref, e00_ref, e01_ref, e11_ref,
    nodes_ref, e02_ref, e12_ref, e22_ref, moment_ref,
    main_ref, shift_ref, shift32_ref, s0_ref, s1_ref,
):
    tiles = main_ref.shape[1]
    count = plane_rows(tiles)
    role, slab = where_am_i()
    gather_nodes(last_ref, from_a, from_b, free_ref, tiles, slab, nodes_ref)
    for s in range(2):
        s0_ref[s] = shifted_tiles(v0_ref, tiles, s)
        s1_ref[s] = shifted_tiles(v1_ref, tiles, s)
    make_tiles(nodes_ref, main_ref, shift_ref, shift32_ref)
    sweep(
        table_ref, main_ref, shift_ref, factor_ref, None,
        [(v0_ref, s0_ref, e02_ref), (v1_ref, s1_ref, e12_ref), (nodes_ref, shift32_ref, e22_ref)],
    )
    half = LANES // 2
    own = iota((1, LANES), 1) < half
    v0 = v0_ref[0 : 2 * count]
    sums = [jnp.sum(v0 * v0, axis=0, keepdims=True)]
    for e_ref in (e00_ref, e01_ref, e11_ref, e12_ref, e22_ref):
        sums.append(jnp.sum(factor_ref[...] * e_ref[...], axis=0, keepdims=True))
    lane = iota((1, LANES), 1)
    out = jnp.zeros((1, LANES), F32)
    for k, s in enumerate(sums):
        total = jnp.sum(jnp.where(own, s, 0.0), axis=1, keepdims=True)
        out = jnp.where(lane == k, total, out)
    moment_ref[...] = jnp.broadcast_to(out, moment_ref.shape)


def combine_kernel(
    moment_ref, v0_ref, v1_ref, v2_ref, e00_ref, e01_ref, e11_ref, e02_ref, e12_ref, e22_ref, density_ref,
    grad_ref, u_ref, nodes_ref,
):
    role, slab = where_am_i()
    parts, _, _, deep, fz = u_ref.shape
    half = fz // 2
    count = v0_ref.shape[0] // 3
    total = jnp.sum(moment_ref[...], axis=0, keepdims=True)
    lane = iota((1, LANES), 1)
    m = [jnp.sum(jnp.where(lane == k, total, 0.0), axis=1, keepdims=True) for k in range(6)]
    s = m[1] / m[0]
    inv = 1.0 / s
    mu = [jnp.ones_like(s)]
    power = 1.0 / m[0]
    for k in range(1, 6):
        power = power * inv
        mu.append(m[k] * power)
    nu = list(mu)
    for depth in range(1, 6):
        for k in range(5, depth - 1, -1):
            nu[k] = nu[k] - nu[k - 1]
    g = [nu[k] + nu[k + 1] for k in range(5)]
    l10 = g[1] / g[0]
    l20 = g[2] / g[0]
    d1 = g[2] - l10 * g[1]
    x12 = g[3] - l10 * g[2]
    r1 = nu[1] - l10 * nu[0]
    r2 = nu[2] - l20 * nu[0]
    l21 = x12 / d1
    d2 = (g[4] - l20 * g[2]) - l21 * x12
    c2 = (r2 - l21 * r1) / d2
    c1 = (r1 - x12 * c2) / d1
    c0 = (nu[0] - g[1] * c1 - g[2] * c2) / g[0]
    w0 = (c0 - c1 + c2) * inv
    w1 = (c1 - 2.0 * c2) * inv * inv
    w2 = c2 * inv * inv * inv
    energy = (
        w0 * (w0 * e00_ref[...] + 2.0 * (w1 * e01_ref[...] + w2 * e02_ref[...]))
        + w1 * (w1 * e11_ref[...] + 2.0 * w2 * e12_ref[...])
        + w2 * w2 * e22_ref[...]
    )
    density = density_ref[...]
    grad = (-3.0 * (1.0 - FLOOR_STIFF) / 32.0) * density * density * energy
    grad_ref[...] = jnp.where(element_lanes(grad.shape, role, half), grad, 0.0)
    nodes_ref[...] = w0 * v0_ref[0 : 2 * count] + w1 * v1_ref[0 : 2 * count] + w2 * v2_ref[0 : 2 * count]
    gi = iota((LANES, fz), 0)
    zi = iota((LANES, fz), 1)
    even_table = jnp.where(zi == 2 * gi, 1.0, 0.0).astype(BF16)
    odd_table = jnp.where(zi == 2 * gi + 1, 1.0, 0.0).astype(BF16)
    for a in range(2):
        for q in range(3):
            even = nodes_ref[pl.ds(a * count + q, parts * deep, stride=8), :]
            odd = nodes_ref[pl.ds(a * count + 4 + q, parts * deep, stride=8), :]
            x = pick_right(even, even_table) + pick_right(odd, odd_table)
            for j in range(parts):
                u_ref[j, q, a] = x[j * deep : (j + 1) * deep]


def last_kernel(grad_ref, ga_ref, gb_ref, sw_ref, out_ref, work_ref):
    planes, fy, fz = out_ref.shape
    width = 2 * fz
    role, slab = where_am_i()
    even = slab % 2 == 0
    rows = grad_ref.shape[0]
    pool_y = jnp.where(iota((fy, rows), 0) // 4 == iota((fy, rows), 1), 1.0, 0.0).astype(BF16)
    pool_z = jnp.where(iota((LANES, width), 1) // 2 == iota((LANES, width), 0), 1.0, 0.0).astype(BF16)
    a = ga_ref[...]
    b = gb_ref[...]
    low = jnp.where(even, b, a)
    high = jnp.where(even, a, b)
    for grad, first, last in ((low, 0, 2), (grad_ref[...], 2, 2 + planes), (high, 2 + planes, 4 + planes)):
        wide = pick_right(pick_left(pool_y, grad), pool_z)
        for p in range(first, last):
            work_ref[p] = wide * sw_ref[p]

    def body(p, _):
        x = work_ref[p] + work_ref[p + 4] + 2.0 * (work_ref[p + 1] + work_ref[p + 3]) + 3.0 * work_ref[p + 2]
        out_ref[p] = smooth_y(smooth_z(x))[:, :fz]
        return 0

    lax.fori_loop(0, planes, body, 0)


def shape(*dims, dtype=F32):
    return jax.ShapeDtypeStruct(dims, dtype)


def on_device(design, force, clamped_dof_mask, stiffness):
    planes, fy, fz = design.shape
    _, bx, by, _ = force.shape
    gx = lax.axis_size("gx")
    gy = lax.axis_size("gy")
    roles = lax.axis_size("role")
    devices = gx * gy * roles
    slabs = gx * gy
    assert roles == 2 and planes == 4 and fz == LANES and bx == 2 * gy and slabs % 2 == 0
    columns = fy // 4
    nodes = fy // 2
    tiles = nodes + 2
    count = tiles * 8
    pairs_a = [(i, i ^ 1) for i in range(slabs)]
    pairs_b = [(i, i + 1 if i % 2 else i - 1) for i in range(1, slabs - 1)]

    def beside(to_a, to_b):
        return lax.ppermute(to_a, LINE, pairs_a), lax.ppermute(to_b, LINE, pairs_b)

    free0 = (1 - clamped_dof_mask[:, 0]).astype(F32)
    next_plane = lax.ppermute(
        jnp.concatenate([free0 * force[:, 0], free0], axis=0), "gx", [(i + 1, i) for i in range(gx - 1)]
    )
    design_a, design_b = beside(design, design)
    pack, table = pl.pallas_call(
        prep_kernel,
        out_shape=(shape(gy, 6, 3, by, fz), shape(2 * ROWS, 2 * ROWS, dtype=BF16)),
        name="prep",
    )(force, clamped_dof_mask, next_plane, stiffness, jnp.asarray(place_table()))
    rf = lax.all_to_all(pack, "gy", 0, 0)

    role = lax.axis_index("role")

    def strip(x):
        return jnp.where(role == 0, x[..., fz - STRIP :], x[..., :STRIP]).reshape(-1, STRIP)

    strips = jnp.concatenate([strip(design), strip(design_a), strip(design_b), strip(rf)], axis=0)
    strips = lax.ppermute(strips, "role", [(0, 1), (1, 0)])

    node_set = shape(3 * count, LANES)
    plane = shape(count, LANES)
    element = shape(columns, LANES)
    tile_scratch = [
        pltpu.VMEM((3, tiles, 16, LANES), BF16),
        pltpu.VMEM((2, tiles, 16, LANES), BF16),
        pltpu.VMEM((2, count, LANES), F32),
    ]
    shift32 = pltpu.VMEM((2, count, LANES), F32)
    sw, factor, density, v0, free, local, to_a, to_b, e00 = pl.pallas_call(
        first_kernel,
        out_shape=(shape(planes + 4, fy, 2 * fz), element, element, node_set, node_set, node_set, plane, plane, element),
        scratch_shapes=[pltpu.VMEM((3 * planes, fy, 2 * fz), F32), pltpu.VMEM((fy, 2 * fz), F32)] + tile_scratch,
        name="first",
    )(design, design_a, design_b, strips, rf, table)
    from_a, from_b = beside(to_a, to_b)
    v1, local, to_a, to_b, e01, e11 = pl.pallas_call(
        second_kernel,
        out_shape=(node_set, node_set, plane, plane, element, element),
        scratch_shapes=tile_scratch + [shift32],
        name="second",
    )(v0, free, local, from_a, from_b, factor, table)
    from_a, from_b = beside(to_a, to_b)
    v2, e02, e12, e22, moments = pl.pallas_call(
        third_kernel,
        out_shape=(node_set, element, element, element, shape(devices, LANES)),
        scratch_shapes=tile_scratch + [shift32, shift32],
        name="third",
    )(v0, v1, free, local, from_a, from_b, factor, table, e00, e01, e11)
    moments = lax.all_to_all(moments, ("role", "gx", "gy"), 0, 0, tiled=True)
    grad, u = pl.pallas_call(
        combine_kernel,
        out_shape=(element, shape(gy, 3, 2, by, fz)),
        scratch_shapes=[pltpu.VMEM((2 * count, LANES), F32)],
        name="combine",
    )(moments, v0, v1, v2, e00, e01, e11, e02, e12, e22, density)
    grad_a, grad_b = beside(grad, grad)
    sensitivity = pl.pallas_call(
        last_kernel,
        out_shape=shape(planes, fy, fz),
        scratch_shapes=[pltpu.VMEM((planes + 4, fy, 2 * fz), F32)],
        name="last",
    )(grad, grad_a, grad_b, sw)
    u = lax.all_to_all(u, "gy", 0, 0)
    displacement = jnp.transpose(u, (1, 0, 2, 3, 4)).reshape(3, bx, by, fz)
    return sensitivity, displacement


def solution(mesh):
    placed = (
        P(("gx", "gy"), None, "role"),
        P(None, "gx", "gy", "role"),
        P(None, "gx", "gy", "role"),
        P(),
    )
    return jax.shard_map(
        on_device,
        mesh=mesh,
        in_specs=placed,
        out_specs=(P(("gx", "gy"), None, "role"), P(None, "gx", "gy", "role")),
        check_vma=False,
    )
```

```python
import jax
import jax.numpy as jnp
import numpy as np
from jax import lax
from jax.experimental import pallas as pl
from jax.experimental.pallas import tpu as pltpu
from jax.sharding import PartitionSpec as P

SHARPNESS = 4.0
THRESHOLD = 0.5
FLOOR_STIFF = 0.001
TANH2 = float(np.tanh(2.0))
LANES = 128
HALO = 3
STRIP = 8
ROWS = 120
LINE = ("gx", "gy")
KEEP = pltpu.CompilerParams(vmem_limit_bytes=20 << 20)
F32 = jnp.float32
BF16 = jnp.bfloat16


def iota(shape, dim):
    return lax.broadcasted_iota(jnp.int32, shape, dim)


def place_table():
    table = np.zeros((ROWS, 81), np.float32)
    for c in range(3):
        for b in range(3):
            for a in range(3):
                for q in range(3):
                    dof = ((c * 3 + b) * 3 + a) * 3 + q
                    if c < 2:
                        row = 8 * (3 * a + b) + 4 * c + q
                    else:
                        row = 72 + 8 * (2 * b + (a == 2)) + 4 * (a == 1) + q
                    table[row, dof] = 1.0
    return table


def split2(x):
    hi = x.astype(BF16)
    return hi, (x - hi.astype(F32)).astype(BF16)


def split3(x):
    hi = x.astype(BF16)
    rest = x - hi.astype(F32)
    mid = rest.astype(BF16)
    return hi, mid, (rest - mid.astype(F32)).astype(BF16)


def dot(a, b):
    return jnp.dot(a, b, preferred_element_type=F32)


def pick_right(x, table):
    hi, mid, lo = split3(x)
    return (dot(hi, table) + dot(mid, table)) + dot(lo, table)


def pick_left(table, x):
    hi, mid, lo = split3(x)
    return (dot(table, hi) + dot(table, mid)) + dot(table, lo)


def where_am_i():
    role = lax.axis_index("role")
    slab = lax.axis_index("gx") * lax.axis_size("gy") + lax.axis_index("gy")
    return role, slab


def element_lanes(shape, role, half):
    lane = iota(shape, len(shape) - 1)
    above = jnp.logical_and(lane >= half, lane < half + HALO)
    below = lane >= LANES - HALO
    roles = lax.axis_size("role")
    return (lane < half) | (above & (role < roles - 1)) | (below & (role > 0))


def hat_count(place, extent):
    low = jnp.where(place == 0, 3.0, jnp.where(place == 1, 1.0, 0.0))
    high = jnp.where(place == extent - 1, 3.0, jnp.where(place == extent - 2, 1.0, 0.0))
    return 9.0 - low - high


def smooth_z(x):
    width = x.shape[1]
    for _ in range(2):
        x = x + pltpu.roll(x, 1, 1) + pltpu.roll(x, width - 1, 1)
    return x


def smooth_y(x):
    rows = x.shape[0]
    x = jnp.concatenate([x, jnp.zeros((8, x.shape[1]), F32)], axis=0)
    for _ in range(2):
        x = x + pltpu.roll(x, 1, 0) + pltpu.roll(x, rows + 7, 0)
    return x[:rows]


def prep_kernel(force_ref, mask_ref, next_ref, stiff_ref, place_ref, pack_ref, table_ref):
    parts = pack_ref.shape[0]
    for q in range(3):
        free = 1.0 - mask_ref[q].astype(F32)
        rhs = free * force_ref[q]
        for row, val in ((q, rhs), (q + 3, free)):
            for j in range(parts):
                for a in range(3):
                    x = 2 * j + a
                    pack_ref[j, row, a] = val[x] if x < 2 * parts else next_ref[row]
    place = place_ref[...]
    half_way = jnp.dot(place, stiff_ref[...], precision=lax.Precision.HIGHEST, preferred_element_type=F32)
    spread = lax.dot_general(
        half_way, place, (((1,), (1,)), ((), ())), precision=lax.Precision.HIGHEST, preferred_element_type=F32
    )
    hi, lo = split2(spread)
    row = iota((ROWS, 2 * ROWS), 0)
    col = iota((ROWS, 2 * ROWS), 1)
    twice = jnp.where(row == 8 * (col // 16) + col % 8, 1.0, 0.0).astype(BF16)
    table_ref[:ROWS] = dot(hi, twice).astype(BF16)
    table_ref[ROWS:] = dot(lo, twice).astype(BF16)


def plane_rows(tiles):
    return tiles * 8


def shifted_tiles(nodes_ref, tiles, s):
    count = plane_rows(tiles)
    upper = (iota((count, LANES), 0) & 4) == 0
    if s == 0:
        first = nodes_ref[0:count]
        second = nodes_ref[count : 2 * count]
        x = jnp.where(upper, first, pltpu.roll(second, 4, 0))
    else:
        x = jnp.where(upper, nodes_ref[2 * count : 3 * count], 0.0)
    return pltpu.roll(x, LANES - 1, 1)


def pair_tiles(x):
    tiles = x.shape[0] // 8
    hi = x.astype(BF16).astype(F32)
    lo = x - hi
    both = jnp.concatenate([hi.reshape(tiles, 8, LANES), lo.reshape(tiles, 8, LANES)], axis=1)
    return both.astype(BF16)


def make_tiles(nodes_ref, main_ref, shift_ref, shift32_ref):
    tiles = main_ref.shape[1]
    count = plane_rows(tiles)
    for a in range(3):
        main_ref[a] = pair_tiles(nodes_ref[a * count : (a + 1) * count])
    for s in range(2):
        x = shifted_tiles(nodes_ref, tiles, s)
        if shift32_ref is not None:
            shift32_ref[s] = x
        shift_ref[s] = pair_tiles(x)


def sweep(table_ref, main_ref, shift_ref, factor_ref, out_ref, energies):
    tiles = main_ref.shape[1]
    columns = factor_ref.shape[0]
    upper = iota((8, LANES), 0) < 4

    def finish(node, parts):
        t0, t1, t2, s0, s1 = parts
        r0 = pltpu.roll(s0, 1, 1)
        r1 = pltpu.roll(s1, 1, 1)
        done = (
            t0 + jnp.where(upper, r0, 0.0),
            t1 + jnp.where(upper, pltpu.roll(r0, 4, 0), 0.0),
            t2 + jnp.where(upper, r1, 0.0),
        )
        for a in range(3):
            out_ref[pl.ds(pl.multiple_of((a * tiles + node) * 8, 8), 8), :] = done[a]

    def body(i, carry):
        cols = []
        for k in range(2):
            base = 4 * i + 2 * k
            pieces = [main_ref[a, base + b] for a in range(3) for b in range(3)]
            pieces += [shift_ref[s, base + b] for b in range(3) for s in range(2)]
            cols.append(jnp.concatenate(pieces, axis=0))
        product = dot(table_ref[...], jnp.concatenate(cols, axis=1))
        product = product[:ROWS] + product[ROWS:]
        parts = []
        for k in range(2):
            y = product[:, k * LANES : (k + 1) * LANES]
            base = 4 * i + 2 * k
            for nodes_ref, shift32_ref, e_ref in energies:
                total = None
                for a in range(3):
                    for b in range(3):
                        at = pl.multiple_of((a * tiles + base + b) * 8, 8)
                        term = nodes_ref[pl.ds(at, 8), :] * y[8 * (3 * a + b) : 8 * (3 * a + b) + 8]
                        total = term if total is None else total + term
                for b in range(3):
                    for s in range(2):
                        at = pl.multiple_of((base + b) * 8, 8)
                        lo = 72 + 8 * (2 * b + s)
                        total = total + shift32_ref[s, pl.ds(at, 8), :] * y[lo : lo + 8]
                e_ref[pl.ds(2 * i + k, 1), :] = jnp.sum(total, axis=0, keepdims=True)
            if out_ref is not None:
                z = y * factor_ref[pl.ds(2 * i + k, 1), :]
                parts.append(
                    [
                        [z[8 * (3 * a + b) : 8 * (3 * a + b) + 8] for a in range(3)]
                        + [z[72 + 8 * (2 * b + s) : 80 + 8 * (2 * b + s)] for s in range(2)]
                        for b in range(3)
                    ]
                )
        if out_ref is None:
            return carry
        left, right = parts
        finish(4 * i, [c + v for c, v in zip(carry, left[0])])
        finish(4 * i + 1, left[1])
        finish(4 * i + 2, [c + v for c, v in zip(left[2], right[0])])
        finish(4 * i + 3, right[1])
        return tuple(right[2])

    if out_ref is None:
        lax.fori_loop(0, columns // 2, lambda i, c: body(i, c), 0)
    else:
        zero = jnp.zeros((8, LANES), F32)
        lax.fori_loop(0, columns // 2, body, (zero,) * 5)
        for a in range(3):
            for node in range(2 * columns, tiles):
                at = (a * tiles + node) * 8
                out_ref[at : at + 8, :] = zero


def send_planes(local_ref, tiles, slab, to_a, to_b):
    count = plane_rows(tiles)
    low = local_ref[0:count]
    high = local_ref[2 * count : 3 * count]
    even = slab % 2 == 0
    to_a[...] = jnp.where(even, high, low)
    to_b[...] = jnp.where(even, low, high)


def gather_nodes(local_ref, from_a, from_b, free_ref, tiles, slab, nodes_ref):
    count = plane_rows(tiles)
    even = slab % 2 == 0
    a = from_a[...]
    b = from_b[...]
    nodes_ref[0:count] = free_ref[0:count] * (local_ref[0:count] + jnp.where(even, b, a))
    nodes_ref[count : 2 * count] = free_ref[count : 2 * count] * local_ref[count : 2 * count]
    nodes_ref[2 * count :] = free_ref[2 * count :] * (local_ref[2 * count :] + jnp.where(even, a, b))


def first_kernel(
    design_ref, da_ref, db_ref, strip_ref, rf_ref, table_ref,
    sw_ref, factor_ref, density_ref, nodes_ref, free_ref, local_ref, to_a, to_b, e00_ref,
    fine_ref, sum_ref, main_ref, shift_ref, shift32_ref,
):
    planes, fy, fz = design_ref.shape
    tiles = main_ref.shape[1]
    count = plane_rows(tiles)
    role, slab = where_am_i()
    slabs = lax.axis_size("gx") * lax.axis_size("gy")
    roles = lax.axis_size("role")
    half = fz // 2
    even = slab % 2 == 0

    at_lane = jnp.where(role == 0, 0, LANES - STRIP)
    put = jnp.where(iota((STRIP, LANES), 1) == iota((STRIP, LANES), 0) + at_lane, 1.0, 0.0).astype(BF16)
    for p in range(planes):
        a = da_ref[p]
        b = db_ref[p]
        fine_ref[p, :, :fz] = jnp.where(even, b, a)
        fine_ref[planes + p, :, :fz] = design_ref[p]
        fine_ref[2 * planes + p, :, :fz] = jnp.where(even, a, b)
    for p in range(planes):
        own = pick_right(strip_ref[p * fy : (p + 1) * fy], put)
        a = pick_right(strip_ref[(planes + p) * fy : (planes + p + 1) * fy], put)
        b = pick_right(strip_ref[(2 * planes + p) * fy : (2 * planes + p + 1) * fy], put)
        fine_ref[p, :, fz:] = jnp.where(even, b, a)
        fine_ref[planes + p, :, fz:] = own
        fine_ref[2 * planes + p, :, fz:] = jnp.where(even, a, b)

    width = 2 * fz
    lane = iota((1, width), 1)
    z_place = role * fz + jnp.where(lane < fz + fz // 2, lane, lane - width)
    inv_z = 1.0 / hat_count(z_place, roles * fz)
    inv_y = 1.0 / hat_count(iota((fy, 1), 0), fy)
    inv_yz = inv_y * inv_z
    sum_ref[...] = jnp.zeros((fy, width), F32)

    def filter_plane(p, _):
        x = fine_ref[p] + fine_ref[p + 4] + 2.0 * (fine_ref[p + 1] + fine_ref[p + 3]) + 3.0 * fine_ref[p + 2]
        x = smooth_y(smooth_z(x))
        place = jnp.full((1, 1), slab * planes + p - 2, jnp.int32)
        inv = inv_yz * (1.0 / hat_count(place, slabs * planes))
        bent = jnp.tanh(SHARPNESS * (x * inv - THRESHOLD))
        sw_ref[p] = (SHARPNESS / (2.0 * TANH2)) * (1.0 - bent * bent) * inv
        mine = jnp.logical_and(p >= 2, p < 2 + planes)
        sum_ref[...] += jnp.where(mine, (TANH2 + bent) * (1.0 / (2.0 * TANH2)), 0.0)
        return 0

    lax.fori_loop(0, planes + 4, filter_plane, 0)

    rows = factor_ref.shape[0]
    pool_y = jnp.where(iota((rows, fy), 1) // 4 == iota((rows, fy), 0), 1.0, 0.0).astype(BF16)
    pool_z = jnp.where(iota((width, LANES), 0) // 2 == iota((width, LANES), 1), 1.0, 0.0).astype(BF16)
    density = pick_right(pick_left(pool_y, sum_ref[...]), pool_z) * (1.0 / 32.0)
    inside = element_lanes((rows, LANES), role, half)
    density = jnp.where(inside, density, 0.0)
    density_ref[...] = density
    factor_ref[...] = jnp.where(inside, FLOOR_STIFF + (1.0 - FLOOR_STIFF) * density * density * density, 0.0)

    nodes_ref[...] = jnp.zeros(nodes_ref.shape, F32)
    free_ref[...] = jnp.zeros(free_ref.shape, F32)
    zi = iota((LANES, width), 0)
    ci = iota((LANES, width), 1)
    lane_of = ci & (LANES - 1)
    odd = ci // LANES
    own_table = jnp.where(zi == 2 * lane_of + odd, 1.0, 0.0).astype(BF16)
    si = iota((STRIP, width), 0)
    ci = iota((STRIP, width), 1)
    lane_of = ci & (LANES - 1)
    odd = ci // LANES
    first_lane = jnp.where(role == 0, half, LANES - STRIP // 2)
    strip_table = jnp.where(si == 2 * (lane_of - first_lane) + odd, 1.0, 0.0).astype(BF16)
    parts = rf_ref.shape[0]
    deep = rf_ref.shape[3]
    base = 3 * planes * fy
    for row in range(6):
        for a in range(3):
            x = jnp.concatenate([rf_ref[j, row, a] for j in range(parts)], axis=0)
            st = jnp.concatenate(
                [
                    strip_ref[base + ((j * 6 + row) * 3 + a) * deep : base + ((j * 6 + row) * 3 + a + 1) * deep]
                    for j in range(parts)
                ],
                axis=0,
            )
            if row < 3:
                y = pick_right(x, own_table) + pick_right(st, strip_table)
                dest = nodes_ref
            else:
                y = dot(x.astype(BF16), own_table) + dot(st.astype(BF16), strip_table)
                dest = free_ref
            q = row % 3
            dest[pl.ds(a * count + q, parts * deep, stride=8), :] = y[:, :LANES]
            dest[pl.ds(a * count + 4 + q, parts * deep, stride=8), :] = y[:, LANES:]

    make_tiles(nodes_ref, main_ref, shift_ref, shift32_ref)
    sweep(table_ref, main_ref, shift_ref, factor_ref, local_ref, [(nodes_ref, shift32_ref, e00_ref)])
    send_planes(local_ref, tiles, slab, to_a, to_b)


def second_kernel(
    prev_ref, free_ref, last_ref, from_a, from_b, factor_ref, table_ref,
    nodes_ref, local_ref, to_a, to_b, e01_ref, e11_ref,
    main_ref, shift_ref, shift32_ref, prev32_ref,
):
    tiles = main_ref.shape[1]
    role, slab = where_am_i()
    gather_nodes(last_ref, from_a, from_b, free_ref, tiles, slab, nodes_ref)
    for s in range(2):
        prev32_ref[s] = shifted_tiles(prev_ref, tiles, s)
    make_tiles(nodes_ref, main_ref, shift_ref, shift32_ref)
    sweep(
        table_ref, main_ref, shift_ref, factor_ref, local_ref,
        [(prev_ref, prev32_ref, e01_ref), (nodes_ref, shift32_ref, e11_ref)],
    )
    send_planes(local_ref, tiles, slab, to_a, to_b)


def third_kernel(
    v0_ref, v1_ref, free_ref, last_ref, from_a, from_b, factor_ref, table_ref, e00_ref, e01_ref, e11_ref,
    nodes_ref, e02_ref, e12_ref, e22_ref, moment_ref,
    main_ref, shift_ref, shift32_ref, s0_ref, s1_ref,
):
    tiles = main_ref.shape[1]
    count = plane_rows(tiles)
    role, slab = where_am_i()
    gather_nodes(last_ref, from_a, from_b, free_ref, tiles, slab, nodes_ref)
    for s in range(2):
        s0_ref[s] = shifted_tiles(v0_ref, tiles, s)
        s1_ref[s] = shifted_tiles(v1_ref, tiles, s)
    make_tiles(nodes_ref, main_ref, shift_ref, shift32_ref)
    sweep(
        table_ref, main_ref, shift_ref, factor_ref, None,
        [(v0_ref, s0_ref, e02_ref), (v1_ref, s1_ref, e12_ref), (nodes_ref, shift32_ref, e22_ref)],
    )
    half = LANES // 2
    own = iota((1, LANES), 1) < half
    v0 = v0_ref[0 : 2 * count]
    sums = [jnp.sum(v0 * v0, axis=0, keepdims=True)]
    for e_ref in (e00_ref, e01_ref, e11_ref, e12_ref, e22_ref):
        sums.append(jnp.sum(factor_ref[...] * e_ref[...], axis=0, keepdims=True))
    lane = iota((1, LANES), 1)
    out = jnp.zeros((1, LANES), F32)
    for k, s in enumerate(sums):
        total = jnp.sum(jnp.where(own, s, 0.0), axis=1, keepdims=True)
        out = jnp.where(lane == k, total, out)
    moment_ref[...] = jnp.broadcast_to(out, moment_ref.shape)


def combine_kernel(
    moment_ref, v0_ref, v1_ref, v2_ref, e00_ref, e01_ref, e11_ref, e02_ref, e12_ref, e22_ref, density_ref,
    grad_ref, u_ref, nodes_ref,
):
    role, slab = where_am_i()
    parts, _, _, deep, fz = u_ref.shape
    half = fz // 2
    count = v0_ref.shape[0] // 3
    total = jnp.sum(moment_ref[...], axis=0, keepdims=True)
    lane = iota((1, LANES), 1)
    m = [jnp.sum(jnp.where(lane == k, total, 0.0), axis=1, keepdims=True) for k in range(6)]
    s = m[1] / m[0]
    inv = 1.0 / s
    mu = [jnp.ones_like(s)]
    power = 1.0 / m[0]
    for k in range(1, 6):
        power = power * inv
        mu.append(m[k] * power)
    nu = list(mu)
    for depth in range(1, 6):
        for k in range(5, depth - 1, -1):
            nu[k] = nu[k] - nu[k - 1]
    g = [nu[k] + nu[k + 1] for k in range(5)]
    l10 = g[1] / g[0]
    l20 = g[2] / g[0]
    d1 = g[2] - l10 * g[1]
    x12 = g[3] - l10 * g[2]
    r1 = nu[1] - l10 * nu[0]
    r2 = nu[2] - l20 * nu[0]
    l21 = x12 / d1
    d2 = (g[4] - l20 * g[2]) - l21 * x12
    c2 = (r2 - l21 * r1) / d2
    c1 = (r1 - x12 * c2) / d1
    c0 = (nu[0] - g[1] * c1 - g[2] * c2) / g[0]
    w0 = (c0 - c1 + c2) * inv
    w1 = (c1 - 2.0 * c2) * inv * inv
    w2 = c2 * inv * inv * inv
    energy = (
        w0 * (w0 * e00_ref[...] + 2.0 * (w1 * e01_ref[...] + w2 * e02_ref[...]))
        + w1 * (w1 * e11_ref[...] + 2.0 * w2 * e12_ref[...])
        + w2 * w2 * e22_ref[...]
    )
    density = density_ref[...]
    grad = (-3.0 * (1.0 - FLOOR_STIFF) / 32.0) * density * density * energy
    grad_ref[...] = jnp.where(element_lanes(grad.shape, role, half), grad, 0.0)
    nodes_ref[...] = w0 * v0_ref[0 : 2 * count] + w1 * v1_ref[0 : 2 * count] + w2 * v2_ref[0 : 2 * count]
    gi = iota((LANES, fz), 0)
    zi = iota((LANES, fz), 1)
    even_table = jnp.where(zi == 2 * gi, 1.0, 0.0).astype(BF16)
    odd_table = jnp.where(zi == 2 * gi + 1, 1.0, 0.0).astype(BF16)
    for a in range(2):
        for q in range(3):
            even = nodes_ref[pl.ds(a * count + q, parts * deep, stride=8), :]
            odd = nodes_ref[pl.ds(a * count + 4 + q, parts * deep, stride=8), :]
            x = pick_right(even, even_table) + pick_right(odd, odd_table)
            for j in range(parts):
                u_ref[j, q, a] = x[j * deep : (j + 1) * deep]


def last_kernel(grad_ref, ga_ref, gb_ref, sw_ref, out_ref, work_ref):
    planes, fy, fz = out_ref.shape
    width = 2 * fz
    role, slab = where_am_i()
    even = slab % 2 == 0
    rows = grad_ref.shape[0]
    pool_y = jnp.where(iota((fy, rows), 0) // 4 == iota((fy, rows), 1), 1.0, 0.0).astype(BF16)
    pool_z = jnp.where(iota((LANES, width), 1) // 2 == iota((LANES, width), 0), 1.0, 0.0).astype(BF16)
    a = ga_ref[...]
    b = gb_ref[...]
    low = jnp.where(even, b, a)
    high = jnp.where(even, a, b)
    for grad, first, last in ((low, 0, 2), (grad_ref[...], 2, 2 + planes), (high, 2 + planes, 4 + planes)):
        wide = pick_right(pick_left(pool_y, grad), pool_z)
        for p in range(first, last):
            work_ref[p] = wide * sw_ref[p]

    def body(p, _):
        x = work_ref[p] + work_ref[p + 4] + 2.0 * (work_ref[p + 1] + work_ref[p + 3]) + 3.0 * work_ref[p + 2]
        out_ref[p] = smooth_y(smooth_z(x))[:, :fz]
        return 0

    lax.fori_loop(0, planes, body, 0)


def shape(*dims, dtype=F32):
    return jax.ShapeDtypeStruct(dims, dtype)


def on_device(design, force, clamped_dof_mask, stiffness):
    planes, fy, fz = design.shape
    _, bx, by, _ = force.shape
    gx = lax.axis_size("gx")
    gy = lax.axis_size("gy")
    roles = lax.axis_size("role")
    devices = gx * gy * roles
    slabs = gx * gy
    assert roles == 2 and planes == 4 and fz == LANES and bx == 2 * gy and slabs % 2 == 0
    columns = fy // 4
    nodes = fy // 2
    tiles = nodes + 2
    count = tiles * 8
    pairs_a = [(i, i ^ 1) for i in range(slabs)]
    pairs_b = [(i, i + 1 if i % 2 else i - 1) for i in range(1, slabs - 1)]

    def beside(to_a, to_b):
        return lax.ppermute(to_a, LINE, pairs_a), lax.ppermute(to_b, LINE, pairs_b)

    free0 = (1 - clamped_dof_mask[:, 0]).astype(F32)
    next_plane = lax.ppermute(
        jnp.concatenate([free0 * force[:, 0], free0], axis=0), "gx", [(i + 1, i) for i in range(gx - 1)]
    )
    design_a, design_b = beside(design, design)
    pack, table = pl.pallas_call(
        prep_kernel,
        out_shape=(shape(gy, 6, 3, by, fz), shape(2 * ROWS, 2 * ROWS, dtype=BF16)),
        name="prep",
        compiler_params=KEEP,
    )(force, clamped_dof_mask, next_plane, stiffness, jnp.asarray(place_table()))
    rf = lax.all_to_all(pack, "gy", 0, 0)

    role = lax.axis_index("role")

    def strip(x):
        return jnp.where(role == 0, x[..., fz - STRIP :], x[..., :STRIP]).reshape(-1, STRIP)

    strips = jnp.concatenate([strip(design), strip(design_a), strip(design_b), strip(rf)], axis=0)
    strips = lax.ppermute(strips, "role", [(0, 1), (1, 0)])

    node_set = shape(3 * count, LANES)
    plane = shape(count, LANES)
    element = shape(columns, LANES)
    tile_scratch = [
        pltpu.VMEM((3, tiles, 16, LANES), BF16),
        pltpu.VMEM((2, tiles, 16, LANES), BF16),
        pltpu.VMEM((2, count, LANES), F32),
    ]
    shift32 = pltpu.VMEM((2, count, LANES), F32)
    sw, factor, density, v0, free, local, to_a, to_b, e00 = pl.pallas_call(
        first_kernel,
        out_shape=(shape(planes + 4, fy, 2 * fz), element, element, node_set, node_set, node_set, plane, plane, element),
        scratch_shapes=[pltpu.VMEM((3 * planes, fy, 2 * fz), F32), pltpu.VMEM((fy, 2 * fz), F32)] + tile_scratch,
        name="first",
        compiler_params=KEEP,
    )(design, design_a, design_b, strips, rf, table)
    from_a, from_b = beside(to_a, to_b)
    v1, local, to_a, to_b, e01, e11 = pl.pallas_call(
        second_kernel,
        out_shape=(node_set, node_set, plane, plane, element, element),
        scratch_shapes=tile_scratch + [shift32],
        name="second",
        compiler_params=KEEP,
    )(v0, free, local, from_a, from_b, factor, table)
    from_a, from_b = beside(to_a, to_b)
    v2, e02, e12, e22, moments = pl.pallas_call(
        third_kernel,
        out_shape=(node_set, element, element, element, shape(devices, LANES)),
        scratch_shapes=tile_scratch + [shift32, shift32],
        name="third",
        compiler_params=KEEP,
    )(v0, v1, free, local, from_a, from_b, factor, table, e00, e01, e11)
    moments = lax.all_to_all(moments, ("role", "gx", "gy"), 0, 0, tiled=True)
    grad, u = pl.pallas_call(
        combine_kernel,
        out_shape=(element, shape(gy, 3, 2, by, fz)),
        scratch_shapes=[pltpu.VMEM((2 * count, LANES), F32)],
        name="combine",
        compiler_params=KEEP,
    )(moments, v0, v1, v2, e00, e01, e11, e02, e12, e22, density)
    grad_a, grad_b = beside(grad, grad)
    sensitivity = pl.pallas_call(
        last_kernel,
        out_shape=shape(planes, fy, fz),
        scratch_shapes=[pltpu.VMEM((planes + 4, fy, 2 * fz), F32)],
        name="last",
        compiler_params=KEEP,
    )(grad, grad_a, grad_b, sw)
    u = lax.all_to_all(u, "gy", 0, 0)
    displacement = jnp.transpose(u, (1, 0, 2, 3, 4)).reshape(3, bx, by, fz)
    return sensitivity, displacement


def solution(mesh):
    placed = (
        P(("gx", "gy"), None, "role"),
        P(None, "gx", "gy", "role"),
        P(None, "gx", "gy", "role"),
        P(),
    )
    return jax.shard_map(
        on_device,
        mesh=mesh,
        in_specs=placed,
        out_specs=(P(("gx", "gy"), None, "role"), P(None, "gx", "gy", "role")),
        check_vma=False,
    )
```

```python
import jax
import jax.numpy as jnp
import numpy as np
from jax import lax
from jax.experimental import pallas as pl
from jax.experimental.pallas import tpu as pltpu
from jax.sharding import PartitionSpec as P

SHARPNESS = 4.0
THRESHOLD = 0.5
FLOOR_STIFF = 0.001
TANH2 = float(np.tanh(2.0))
LANES = 128
HALO = 3
STRIP = 8
ROWS = 120
LINE = ("gx", "gy")
KEEP = pltpu.CompilerParams(vmem_limit_bytes=12 << 20)
F32 = jnp.float32
BF16 = jnp.bfloat16


def iota(shape, dim):
    return lax.broadcasted_iota(jnp.int32, shape, dim)


def place_table():
    table = np.zeros((ROWS, 81), np.float32)
    for c in range(3):
        for b in range(3):
            for a in range(3):
                for q in range(3):
                    dof = ((c * 3 + b) * 3 + a) * 3 + q
                    if c < 2:
                        row = 8 * (3 * a + b) + 4 * c + q
                    else:
                        row = 72 + 8 * (2 * b + (a == 2)) + 4 * (a == 1) + q
                    table[row, dof] = 1.0
    return table


def split2(x):
    hi = x.astype(BF16)
    return hi, (x - hi.astype(F32)).astype(BF16)


def split3(x):
    hi = x.astype(BF16)
    rest = x - hi.astype(F32)
    mid = rest.astype(BF16)
    return hi, mid, (rest - mid.astype(F32)).astype(BF16)


def dot(a, b):
    return jnp.dot(a, b, preferred_element_type=F32)


def pick_right(x, table):
    hi, mid, lo = split3(x)
    return (dot(hi, table) + dot(mid, table)) + dot(lo, table)


def pick_left(table, x):
    hi, mid, lo = split3(x)
    return (dot(table, hi) + dot(table, mid)) + dot(table, lo)


def where_am_i():
    role = lax.axis_index("role")
    slab = lax.axis_index("gx") * lax.axis_size("gy") + lax.axis_index("gy")
    return role, slab


def element_lanes(shape, role, half):
    lane = iota(shape, len(shape) - 1)
    above = jnp.logical_and(lane >= half, lane < half + HALO)
    below = lane >= LANES - HALO
    roles = lax.axis_size("role")
    return (lane < half) | (above & (role < roles - 1)) | (below & (role > 0))


def hat_count(place, extent):
    low = jnp.where(place == 0, 3.0, jnp.where(place == 1, 1.0, 0.0))
    high = jnp.where(place == extent - 1, 3.0, jnp.where(place == extent - 2, 1.0, 0.0))
    return 9.0 - low - high


def smooth_z(x):
    width = x.shape[1]
    for _ in range(2):
        x = x + pltpu.roll(x, 1, 1) + pltpu.roll(x, width - 1, 1)
    return x


def smooth_y(x):
    rows = x.shape[0]
    x = jnp.concatenate([x, jnp.zeros((8, x.shape[1]), F32)], axis=0)
    for _ in range(2):
        x = x + pltpu.roll(x, 1, 0) + pltpu.roll(x, rows + 7, 0)
    return x[:rows]


def strip_rows_kernel(force_ref, mask_ref, plane_ref, strip_ref, corner_ref):
    _, bx, by, fz = force_ref.shape
    role, _ = where_am_i()
    first = jnp.where(role == 0, fz - STRIP, 0)
    take = jnp.where(iota((fz, LANES), 0) == first + (iota((fz, LANES), 1) & (STRIP - 1)), 1.0, 0.0).astype(BF16)
    own_y = (iota((bx, by, LANES), 2) // STRIP) == iota((bx, by, LANES), 1)
    corner_ref[...] = jnp.zeros(corner_ref.shape, F32)
    for q in range(3):
        free = 1.0 - mask_ref[q].astype(F32)
        rhs = free * force_ref[q]
        plane_ref[q * by : (q + 1) * by] = rhs[0]
        plane_ref[(q + 3) * by : (q + 4) * by] = free[0]
        edge = pick_right(rhs.reshape(bx * by, fz), take), dot(free.reshape(bx * by, fz).astype(BF16), take)
        for row, x in ((q, edge[0]), (q + 3, edge[1])):
            x = jnp.sum(jnp.where(own_y, x.reshape(bx, by, LANES), 0.0), axis=1)
            strip_ref[row * bx : (row + 1) * bx] = x
            corner_ref[row : row + 1] = x[0:1]


def pack_kernel(force_ref, mask_ref, plane_ref, strip_ref, corner_ref, stiff_ref, place_ref, pack_ref, table_ref):
    _, bx, by, _ = force_ref.shape
    parts = pack_ref.shape[0]
    tail = 18 * by
    for j in range(parts):
        pack_ref[j, tail + 18 :] = jnp.zeros((pack_ref.shape[1] - tail - 18, LANES), F32)
    for q in range(3):
        free = 1.0 - mask_ref[q].astype(F32)
        rhs = free * force_ref[q]
        for row, val in ((q, rhs), (q + 3, free)):
            for j in range(parts):
                for a in range(3):
                    x = 2 * j + a
                    at = row * 3 + a
                    inner = x < bx
                    pack_ref[j, at * by : (at + 1) * by] = val[x] if inner else plane_ref[row * by : (row + 1) * by]
                    edge = strip_ref[row * bx + x : row * bx + x + 1] if inner else corner_ref[row : row + 1]
                    pack_ref[j, tail + at : tail + at + 1] = edge
    place = place_ref[...]
    half_way = jnp.dot(place, stiff_ref[...], precision=lax.Precision.HIGHEST, preferred_element_type=F32)
    spread = lax.dot_general(
        half_way, place, (((1,), (1,)), ((), ())), precision=lax.Precision.HIGHEST, preferred_element_type=F32
    )
    hi, lo = split2(spread)
    row = iota((ROWS, 2 * ROWS), 0)
    col = iota((ROWS, 2 * ROWS), 1)
    twice = jnp.where(row == 8 * (col // 16) + col % 8, 1.0, 0.0).astype(BF16)
    table_ref[:ROWS] = dot(hi, twice).astype(BF16)
    table_ref[ROWS:] = dot(lo, twice).astype(BF16)


def plane_rows(tiles):
    return tiles * 8


def shifted_tiles(nodes_ref, tiles, s):
    count = plane_rows(tiles)
    upper = (iota((count, LANES), 0) & 4) == 0
    if s == 0:
        first = nodes_ref[0:count]
        second = nodes_ref[count : 2 * count]
        x = jnp.where(upper, first, pltpu.roll(second, 4, 0))
    else:
        x = jnp.where(upper, nodes_ref[2 * count : 3 * count], 0.0)
    return pltpu.roll(x, LANES - 1, 1)


def pair_tiles(x):
    tiles = x.shape[0] // 8
    hi = x.astype(BF16).astype(F32)
    lo = x - hi
    both = jnp.concatenate([hi.reshape(tiles, 8, LANES), lo.reshape(tiles, 8, LANES)], axis=1)
    return both.astype(BF16)


def make_tiles(nodes_ref, main_ref, shift_ref, shift32_ref):
    tiles = main_ref.shape[1]
    count = plane_rows(tiles)
    for a in range(3):
        main_ref[a] = pair_tiles(nodes_ref[a * count : (a + 1) * count])
    for s in range(2):
        x = shifted_tiles(nodes_ref, tiles, s)
        if shift32_ref is not None:
            shift32_ref[s] = x
        shift_ref[s] = pair_tiles(x)


def sweep(table_ref, main_ref, shift_ref, factor_ref, out_ref, energies):
    tiles = main_ref.shape[1]
    columns = factor_ref.shape[0]
    upper = iota((8, LANES), 0) < 4

    def finish(node, parts):
        t0, t1, t2, s0, s1 = parts
        r0 = pltpu.roll(s0, 1, 1)
        r1 = pltpu.roll(s1, 1, 1)
        done = (
            t0 + jnp.where(upper, r0, 0.0),
            t1 + jnp.where(upper, pltpu.roll(r0, 4, 0), 0.0),
            t2 + jnp.where(upper, r1, 0.0),
        )
        for a in range(3):
            out_ref[pl.ds(pl.multiple_of((a * tiles + node) * 8, 8), 8), :] = done[a]

    def body(i, carry):
        cols = []
        for k in range(2):
            base = 4 * i + 2 * k
            pieces = [main_ref[a, base + b] for a in range(3) for b in range(3)]
            pieces += [shift_ref[s, base + b] for b in range(3) for s in range(2)]
            cols.append(jnp.concatenate(pieces, axis=0))
        product = dot(table_ref[...], jnp.concatenate(cols, axis=1))
        product = product[:ROWS] + product[ROWS:]
        parts = []
        for k in range(2):
            y = product[:, k * LANES : (k + 1) * LANES]
            base = 4 * i + 2 * k
            for nodes_ref, shift32_ref, e_ref in energies:
                total = None
                for a in range(3):
                    for b in range(3):
                        at = pl.multiple_of((a * tiles + base + b) * 8, 8)
                        term = nodes_ref[pl.ds(at, 8), :] * y[8 * (3 * a + b) : 8 * (3 * a + b) + 8]
                        total = term if total is None else total + term
                for b in range(3):
                    for s in range(2):
                        at = pl.multiple_of((base + b) * 8, 8)
                        lo = 72 + 8 * (2 * b + s)
                        total = total + shift32_ref[s, pl.ds(at, 8), :] * y[lo : lo + 8]
                e_ref[pl.ds(2 * i + k, 1), :] = jnp.sum(total, axis=0, keepdims=True)
            if out_ref is not None:
                z = y * factor_ref[pl.ds(2 * i + k, 1), :]
                parts.append(
                    [
                        [z[8 * (3 * a + b) : 8 * (3 * a + b) + 8] for a in range(3)]
                        + [z[72 + 8 * (2 * b + s) : 80 + 8 * (2 * b + s)] for s in range(2)]
                        for b in range(3)
                    ]
                )
        if out_ref is None:
            return carry
        left, right = parts
        finish(4 * i, [c + v for c, v in zip(carry, left[0])])
        finish(4 * i + 1, left[1])
        finish(4 * i + 2, [c + v for c, v in zip(left[2], right[0])])
        finish(4 * i + 3, right[1])
        return tuple(right[2])

    if out_ref is None:
        lax.fori_loop(0, columns // 2, lambda i, c: body(i, c), 0)
    else:
        zero = jnp.zeros((8, LANES), F32)
        lax.fori_loop(0, columns // 2, body, (zero,) * 5)
        for a in range(3):
            for node in range(2 * columns, tiles):
                at = (a * tiles + node) * 8
                out_ref[at : at + 8, :] = zero


def send_planes(local_ref, tiles, slab, to_a, to_b):
    count = plane_rows(tiles)
    low = local_ref[0:count]
    high = local_ref[2 * count : 3 * count]
    even = slab % 2 == 0
    to_a[...] = jnp.where(even, high, low)
    to_b[...] = jnp.where(even, low, high)


def gather_nodes(local_ref, from_a, from_b, free_ref, tiles, slab, nodes_ref):
    count = plane_rows(tiles)
    even = slab % 2 == 0
    a = from_a[...]
    b = from_b[...]
    nodes_ref[0:count] = free_ref[0:count] * (local_ref[0:count] + jnp.where(even, b, a))
    nodes_ref[count : 2 * count] = free_ref[count : 2 * count] * local_ref[count : 2 * count]
    nodes_ref[2 * count :] = free_ref[2 * count :] * (local_ref[2 * count :] + jnp.where(even, a, b))


def filter_kernel(design_ref, da_ref, db_ref, strip_ref, sw_ref, factor_ref, density_ref, fine_ref, sum_ref):
    planes, fy, fz = design_ref.shape
    role, slab = where_am_i()
    slabs = lax.axis_size("gx") * lax.axis_size("gy")
    roles = lax.axis_size("role")
    half = fz // 2
    even = slab % 2 == 0

    at_lane = jnp.where(role == 0, 0, LANES - STRIP)
    put = jnp.where(iota((STRIP, LANES), 1) == iota((STRIP, LANES), 0) + at_lane, 1.0, 0.0).astype(BF16)
    for p in range(planes):
        a = da_ref[p]
        b = db_ref[p]
        fine_ref[p, :, :fz] = jnp.where(even, b, a)
        fine_ref[planes + p, :, :fz] = design_ref[p]
        fine_ref[2 * planes + p, :, :fz] = jnp.where(even, a, b)
    for p in range(planes):
        own = pick_right(strip_ref[p * fy : (p + 1) * fy], put)
        a = pick_right(strip_ref[(planes + p) * fy : (planes + p + 1) * fy], put)
        b = pick_right(strip_ref[(2 * planes + p) * fy : (2 * planes + p + 1) * fy], put)
        fine_ref[p, :, fz:] = jnp.where(even, b, a)
        fine_ref[planes + p, :, fz:] = own
        fine_ref[2 * planes + p, :, fz:] = jnp.where(even, a, b)

    width = 2 * fz
    lane = iota((1, width), 1)
    z_place = role * fz + jnp.where(lane < fz + fz // 2, lane, lane - width)
    inv_z = 1.0 / hat_count(z_place, roles * fz)
    inv_y = 1.0 / hat_count(iota((fy, 1), 0), fy)
    inv_yz = inv_y * inv_z
    sum_ref[...] = jnp.zeros((fy, width), F32)

    def filter_plane(p, _):
        x = fine_ref[p] + fine_ref[p + 4] + 2.0 * (fine_ref[p + 1] + fine_ref[p + 3]) + 3.0 * fine_ref[p + 2]
        x = smooth_y(smooth_z(x))
        place = jnp.full((1, 1), slab * planes + p - 2, jnp.int32)
        inv = inv_yz * (1.0 / hat_count(place, slabs * planes))
        bent = jnp.tanh(SHARPNESS * (x * inv - THRESHOLD))
        sw_ref[p] = (SHARPNESS / (2.0 * TANH2)) * (1.0 - bent * bent) * inv
        mine = jnp.logical_and(p >= 2, p < 2 + planes)
        sum_ref[...] += jnp.where(mine, (TANH2 + bent) * (1.0 / (2.0 * TANH2)), 0.0)
        return 0

    lax.fori_loop(0, planes + 4, filter_plane, 0)

    rows = factor_ref.shape[0]
    pool_y = jnp.where(iota((rows, fy), 1) // 4 == iota((rows, fy), 0), 1.0, 0.0).astype(BF16)
    pool_z = jnp.where(iota((width, LANES), 0) // 2 == iota((width, LANES), 1), 1.0, 0.0).astype(BF16)
    density = pick_right(pick_left(pool_y, sum_ref[...]), pool_z) * (1.0 / 32.0)
    inside = element_lanes((rows, LANES), role, half)
    density = jnp.where(inside, density, 0.0)
    density_ref[...] = density
    factor_ref[...] = jnp.where(inside, FLOOR_STIFF + (1.0 - FLOOR_STIFF) * density * density * density, 0.0)


def first_kernel(
    rf_ref, factor_ref, table_ref,
    nodes_ref, free_ref, local_ref, to_a, to_b, e00_ref,
    main_ref, shift_ref, shift32_ref,
):
    tiles = main_ref.shape[1]
    count = plane_rows(tiles)
    role, slab = where_am_i()
    half = LANES // 2
    parts = rf_ref.shape[0]
    deep = (2 * factor_ref.shape[0]) // parts
    tail = 18 * deep

    nodes_ref[...] = jnp.zeros(nodes_ref.shape, F32)
    free_ref[...] = jnp.zeros(free_ref.shape, F32)
    zi = iota((2 * LANES, 2 * LANES), 0)
    ci = iota((2 * LANES, 2 * LANES), 1)
    lane_of = ci & (LANES - 1)
    odd = ci // LANES
    first_lane = jnp.where(role == 0, half, LANES - STRIP // 2)
    own = zi == 2 * lane_of + odd
    edge = (zi & (STRIP - 1)) == 2 * (lane_of - first_lane) + odd
    table = jnp.where(zi < LANES, jnp.where(own, 1.0, 0.0), jnp.where(edge, 1.0, 0.0)).astype(BF16)
    own_y = (iota((deep, LANES), 1) // STRIP) == iota((deep, LANES), 0)
    for row in range(6):
        for a in range(3):
            at = row * 3 + a
            x = jnp.concatenate([rf_ref[j, at * deep : (at + 1) * deep] for j in range(parts)], axis=0)
            st = jnp.concatenate(
                [jnp.where(own_y, rf_ref[j, tail + at : tail + at + 1], 0.0) for j in range(parts)], axis=0
            )
            x = jnp.concatenate([x, st], axis=1)
            if row < 3:
                y = pick_right(x, table)
                dest = nodes_ref
            else:
                y = dot(x.astype(BF16), table)
                dest = free_ref
            q = row % 3
            dest[pl.ds(a * count + q, parts * deep, stride=8), :] = y[:, :LANES]
            dest[pl.ds(a * count + 4 + q, parts * deep, stride=8), :] = y[:, LANES:]

    make_tiles(nodes_ref, main_ref, shift_ref, shift32_ref)
    sweep(table_ref, main_ref, shift_ref, factor_ref, local_ref, [(nodes_ref, shift32_ref, e00_ref)])
    send_planes(local_ref, tiles, slab, to_a, to_b)


def second_kernel(
    prev_ref, free_ref, last_ref, from_a, from_b, factor_ref, table_ref,
    nodes_ref, local_ref, to_a, to_b, e01_ref, e11_ref,
    main_ref, shift_ref, shift32_ref, prev32_ref,
):
    tiles = main_ref.shape[1]
    role, slab = where_am_i()
    gather_nodes(last_ref, from_a, from_b, free_ref, tiles, slab, nodes_ref)
    for s in range(2):
        prev32_ref[s] = shifted_tiles(prev_ref, tiles, s)
    make_tiles(nodes_ref, main_ref, shift_ref, shift32_ref)
    sweep(
        table_ref, main_ref, shift_ref, factor_ref, local_ref,
        [(prev_ref, prev32_ref, e01_ref), (nodes_ref, shift32_ref, e11_ref)],
    )
    send_planes(local_ref, tiles, slab, to_a, to_b)


def third_kernel(
    v0_ref, v1_ref, free_ref, last_ref, from_a, from_b, factor_ref, table_ref, e00_ref, e01_ref, e11_ref,
    nodes_ref, e02_ref, e12_ref, e22_ref, moment_ref,
    main_ref, shift_ref, shift32_ref, s0_ref, s1_ref,
):
    tiles = main_ref.shape[1]
    count = plane_rows(tiles)
    role, slab = where_am_i()
    gather_nodes(last_ref, from_a, from_b, free_ref, tiles, slab, nodes_ref)
    for s in range(2):
        s0_ref[s] = shifted_tiles(v0_ref, tiles, s)
        s1_ref[s] = shifted_tiles(v1_ref, tiles, s)
    make_tiles(nodes_ref, main_ref, shift_ref, shift32_ref)
    sweep(
        table_ref, main_ref, shift_ref, factor_ref, None,
        [(v0_ref, s0_ref, e02_ref), (v1_ref, s1_ref, e12_ref), (nodes_ref, shift32_ref, e22_ref)],
    )
    half = LANES // 2
    own = iota((1, LANES), 1) < half
    v0 = v0_ref[0 : 2 * count]
    sums = [jnp.sum(v0 * v0, axis=0, keepdims=True)]
    for e_ref in (e00_ref, e01_ref, e11_ref, e12_ref, e22_ref):
        sums.append(jnp.sum(factor_ref[...] * e_ref[...], axis=0, keepdims=True))
    lane = iota((1, LANES), 1)
    out = jnp.zeros((1, LANES), F32)
    for k, s in enumerate(sums):
        total = jnp.sum(jnp.where(own, s, 0.0), axis=1, keepdims=True)
        out = jnp.where(lane == k, total, out)
    moment_ref[...] = jnp.broadcast_to(out, moment_ref.shape)


def combine_kernel(
    moment_ref, v0_ref, v1_ref, v2_ref, e00_ref, e01_ref, e11_ref, e02_ref, e12_ref, e22_ref, density_ref,
    grad_ref, u_ref, nodes_ref,
):
    role, slab = where_am_i()
    parts, _, _, deep, fz = u_ref.shape
    half = fz // 2
    count = v0_ref.shape[0] // 3
    total = jnp.sum(moment_ref[...], axis=0, keepdims=True)
    lane = iota((1, LANES), 1)
    m = [jnp.sum(jnp.where(lane == k, total, 0.0), axis=1, keepdims=True) for k in range(6)]
    s = m[1] / m[0]
    inv = 1.0 / s
    mu = [jnp.ones_like(s)]
    power = 1.0 / m[0]
    for k in range(1, 6):
        power = power * inv
        mu.append(m[k] * power)
    nu = list(mu)
    for depth in range(1, 6):
        for k in range(5, depth - 1, -1):
            nu[k] = nu[k] - nu[k - 1]
    g = [nu[k] + nu[k + 1] for k in range(5)]
    l10 = g[1] / g[0]
    l20 = g[2] / g[0]
    d1 = g[2] - l10 * g[1]
    x12 = g[3] - l10 * g[2]
    r1 = nu[1] - l10 * nu[0]
    r2 = nu[2] - l20 * nu[0]
    l21 = x12 / d1
    d2 = (g[4] - l20 * g[2]) - l21 * x12
    c2 = (r2 - l21 * r1) / d2
    c1 = (r1 - x12 * c2) / d1
    c0 = (nu[0] - g[1] * c1 - g[2] * c2) / g[0]
    w0 = (c0 - c1 + c2) * inv
    w1 = (c1 - 2.0 * c2) * inv * inv
    w2 = c2 * inv * inv * inv
    energy = (
        w0 * (w0 * e00_ref[...] + 2.0 * (w1 * e01_ref[...] + w2 * e02_ref[...]))
        + w1 * (w1 * e11_ref[...] + 2.0 * w2 * e12_ref[...])
        + w2 * w2 * e22_ref[...]
    )
    density = density_ref[...]
    grad = (-3.0 * (1.0 - FLOOR_STIFF) / 32.0) * density * density * energy
    grad_ref[...] = jnp.where(element_lanes(grad.shape, role, half), grad, 0.0)
    nodes_ref[...] = w0 * v0_ref[0 : 2 * count] + w1 * v1_ref[0 : 2 * count] + w2 * v2_ref[0 : 2 * count]
    gi = iota((LANES, fz), 0)
    zi = iota((LANES, fz), 1)
    even_table = jnp.where(zi == 2 * gi, 1.0, 0.0).astype(BF16)
    odd_table = jnp.where(zi == 2 * gi + 1, 1.0, 0.0).astype(BF16)
    for a in range(2):
        for q in range(3):
            even = nodes_ref[pl.ds(a * count + q, parts * deep, stride=8), :]
            odd = nodes_ref[pl.ds(a * count + 4 + q, parts * deep, stride=8), :]
            x = pick_right(even, even_table) + pick_right(odd, odd_table)
            for j in range(parts):
                u_ref[j, q, a] = x[j * deep : (j + 1) * deep]


def last_kernel(grad_ref, ga_ref, gb_ref, sw_ref, out_ref, work_ref):
    planes, fy, fz = out_ref.shape
    width = 2 * fz
    role, slab = where_am_i()
    even = slab % 2 == 0
    rows = grad_ref.shape[0]
    pool_y = jnp.where(iota((fy, rows), 0) // 4 == iota((fy, rows), 1), 1.0, 0.0).astype(BF16)
    pool_z = jnp.where(iota((LANES, width), 1) // 2 == iota((LANES, width), 0), 1.0, 0.0).astype(BF16)
    a = ga_ref[...]
    b = gb_ref[...]
    low = jnp.where(even, b, a)
    high = jnp.where(even, a, b)
    for grad, first, last in ((low, 0, 2), (grad_ref[...], 2, 2 + planes), (high, 2 + planes, 4 + planes)):
        wide = pick_right(pick_left(pool_y, grad), pool_z)
        for p in range(first, last):
            work_ref[p] = wide * sw_ref[p]

    def body(p, _):
        x = work_ref[p] + work_ref[p + 4] + 2.0 * (work_ref[p + 1] + work_ref[p + 3]) + 3.0 * work_ref[p + 2]
        out_ref[p] = smooth_y(smooth_z(x))[:, :fz]
        return 0

    lax.fori_loop(0, planes, body, 0)


def shape(*dims, dtype=F32):
    return jax.ShapeDtypeStruct(dims, dtype)


def on_device(design, force, clamped_dof_mask, stiffness):
    planes, fy, fz = design.shape
    _, bx, by, _ = force.shape
    gx = lax.axis_size("gx")
    gy = lax.axis_size("gy")
    roles = lax.axis_size("role")
    devices = gx * gy * roles
    slabs = gx * gy
    assert roles == 2 and planes == 4 and fz == LANES and bx == 2 * gy and slabs % 2 == 0
    columns = fy // 4
    nodes = fy // 2
    tiles = nodes + 2
    count = tiles * 8
    pairs_a = [(i, i ^ 1) for i in range(slabs)]
    pairs_b = [(i, i + 1 if i % 2 else i - 1) for i in range(1, slabs - 1)]

    def beside(to_a, to_b):
        return lax.ppermute(to_a, LINE, pairs_a), lax.ppermute(to_b, LINE, pairs_b)

    plane0, strips, corner = pl.pallas_call(
        strip_rows_kernel,
        out_shape=(shape(6 * by, fz), shape(6 * bx, LANES), shape(8, LANES)),
        name="rows",
        compiler_params=KEEP,
    )(force, clamped_dof_mask)
    plane0, strips, corner, design = lax.optimization_barrier((plane0, strips, corner, design))
    next_plane = lax.ppermute(plane0, "gx", [(i + 1, i) for i in range(gx - 1)])
    strips = lax.ppermute(strips, "role", [(0, 1), (1, 0)])
    corner = lax.ppermute(
        corner, ("role", "gx"), [((1 - r) * gx + i + 1, r * gx + i) for r in range(2) for i in range(gx - 1)]
    )
    design_a, design_b = beside(design, design)
    pack, table = pl.pallas_call(
        pack_kernel,
        out_shape=(shape(gy, 18 * by + 24, fz), shape(2 * ROWS, 2 * ROWS, dtype=BF16)),
        name="pack",
        compiler_params=KEEP,
    )(force, clamped_dof_mask, next_plane, strips, corner, stiffness, jnp.asarray(place_table()))
    rf = lax.all_to_all(pack, "gy", 0, 0)

    role = lax.axis_index("role")

    def strip(x):
        return jnp.where(role == 0, x[..., fz - STRIP :], x[..., :STRIP]).reshape(-1, STRIP)

    fine_strips = jnp.concatenate([strip(design), strip(design_a), strip(design_b)], axis=0)
    fine_strips = lax.ppermute(fine_strips, "role", [(0, 1), (1, 0)])

    node_set = shape(3 * count, LANES)
    plane = shape(count, LANES)
    element = shape(columns, LANES)
    tile_scratch = [
        pltpu.VMEM((3, tiles, 16, LANES), BF16),
        pltpu.VMEM((2, tiles, 16, LANES), BF16),
        pltpu.VMEM((2, count, LANES), F32),
    ]
    shift32 = pltpu.VMEM((2, count, LANES), F32)
    sw, factor, density = pl.pallas_call(
        filter_kernel,
        out_shape=(shape(planes + 4, fy, 2 * fz), element, element),
        scratch_shapes=[pltpu.VMEM((3 * planes, fy, 2 * fz), F32), pltpu.VMEM((fy, 2 * fz), F32)],
        name="filter",
        compiler_params=KEEP,
        cost_estimate=pl.CostEstimate(flops=30_000_000, transcendentals=0, bytes_accessed=4_000_000),
    )(design, design_a, design_b, fine_strips)
    v0, free, local, to_a, to_b, e00 = pl.pallas_call(
        first_kernel,
        out_shape=(node_set, node_set, node_set, plane, plane, element),
        scratch_shapes=tile_scratch,
        name="first",
        compiler_params=KEEP,
    )(rf, factor, table)
    from_a, from_b = beside(to_a, to_b)
    v1, local, to_a, to_b, e01, e11 = pl.pallas_call(
        second_kernel,
        out_shape=(node_set, node_set, plane, plane, element, element),
        scratch_shapes=tile_scratch + [shift32],
        name="second",
        compiler_params=KEEP,
    )(v0, free, local, from_a, from_b, factor, table)
    from_a, from_b = beside(to_a, to_b)
    v2, e02, e12, e22, moments = pl.pallas_call(
        third_kernel,
        out_shape=(node_set, element, element, element, shape(devices, LANES)),
        scratch_shapes=tile_scratch + [shift32, shift32],
        name="third",
        compiler_params=KEEP,
    )(v0, v1, free, local, from_a, from_b, factor, table, e00, e01, e11)
    moments = lax.all_to_all(moments, ("role", "gx", "gy"), 0, 0, tiled=True)
    grad, u = pl.pallas_call(
        combine_kernel,
        out_shape=(element, shape(gy, 3, 2, by, fz)),
        scratch_shapes=[pltpu.VMEM((2 * count, LANES), F32)],
        name="combine",
        compiler_params=KEEP,
    )(moments, v0, v1, v2, e00, e01, e11, e02, e12, e22, density)
    grad_a, grad_b = beside(grad, grad)
    sensitivity = pl.pallas_call(
        last_kernel,
        out_shape=shape(planes, fy, fz),
        scratch_shapes=[pltpu.VMEM((planes + 4, fy, 2 * fz), F32)],
        name="last",
        compiler_params=KEEP,
    )(grad, grad_a, grad_b, sw)
    u = lax.all_to_all(u, "gy", 0, 0)
    displacement = jnp.transpose(u, (1, 0, 2, 3, 4)).reshape(3, bx, by, fz)
    return sensitivity, displacement


def solution(mesh):
    placed = (
        P(("gx", "gy"), None, "role"),
        P(None, "gx", "gy", "role"),
        P(None, "gx", "gy", "role"),
        P(),
    )
    return jax.shard_map(
        on_device,
        mesh=mesh,
        in_specs=placed,
        out_specs=(P(("gx", "gy"), None, "role"), P(None, "gx", "gy", "role")),
        check_vma=False,
    )
```

```python
import jax
import jax.numpy as jnp
import numpy as np
from jax import lax
from jax.experimental import pallas as pl
from jax.experimental.pallas import tpu as pltpu
from jax.sharding import PartitionSpec as P

SHARPNESS = 4.0
THRESHOLD = 0.5
FLOOR_STIFF = 0.001
TANH2 = float(np.tanh(2.0))
LANES = 128
HALO = 3
STRIP = 8
ROWS = 120
LINE = ("gx", "gy")
KEEP = pltpu.CompilerParams(vmem_limit_bytes=12 << 20)
F32 = jnp.float32
BF16 = jnp.bfloat16


def iota(shape, dim):
    return lax.broadcasted_iota(jnp.int32, shape, dim)


def place_table():
    table = np.zeros((ROWS, 81), np.float32)
    for c in range(3):
        for b in range(3):
            for a in range(3):
                for q in range(3):
                    dof = ((c * 3 + b) * 3 + a) * 3 + q
                    if c < 2:
                        row = 8 * (3 * a + b) + 4 * c + q
                    else:
                        row = 72 + 8 * (2 * b + (a == 2)) + 4 * (a == 1) + q
                    table[row, dof] = 1.0
    return table


def split2(x):
    hi = x.astype(BF16)
    return hi, (x - hi.astype(F32)).astype(BF16)


def split3(x):
    hi = x.astype(BF16)
    rest = x - hi.astype(F32)
    mid = rest.astype(BF16)
    return hi, mid, (rest - mid.astype(F32)).astype(BF16)


def dot(a, b):
    return jnp.dot(a, b, preferred_element_type=F32)


def pick_right(x, table):
    hi, mid, lo = split3(x)
    return (dot(hi, table) + dot(mid, table)) + dot(lo, table)


def pick_left(table, x):
    hi, mid, lo = split3(x)
    return (dot(table, hi) + dot(table, mid)) + dot(table, lo)


def where_am_i():
    role = lax.axis_index("role")
    slab = lax.axis_index("gx") * lax.axis_size("gy") + lax.axis_index("gy")
    return role, slab


def element_lanes(shape, role, half):
    lane = iota(shape, len(shape) - 1)
    above = jnp.logical_and(lane >= half, lane < half + HALO)
    below = lane >= LANES - HALO
    roles = lax.axis_size("role")
    return (lane < half) | (above & (role < roles - 1)) | (below & (role > 0))


def hat_count(place, extent):
    low = jnp.where(place == 0, 3.0, jnp.where(place == 1, 1.0, 0.0))
    high = jnp.where(place == extent - 1, 3.0, jnp.where(place == extent - 2, 1.0, 0.0))
    return 9.0 - low - high


def smooth_z(x):
    width = x.shape[1]
    for _ in range(2):
        x = x + pltpu.roll(x, 1, 1) + pltpu.roll(x, width - 1, 1)
    return x


def smooth_y(x):
    rows = x.shape[0]
    x = jnp.concatenate([x, jnp.zeros((8, x.shape[1]), F32)], axis=0)
    for _ in range(2):
        x = x + pltpu.roll(x, 1, 0) + pltpu.roll(x, rows + 7, 0)
    return x[:rows]


def strip_rows_kernel(force_ref, mask_ref, plane_ref, strip_ref, corner_ref):
    _, bx, by, fz = force_ref.shape
    role, _ = where_am_i()
    first = jnp.where(role == 0, fz - STRIP, 0)
    take = jnp.where(iota((fz, LANES), 0) == first + (iota((fz, LANES), 1) & (STRIP - 1)), 1.0, 0.0).astype(BF16)
    own_y = (iota((bx, by, LANES), 2) // STRIP) == iota((bx, by, LANES), 1)
    corner_ref[...] = jnp.zeros(corner_ref.shape, F32)
    for q in range(3):
        free = 1.0 - mask_ref[q].astype(F32)
        rhs = free * force_ref[q]
        plane_ref[q * by : (q + 1) * by] = rhs[0]
        plane_ref[(q + 3) * by : (q + 4) * by] = free[0]
        edge = pick_right(rhs.reshape(bx * by, fz), take), dot(free.reshape(bx * by, fz).astype(BF16), take)
        for row, x in ((q, edge[0]), (q + 3, edge[1])):
            x = jnp.sum(jnp.where(own_y, x.reshape(bx, by, LANES), 0.0), axis=1)
            strip_ref[row * bx : (row + 1) * bx] = x
            corner_ref[row : row + 1] = x[0:1]


def pack_kernel(force_ref, mask_ref, plane_ref, strip_ref, corner_ref, stiff_ref, place_ref, pack_ref, table_ref):
    _, bx, by, _ = force_ref.shape
    parts = pack_ref.shape[0]
    tail = 18 * by
    for j in range(parts):
        pack_ref[j, tail + 18 :] = jnp.zeros((pack_ref.shape[1] - tail - 18, LANES), F32)
    for q in range(3):
        free = 1.0 - mask_ref[q].astype(F32)
        rhs = free * force_ref[q]
        for row, val in ((q, rhs), (q + 3, free)):
            for j in range(parts):
                for a in range(3):
                    x = 2 * j + a
                    at = row * 3 + a
                    inner = x < bx
                    pack_ref[j, at * by : (at + 1) * by] = val[x] if inner else plane_ref[row * by : (row + 1) * by]
                    edge = strip_ref[row * bx + x : row * bx + x + 1] if inner else corner_ref[row : row + 1]
                    pack_ref[j, tail + at : tail + at + 1] = edge
    place = place_ref[...]
    half_way = jnp.dot(place, stiff_ref[...], precision=lax.Precision.HIGHEST, preferred_element_type=F32)
    spread = lax.dot_general(
        half_way, place, (((1,), (1,)), ((), ())), precision=lax.Precision.HIGHEST, preferred_element_type=F32
    )
    hi, lo = split2(spread)
    row = iota((ROWS, 2 * ROWS), 0)
    col = iota((ROWS, 2 * ROWS), 1)
    twice = jnp.where(row == 8 * (col // 16) + col % 8, 1.0, 0.0).astype(BF16)
    table_ref[:ROWS] = dot(hi, twice).astype(BF16)
    table_ref[ROWS:] = dot(lo, twice).astype(BF16)


def plane_rows(tiles):
    return tiles * 8


def shifted_tiles(nodes_ref, tiles, s):
    count = plane_rows(tiles)
    upper = (iota((count, LANES), 0) & 4) == 0
    if s == 0:
        first = nodes_ref[0:count]
        second = nodes_ref[count : 2 * count]
        x = jnp.where(upper, first, pltpu.roll(second, 4, 0))
    else:
        x = jnp.where(upper, nodes_ref[2 * count : 3 * count], 0.0)
    return pltpu.roll(x, LANES - 1, 1)


def pair_tiles(x):
    tiles = x.shape[0] // 8
    hi = x.astype(BF16).astype(F32)
    lo = x - hi
    both = jnp.concatenate([hi.reshape(tiles, 8, LANES), lo.reshape(tiles, 8, LANES)], axis=1)
    return both.astype(BF16)


def make_tiles(nodes_ref, main_ref, shift_ref, shift32_ref):
    tiles = main_ref.shape[1]
    count = plane_rows(tiles)
    for a in range(3):
        main_ref[a] = pair_tiles(nodes_ref[a * count : (a + 1) * count])
    for s in range(2):
        x = shifted_tiles(nodes_ref, tiles, s)
        if shift32_ref is not None:
            shift32_ref[s] = x
        shift_ref[s] = pair_tiles(x)


def sweep(table_ref, main_ref, shift_ref, factor_ref, out_ref, energies):
    tiles = main_ref.shape[1]
    columns = factor_ref.shape[0]
    upper = iota((8, LANES), 0) < 4

    def finish(node, parts):
        t0, t1, t2, s0, s1 = parts
        r0 = pltpu.roll(s0, 1, 1)
        r1 = pltpu.roll(s1, 1, 1)
        done = (
            t0 + jnp.where(upper, r0, 0.0),
            t1 + jnp.where(upper, pltpu.roll(r0, 4, 0), 0.0),
            t2 + jnp.where(upper, r1, 0.0),
        )
        for a in range(3):
            out_ref[pl.ds(pl.multiple_of((a * tiles + node) * 8, 8), 8), :] = done[a]

    def body(i, carry):
        cols = []
        for k in range(2):
            base = 4 * i + 2 * k
            pieces = [main_ref[a, base + b] for a in range(3) for b in range(3)]
            pieces += [shift_ref[s, base + b] for b in range(3) for s in range(2)]
            cols.append(jnp.concatenate(pieces, axis=0))
        product = dot(table_ref[...], jnp.concatenate(cols, axis=1))
        product = product[:ROWS] + product[ROWS:]
        parts = []
        for k in range(2):
            y = product[:, k * LANES : (k + 1) * LANES]
            base = 4 * i + 2 * k
            for nodes_ref, shift32_ref, e_ref in energies:
                total = None
                for a in range(3):
                    for b in range(3):
                        at = pl.multiple_of((a * tiles + base + b) * 8, 8)
                        term = nodes_ref[pl.ds(at, 8), :] * y[8 * (3 * a + b) : 8 * (3 * a + b) + 8]
                        total = term if total is None else total + term
                for b in range(3):
                    for s in range(2):
                        at = pl.multiple_of((base + b) * 8, 8)
                        lo = 72 + 8 * (2 * b + s)
                        total = total + shift32_ref[s, pl.ds(at, 8), :] * y[lo : lo + 8]
                e_ref[pl.ds(2 * i + k, 1), :] = jnp.sum(total, axis=0, keepdims=True)
            if out_ref is not None:
                z = y * factor_ref[pl.ds(2 * i + k, 1), :]
                parts.append(
                    [
                        [z[8 * (3 * a + b) : 8 * (3 * a + b) + 8] for a in range(3)]
                        + [z[72 + 8 * (2 * b + s) : 80 + 8 * (2 * b + s)] for s in range(2)]
                        for b in range(3)
                    ]
                )
        if out_ref is None:
            return carry
        left, right = parts
        finish(4 * i, [c + v for c, v in zip(carry, left[0])])
        finish(4 * i + 1, left[1])
        finish(4 * i + 2, [c + v for c, v in zip(left[2], right[0])])
        finish(4 * i + 3, right[1])
        return tuple(right[2])

    if out_ref is None:
        lax.fori_loop(0, columns // 2, lambda i, c: body(i, c), 0, unroll=min(16, columns // 2))
    else:
        zero = jnp.zeros((8, LANES), F32)
        lax.fori_loop(0, columns // 2, body, (zero,) * 5, unroll=min(16, columns // 2))
        for a in range(3):
            for node in range(2 * columns, tiles):
                at = (a * tiles + node) * 8
                out_ref[at : at + 8, :] = zero


def send_planes(local_ref, tiles, slab, to_a, to_b):
    count = plane_rows(tiles)
    low = local_ref[0:count]
    high = local_ref[2 * count : 3 * count]
    even = slab % 2 == 0
    to_a[...] = jnp.where(even, high, low)
    to_b[...] = jnp.where(even, low, high)


def gather_nodes(local_ref, from_a, from_b, free_ref, tiles, slab, nodes_ref):
    count = plane_rows(tiles)
    even = slab % 2 == 0
    a = from_a[...]
    b = from_b[...]
    nodes_ref[0:count] = free_ref[0:count] * (local_ref[0:count] + jnp.where(even, b, a))
    nodes_ref[count : 2 * count] = free_ref[count : 2 * count] * local_ref[count : 2 * count]
    nodes_ref[2 * count :] = free_ref[2 * count :] * (local_ref[2 * count :] + jnp.where(even, a, b))


def filter_kernel(design_ref, da_ref, db_ref, strip_ref, sw_ref, factor_ref, density_ref, fine_ref, sum_ref):
    planes, fy, fz = design_ref.shape
    role, slab = where_am_i()
    slabs = lax.axis_size("gx") * lax.axis_size("gy")
    roles = lax.axis_size("role")
    half = fz // 2
    even = slab % 2 == 0

    at_lane = jnp.where(role == 0, 0, LANES - STRIP)
    put = jnp.where(iota((STRIP, LANES), 1) == iota((STRIP, LANES), 0) + at_lane, 1.0, 0.0).astype(BF16)
    for p in range(planes):
        a = da_ref[p]
        b = db_ref[p]
        fine_ref[p, :, :fz] = jnp.where(even, b, a)
        fine_ref[planes + p, :, :fz] = design_ref[p]
        fine_ref[2 * planes + p, :, :fz] = jnp.where(even, a, b)
    for p in range(planes):
        own = pick_right(strip_ref[p * fy : (p + 1) * fy], put)
        a = pick_right(strip_ref[(planes + p) * fy : (planes + p + 1) * fy], put)
        b = pick_right(strip_ref[(2 * planes + p) * fy : (2 * planes + p + 1) * fy], put)
        fine_ref[p, :, fz:] = jnp.where(even, b, a)
        fine_ref[planes + p, :, fz:] = own
        fine_ref[2 * planes + p, :, fz:] = jnp.where(even, a, b)

    width = 2 * fz
    lane = iota((1, width), 1)
    z_place = role * fz + jnp.where(lane < fz + fz // 2, lane, lane - width)
    inv_z = 1.0 / hat_count(z_place, roles * fz)
    inv_y = 1.0 / hat_count(iota((fy, 1), 0), fy)
    inv_yz = inv_y * inv_z
    sum_ref[...] = jnp.zeros((fy, width), F32)

    def filter_plane(p, _):
        x = fine_ref[p] + fine_ref[p + 4] + 2.0 * (fine_ref[p + 1] + fine_ref[p + 3]) + 3.0 * fine_ref[p + 2]
        x = smooth_y(smooth_z(x))
        place = jnp.full((1, 1), slab * planes + p - 2, jnp.int32)
        inv = inv_yz * (1.0 / hat_count(place, slabs * planes))
        bent = jnp.tanh(SHARPNESS * (x * inv - THRESHOLD))
        sw_ref[p] = (SHARPNESS / (2.0 * TANH2)) * (1.0 - bent * bent) * inv
        mine = jnp.logical_and(p >= 2, p < 2 + planes)
        sum_ref[...] += jnp.where(mine, (TANH2 + bent) * (1.0 / (2.0 * TANH2)), 0.0)
        return 0

    lax.fori_loop(0, planes + 4, filter_plane, 0)

    rows = factor_ref.shape[0]
    pool_y = jnp.where(iota((rows, fy), 1) // 4 == iota((rows, fy), 0), 1.0, 0.0).astype(BF16)
    pool_z = jnp.where(iota((width, LANES), 0) // 2 == iota((width, LANES), 1), 1.0, 0.0).astype(BF16)
    density = pick_right(pick_left(pool_y, sum_ref[...]), pool_z) * (1.0 / 32.0)
    inside = element_lanes((rows, LANES), role, half)
    density = jnp.where(inside, density, 0.0)
    density_ref[...] = density
    factor_ref[...] = jnp.where(inside, FLOOR_STIFF + (1.0 - FLOOR_STIFF) * density * density * density, 0.0)


def first_kernel(
    rf_ref, factor_ref, table_ref,
    nodes_ref, free_ref, local_ref, to_a, to_b, e00_ref,
    main_ref, shift_ref, shift32_ref,
):
    tiles = main_ref.shape[1]
    count = plane_rows(tiles)
    role, slab = where_am_i()
    half = LANES // 2
    parts = rf_ref.shape[0]
    deep = (2 * factor_ref.shape[0]) // parts
    tail = 18 * deep

    nodes_ref[...] = jnp.zeros(nodes_ref.shape, F32)
    free_ref[...] = jnp.zeros(free_ref.shape, F32)
    zi = iota((2 * LANES, 2 * LANES), 0)
    ci = iota((2 * LANES, 2 * LANES), 1)
    lane_of = ci & (LANES - 1)
    odd = ci // LANES
    first_lane = jnp.where(role == 0, half, LANES - STRIP // 2)
    own = zi == 2 * lane_of + odd
    edge = (zi & (STRIP - 1)) == 2 * (lane_of - first_lane) + odd
    table = jnp.where(zi < LANES, jnp.where(own, 1.0, 0.0), jnp.where(edge, 1.0, 0.0)).astype(BF16)
    own_y = (iota((deep, LANES), 1) // STRIP) == iota((deep, LANES), 0)
    for row in range(6):
        for a in range(3):
            at = row * 3 + a
            x = jnp.concatenate([rf_ref[j, at * deep : (at + 1) * deep] for j in range(parts)], axis=0)
            st = jnp.concatenate(
                [jnp.where(own_y, rf_ref[j, tail + at : tail + at + 1], 0.0) for j in range(parts)], axis=0
            )
            x = jnp.concatenate([x, st], axis=1)
            if row < 3:
                y = pick_right(x, table)
                dest = nodes_ref
            else:
                y = dot(x.astype(BF16), table)
                dest = free_ref
            q = row % 3
            dest[pl.ds(a * count + q, parts * deep, stride=8), :] = y[:, :LANES]
            dest[pl.ds(a * count + 4 + q, parts * deep, stride=8), :] = y[:, LANES:]

    make_tiles(nodes_ref, main_ref, shift_ref, shift32_ref)
    sweep(table_ref, main_ref, shift_ref, factor_ref, local_ref, [(nodes_ref, shift32_ref, e00_ref)])
    send_planes(local_ref, tiles, slab, to_a, to_b)


def second_kernel(
    prev_ref, free_ref, last_ref, from_a, from_b, factor_ref, table_ref,
    nodes_ref, local_ref, to_a, to_b, e01_ref, e11_ref,
    main_ref, shift_ref, shift32_ref, prev32_ref,
):
    tiles = main_ref.shape[1]
    role, slab = where_am_i()
    gather_nodes(last_ref, from_a, from_b, free_ref, tiles, slab, nodes_ref)
    for s in range(2):
        prev32_ref[s] = shifted_tiles(prev_ref, tiles, s)
    make_tiles(nodes_ref, main_ref, shift_ref, shift32_ref)
    sweep(
        table_ref, main_ref, shift_ref, factor_ref, local_ref,
        [(prev_ref, prev32_ref, e01_ref), (nodes_ref, shift32_ref, e11_ref)],
    )
    send_planes(local_ref, tiles, slab, to_a, to_b)


def third_kernel(
    v0_ref, v1_ref, free_ref, last_ref, from_a, from_b, factor_ref, table_ref, e00_ref, e01_ref, e11_ref,
    nodes_ref, e02_ref, e12_ref, e22_ref, moment_ref,
    main_ref, shift_ref, shift32_ref, s0_ref, s1_ref,
):
    tiles = main_ref.shape[1]
    count = plane_rows(tiles)
    role, slab = where_am_i()
    gather_nodes(last_ref, from_a, from_b, free_ref, tiles, slab, nodes_ref)
    for s in range(2):
        s0_ref[s] = shifted_tiles(v0_ref, tiles, s)
        s1_ref[s] = shifted_tiles(v1_ref, tiles, s)
    make_tiles(nodes_ref, main_ref, shift_ref, shift32_ref)
    sweep(
        table_ref, main_ref, shift_ref, factor_ref, None,
        [(v0_ref, s0_ref, e02_ref), (v1_ref, s1_ref, e12_ref), (nodes_ref, shift32_ref, e22_ref)],
    )
    half = LANES // 2
    own = iota((1, LANES), 1) < half
    v0 = v0_ref[0 : 2 * count]
    sums = [jnp.sum(v0 * v0, axis=0, keepdims=True)]
    for e_ref in (e00_ref, e01_ref, e11_ref, e12_ref, e22_ref):
        sums.append(jnp.sum(factor_ref[...] * e_ref[...], axis=0, keepdims=True))
    lane = iota((1, LANES), 1)
    out = jnp.zeros((1, LANES), F32)
    for k, s in enumerate(sums):
        total = jnp.sum(jnp.where(own, s, 0.0), axis=1, keepdims=True)
        out = jnp.where(lane == k, total, out)
    moment_ref[...] = jnp.broadcast_to(out, moment_ref.shape)


def combine_kernel(
    moment_ref, v0_ref, v1_ref, v2_ref, e00_ref, e01_ref, e11_ref, e02_ref, e12_ref, e22_ref, density_ref,
    grad_ref, u_ref, nodes_ref,
):
    role, slab = where_am_i()
    parts, _, _, deep, fz = u_ref.shape
    half = fz // 2
    count = v0_ref.shape[0] // 3
    total = jnp.sum(moment_ref[...], axis=0, keepdims=True)
    lane = iota((1, LANES), 1)
    m = [jnp.sum(jnp.where(lane == k, total, 0.0), axis=1, keepdims=True) for k in range(6)]
    s = m[1] / m[0]
    inv = 1.0 / s
    mu = [jnp.ones_like(s)]
    power = 1.0 / m[0]
    for k in range(1, 6):
        power = power * inv
        mu.append(m[k] * power)
    nu = list(mu)
    for depth in range(1, 6):
        for k in range(5, depth - 1, -1):
            nu[k] = nu[k] - nu[k - 1]
    g = [nu[k] + nu[k + 1] for k in range(5)]
    l10 = g[1] / g[0]
    l20 = g[2] / g[0]
    d1 = g[2] - l10 * g[1]
    x12 = g[3] - l10 * g[2]
    r1 = nu[1] - l10 * nu[0]
    r2 = nu[2] - l20 * nu[0]
    l21 = x12 / d1
    d2 = (g[4] - l20 * g[2]) - l21 * x12
    c2 = (r2 - l21 * r1) / d2
    c1 = (r1 - x12 * c2) / d1
    c0 = (nu[0] - g[1] * c1 - g[2] * c2) / g[0]
    w0 = (c0 - c1 + c2) * inv
    w1 = (c1 - 2.0 * c2) * inv * inv
    w2 = c2 * inv * inv * inv
    energy = (
        w0 * (w0 * e00_ref[...] + 2.0 * (w1 * e01_ref[...] + w2 * e02_ref[...]))
        + w1 * (w1 * e11_ref[...] + 2.0 * w2 * e12_ref[...])
        + w2 * w2 * e22_ref[...]
    )
    density = density_ref[...]
    grad = (-3.0 * (1.0 - FLOOR_STIFF) / 32.0) * density * density * energy
    grad_ref[...] = jnp.where(element_lanes(grad.shape, role, half), grad, 0.0)
    nodes_ref[...] = w0 * v0_ref[0 : 2 * count] + w1 * v1_ref[0 : 2 * count] + w2 * v2_ref[0 : 2 * count]
    gi = iota((LANES, fz), 0)
    zi = iota((LANES, fz), 1)
    even_table = jnp.where(zi == 2 * gi, 1.0, 0.0).astype(BF16)
    odd_table = jnp.where(zi == 2 * gi + 1, 1.0, 0.0).astype(BF16)
    for a in range(2):
        for q in range(3):
            even = nodes_ref[pl.ds(a * count + q, parts * deep, stride=8), :]
            odd = nodes_ref[pl.ds(a * count + 4 + q, parts * deep, stride=8), :]
            x = pick_right(even, even_table) + pick_right(odd, odd_table)
            for j in range(parts):
                u_ref[j, q, a] = x[j * deep : (j + 1) * deep]


def last_kernel(grad_ref, ga_ref, gb_ref, sw_ref, out_ref, work_ref):
    planes, fy, fz = out_ref.shape
    width = 2 * fz
    role, slab = where_am_i()
    even = slab % 2 == 0
    rows = grad_ref.shape[0]
    pool_y = jnp.where(iota((fy, rows), 0) // 4 == iota((fy, rows), 1), 1.0, 0.0).astype(BF16)
    pool_z = jnp.where(iota((LANES, width), 1) // 2 == iota((LANES, width), 0), 1.0, 0.0).astype(BF16)
    a = ga_ref[...]
    b = gb_ref[...]
    low = jnp.where(even, b, a)
    high = jnp.where(even, a, b)
    for grad, first, last in ((low, 0, 2), (grad_ref[...], 2, 2 + planes), (high, 2 + planes, 4 + planes)):
        wide = pick_right(pick_left(pool_y, grad), pool_z)
        for p in range(first, last):
            work_ref[p] = wide * sw_ref[p]

    def body(p, _):
        x = work_ref[p] + work_ref[p + 4] + 2.0 * (work_ref[p + 1] + work_ref[p + 3]) + 3.0 * work_ref[p + 2]
        out_ref[p] = smooth_y(smooth_z(x))[:, :fz]
        return 0

    lax.fori_loop(0, planes, body, 0)


def shape(*dims, dtype=F32):
    return jax.ShapeDtypeStruct(dims, dtype)


def on_device(design, force, clamped_dof_mask, stiffness):
    planes, fy, fz = design.shape
    _, bx, by, _ = force.shape
    gx = lax.axis_size("gx")
    gy = lax.axis_size("gy")
    roles = lax.axis_size("role")
    devices = gx * gy * roles
    slabs = gx * gy
    assert roles == 2 and planes == 4 and fz == LANES and bx == 2 * gy and slabs % 2 == 0
    columns = fy // 4
    nodes = fy // 2
    tiles = nodes + 2
    count = tiles * 8
    pairs_a = [(i, i ^ 1) for i in range(slabs)]
    pairs_b = [(i, i + 1 if i % 2 else i - 1) for i in range(1, slabs - 1)]

    def beside(to_a, to_b):
        return lax.ppermute(to_a, LINE, pairs_a), lax.ppermute(to_b, LINE, pairs_b)

    plane0, strips, corner = pl.pallas_call(
        strip_rows_kernel,
        out_shape=(shape(6 * by, fz), shape(6 * bx, LANES), shape(8, LANES)),
        name="rows",
        compiler_params=KEEP,
    )(force, clamped_dof_mask)
    plane0, strips, corner, design = lax.optimization_barrier((plane0, strips, corner, design))
    next_plane = lax.ppermute(plane0, "gx", [(i + 1, i) for i in range(gx - 1)])
    strips = lax.ppermute(strips, "role", [(0, 1), (1, 0)])
    corner = lax.ppermute(
        corner, ("role", "gx"), [((1 - r) * gx + i + 1, r * gx + i) for r in range(2) for i in range(gx - 1)]
    )
    design_a, design_b = beside(design, design)
    pack, table = pl.pallas_call(
        pack_kernel,
        out_shape=(shape(gy, 18 * by + 24, fz), shape(2 * ROWS, 2 * ROWS, dtype=BF16)),
        name="pack",
        compiler_params=KEEP,
    )(force, clamped_dof_mask, next_plane, strips, corner, stiffness, jnp.asarray(place_table()))
    rf = lax.all_to_all(pack, "gy", 0, 0)

    role = lax.axis_index("role")

    def strip(x):
        return jnp.where(role == 0, x[..., fz - STRIP :], x[..., :STRIP]).reshape(-1, STRIP)

    fine_strips = jnp.concatenate([strip(design), strip(design_a), strip(design_b)], axis=0)
    fine_strips = lax.ppermute(fine_strips, "role", [(0, 1), (1, 0)])

    node_set = shape(3 * count, LANES)
    plane = shape(count, LANES)
    element = shape(columns, LANES)
    tile_scratch = [
        pltpu.VMEM((3, tiles, 16, LANES), BF16),
        pltpu.VMEM((2, tiles, 16, LANES), BF16),
        pltpu.VMEM((2, count, LANES), F32),
    ]
    shift32 = pltpu.VMEM((2, count, LANES), F32)
    sw, factor, density = pl.pallas_call(
        filter_kernel,
        out_shape=(shape(planes + 4, fy, 2 * fz), element, element),
        scratch_shapes=[pltpu.VMEM((3 * planes, fy, 2 * fz), F32), pltpu.VMEM((fy, 2 * fz), F32)],
        name="filter",
        compiler_params=KEEP,
        cost_estimate=pl.CostEstimate(flops=30_000_000, transcendentals=0, bytes_accessed=4_000_000),
    )(design, design_a, design_b, fine_strips)
    v0, free, local, to_a, to_b, e00 = pl.pallas_call(
        first_kernel,
        out_shape=(node_set, node_set, node_set, plane, plane, element),
        scratch_shapes=tile_scratch,
        name="first",
        compiler_params=KEEP,
    )(rf, factor, table)
    from_a, from_b = beside(to_a, to_b)
    v1, local, to_a, to_b, e01, e11 = pl.pallas_call(
        second_kernel,
        out_shape=(node_set, node_set, plane, plane, element, element),
        scratch_shapes=tile_scratch + [shift32],
        name="second",
        compiler_params=KEEP,
    )(v0, free, local, from_a, from_b, factor, table)
    from_a, from_b = beside(to_a, to_b)
    v2, e02, e12, e22, moments = pl.pallas_call(
        third_kernel,
        out_shape=(node_set, element, element, element, shape(devices, LANES)),
        scratch_shapes=tile_scratch + [shift32, shift32],
        name="third",
        compiler_params=KEEP,
    )(v0, v1, free, local, from_a, from_b, factor, table, e00, e01, e11)
    moments = lax.all_to_all(moments, ("role", "gx", "gy"), 0, 0, tiled=True)
    grad, u = pl.pallas_call(
        combine_kernel,
        out_shape=(element, shape(gy, 3, 2, by, fz)),
        scratch_shapes=[pltpu.VMEM((2 * count, LANES), F32)],
        name="combine",
        compiler_params=KEEP,
    )(moments, v0, v1, v2, e00, e01, e11, e02, e12, e22, density)
    grad_a, grad_b = beside(grad, grad)
    sensitivity = pl.pallas_call(
        last_kernel,
        out_shape=shape(planes, fy, fz),
        scratch_shapes=[pltpu.VMEM((planes + 4, fy, 2 * fz), F32)],
        name="last",
        compiler_params=KEEP,
    )(grad, grad_a, grad_b, sw)
    u = lax.all_to_all(u, "gy", 0, 0)
    displacement = jnp.transpose(u, (1, 0, 2, 3, 4)).reshape(3, bx, by, fz)
    return sensitivity, displacement


def solution(mesh):
    placed = (
        P(("gx", "gy"), None, "role"),
        P(None, "gx", "gy", "role"),
        P(None, "gx", "gy", "role"),
        P(),
    )
    return jax.shard_map(
        on_device,
        mesh=mesh,
        in_specs=placed,
        out_specs=(P(("gx", "gy"), None, "role"), P(None, "gx", "gy", "role")),
        check_vma=False,
    )
```

```python
import jax
import jax.numpy as jnp
import numpy as np
from jax import lax
from jax.experimental import pallas as pl
from jax.experimental.pallas import tpu as pltpu
from jax.sharding import PartitionSpec as P


SHARPNESS = 4.0
THRESHOLD = 0.5
FLOOR_STIFF = 0.001
TANH2 = float(np.tanh(2.0))
LANES = 128
HALO = 3
STRIP = 8
ROWS = 120
LINE = ("gx", "gy")
KEEP = pltpu.CompilerParams(vmem_limit_bytes=12 << 20)
F32 = jnp.float32
BF16 = jnp.bfloat16


def iota(shape, dim):
    return lax.broadcasted_iota(jnp.int32, shape, dim)


def place_table():
    table = np.zeros((ROWS, 81), np.float32)
    for c in range(3):
        for b in range(3):
            for a in range(3):
                for q in range(3):
                    dof = ((c * 3 + b) * 3 + a) * 3 + q
                    if c < 2:
                        row = 8 * (3 * a + b) + 4 * c + q
                    else:
                        row = 72 + 8 * (2 * b + (a == 2)) + 4 * (a == 1) + q
                    table[row, dof] = 1.0
    return table


def split2(x):
    hi = x.astype(BF16)
    return hi, (x - hi.astype(F32)).astype(BF16)


def split3(x):
    hi = x.astype(BF16)
    rest = x - hi.astype(F32)
    mid = rest.astype(BF16)
    return hi, mid, (rest - mid.astype(F32)).astype(BF16)


def dot(a, b):
    return jnp.dot(a, b, preferred_element_type=F32)


def pick_right(x, table):
    hi, mid, lo = split3(x)
    return (dot(hi, table) + dot(mid, table)) + dot(lo, table)


def pick_left(table, x):
    hi, mid, lo = split3(x)
    return (dot(table, hi) + dot(table, mid)) + dot(table, lo)


def where_am_i():
    role = lax.axis_index("role")
    slab = lax.axis_index("gx") * lax.axis_size("gy") + lax.axis_index("gy")
    return role, slab


def element_lanes(shape, role, half):
    lane = iota(shape, len(shape) - 1)
    above = jnp.logical_and(lane >= half, lane < half + HALO)
    below = lane >= LANES - HALO
    roles = lax.axis_size("role")
    return (lane < half) | (above & (role < roles - 1)) | (below & (role > 0))


def hat_count(place, extent):
    low = jnp.where(place == 0, 3.0, jnp.where(place == 1, 1.0, 0.0))
    high = jnp.where(place == extent - 1, 3.0, jnp.where(place == extent - 2, 1.0, 0.0))
    return 9.0 - low - high


def smooth_z(x):
    width = x.shape[1]
    for _ in range(2):
        x = x + pltpu.roll(x, 1, 1) + pltpu.roll(x, width - 1, 1)
    return x


def smooth_y(x):
    rows = x.shape[0]
    x = jnp.concatenate([x, jnp.zeros((8, x.shape[1]), F32)], axis=0)
    for _ in range(2):
        x = x + pltpu.roll(x, 1, 0) + pltpu.roll(x, rows + 7, 0)
    return x[:rows]


def strip_rows_kernel(force_hbm, mask_hbm, plane_ref, strip_ref, corner_ref, force_ref, mask_ref, sems):
    copies = (
        pltpu.make_async_copy(force_hbm, force_ref, sems.at[0]),
        pltpu.make_async_copy(mask_hbm, mask_ref, sems.at[1]),
    )
    for copy in copies:
        copy.start()
    for copy in copies:
        copy.wait()
    _, bx, by, fz = force_ref.shape
    role, _ = where_am_i()
    first = jnp.where(role == 0, fz - STRIP, 0)
    take = jnp.where(iota((fz, LANES), 0) == first + (iota((fz, LANES), 1) & (STRIP - 1)), 1.0, 0.0).astype(BF16)
    own_y = (iota((bx, by, LANES), 2) // STRIP) == iota((bx, by, LANES), 1)
    corner_ref[...] = jnp.zeros(corner_ref.shape, F32)
    for q in range(3):
        free = 1.0 - mask_ref[q].astype(F32)
        rhs = free * force_ref[q]
        plane_ref[q * by : (q + 1) * by] = rhs[0]
        plane_ref[(q + 3) * by : (q + 4) * by] = free[0]
        edge = pick_right(rhs.reshape(bx * by, fz), take), dot(free.reshape(bx * by, fz).astype(BF16), take)
        for row, x in ((q, edge[0]), (q + 3, edge[1])):
            x = jnp.sum(jnp.where(own_y, x.reshape(bx, by, LANES), 0.0), axis=1)
            strip_ref[row * bx : (row + 1) * bx] = x
            corner_ref[row : row + 1] = x[0:1]


def pack_kernel(force_ref, mask_ref, plane_ref, strip_ref, corner_ref, stiff_ref, place_ref, pack_ref, table_ref):
    _, bx, by, _ = force_ref.shape
    parts = pack_ref.shape[0]
    tail = 18 * by
    for j in range(parts):
        pack_ref[j, tail + 18 :] = jnp.zeros((pack_ref.shape[1] - tail - 18, LANES), F32)
    for q in range(3):
        free = 1.0 - mask_ref[q].astype(F32)
        rhs = free * force_ref[q]
        for row, val in ((q, rhs), (q + 3, free)):
            for j in range(parts):
                for a in range(3):
                    x = 2 * j + a
                    at = row * 3 + a
                    inner = x < bx
                    pack_ref[j, at * by : (at + 1) * by] = val[x] if inner else plane_ref[row * by : (row + 1) * by]
                    edge = strip_ref[row * bx + x : row * bx + x + 1] if inner else corner_ref[row : row + 1]
                    pack_ref[j, tail + at : tail + at + 1] = edge
    place = place_ref[...]
    half_way = jnp.dot(place, stiff_ref[...], precision=lax.Precision.HIGHEST, preferred_element_type=F32)
    spread = lax.dot_general(
        half_way, place, (((1,), (1,)), ((), ())), precision=lax.Precision.HIGHEST, preferred_element_type=F32
    )
    hi, lo = split2(spread)
    row = iota((ROWS, 2 * ROWS), 0)
    col = iota((ROWS, 2 * ROWS), 1)
    twice = jnp.where(row == 8 * (col // 16) + col % 8, 1.0, 0.0).astype(BF16)
    table_ref[:ROWS] = dot(hi, twice).astype(BF16)
    table_ref[ROWS:] = dot(lo, twice).astype(BF16)


def plane_rows(tiles):
    return tiles * 8


def shifted_tiles(nodes_ref, tiles, s):
    count = plane_rows(tiles)
    upper = (iota((count, LANES), 0) & 4) == 0
    if s == 0:
        first = nodes_ref[0:count]
        second = nodes_ref[count : 2 * count]
        x = jnp.where(upper, first, pltpu.roll(second, 4, 0))
    else:
        x = jnp.where(upper, nodes_ref[2 * count : 3 * count], 0.0)
    return pltpu.roll(x, LANES - 1, 1)


def pair_tiles(x):
    tiles = x.shape[0] // 8
    hi = x.astype(BF16).astype(F32)
    lo = x - hi
    both = jnp.concatenate([hi.reshape(tiles, 8, LANES), lo.reshape(tiles, 8, LANES)], axis=1)
    return both.astype(BF16)


def make_tiles(nodes_ref, main_ref, shift_ref, shift32_ref):
    tiles = main_ref.shape[1]
    count = plane_rows(tiles)
    for a in range(3):
        main_ref[a] = pair_tiles(nodes_ref[a * count : (a + 1) * count])
    for s in range(2):
        x = shifted_tiles(nodes_ref, tiles, s)
        if shift32_ref is not None:
            shift32_ref[s] = x
        shift_ref[s] = pair_tiles(x)


def sweep(table_ref, main_ref, shift_ref, factor_ref, out_ref, energies):
    tiles = main_ref.shape[1]
    columns = factor_ref.shape[0]
    upper = iota((8, LANES), 0) < 4

    def finish(node, parts):
        t0, t1, t2, s0, s1 = parts
        r0 = pltpu.roll(s0, 1, 1)
        r1 = pltpu.roll(s1, 1, 1)
        done = (
            t0 + jnp.where(upper, r0, 0.0),
            t1 + jnp.where(upper, pltpu.roll(r0, 4, 0), 0.0),
            t2 + jnp.where(upper, r1, 0.0),
        )
        for a in range(3):
            out_ref[pl.ds(pl.multiple_of((a * tiles + node) * 8, 8), 8), :] = done[a]

    def body(i, carry):
        cols = []
        for k in range(2):
            base = 4 * i + 2 * k
            pieces = [main_ref[a, base + b] for a in range(3) for b in range(3)]
            pieces += [shift_ref[s, base + b] for b in range(3) for s in range(2)]
            cols.append(jnp.concatenate(pieces, axis=0))
        product = dot(table_ref[...], jnp.concatenate(cols, axis=1))
        product = product[:ROWS] + product[ROWS:]
        parts = []
        for k in range(2):
            y = product[:, k * LANES : (k + 1) * LANES]
            base = 4 * i + 2 * k
            for nodes_ref, shift32_ref, e_ref in energies:
                total = None
                for a in range(3):
                    for b in range(3):
                        at = pl.multiple_of((a * tiles + base + b) * 8, 8)
                        term = nodes_ref[pl.ds(at, 8), :] * y[8 * (3 * a + b) : 8 * (3 * a + b) + 8]
                        total = term if total is None else total + term
                for b in range(3):
                    for s in range(2):
                        at = pl.multiple_of((base + b) * 8, 8)
                        lo = 72 + 8 * (2 * b + s)
                        total = total + shift32_ref[s, pl.ds(at, 8), :] * y[lo : lo + 8]
                e_ref[pl.ds(2 * i + k, 1), :] = jnp.sum(total, axis=0, keepdims=True)
            if out_ref is not None:
                z = y * factor_ref[pl.ds(2 * i + k, 1), :]
                parts.append(
                    [
                        [z[8 * (3 * a + b) : 8 * (3 * a + b) + 8] for a in range(3)]
                        + [z[72 + 8 * (2 * b + s) : 80 + 8 * (2 * b + s)] for s in range(2)]
                        for b in range(3)
                    ]
                )
        if out_ref is None:
            return carry
        left, right = parts
        finish(4 * i, [c + v for c, v in zip(carry, left[0])])
        finish(4 * i + 1, left[1])
        finish(4 * i + 2, [c + v for c, v in zip(left[2], right[0])])
        finish(4 * i + 3, right[1])
        return tuple(right[2])

    if out_ref is None:
        lax.fori_loop(0, columns // 2, lambda i, c: body(i, c), 0, unroll=min(16, columns // 2))
    else:
        zero = jnp.zeros((8, LANES), F32)
        lax.fori_loop(0, columns // 2, body, (zero,) * 5, unroll=min(16, columns // 2))
        for a in range(3):
            for node in range(2 * columns, tiles):
                at = (a * tiles + node) * 8
                out_ref[at : at + 8, :] = zero


def pack_pair(x, y):
    lane = iota((8, LANES), 1)
    row = iota((8, LANES), 0)
    half = LANES // 2
    even = jnp.where(row < 4, x, pltpu.roll(y, 4, 0))
    odd = jnp.where(row < 4, pltpu.roll(x, 4, 0), y)
    main = jnp.where(lane < half, even, pltpu.roll(odd, half, 1))
    edge = jnp.zeros((8, LANES), F32)
    for tile, first in ((x, 0), (y, 28)):
        moved = pltpu.roll(tile, half + first, 1, stride=4, stride_axis=0)
        at = lane - first - 4 * row
        edge = jnp.where(((at >= 0) & (at < 4)) | ((at >= 60) & (at < 64)), moved, edge)
    for shift in (4, 2, 1):
        edge = edge + pltpu.roll(edge, shift, 0)
    return jnp.where(row == 3, edge, main)


def unpack_pair(x):
    lane = iota((8, LANES), 1)
    row = iota((8, LANES), 0)
    half = LANES // 2
    own_even = (lane < half) & (row < 3)
    live = (row & 3) < 3
    own_odd = (lane < half) & (row >= 4) & live
    rim = (lane // 4 == half // 4) | (lane // 4 == LANES // 4 - 1)
    swapped = pltpu.roll(x, half, 1)
    first = jnp.where(own_even, x, jnp.where(own_odd, pltpu.roll(swapped, 4, 0), 0.0))
    second = jnp.where(own_even, pltpu.roll(x, 4, 0), jnp.where(own_odd, swapped, 0.0))
    edge = jnp.broadcast_to(x[3:4], (8, LANES))
    out = []
    for tile, start in ((first, 0), (second, 28)):
        for r in (0, 1, 2, 4, 5, 6):
            tile = jnp.where(rim & (row == r), pltpu.roll(edge, (half - start - 4 * r) % LANES, 1), tile)
        out.append(tile)
    return out


def send_planes(local_ref, tiles, slab, to_a, to_b):
    count = plane_rows(tiles)
    half = count // 2
    even = slab % 2 == 0

    def body(i, _):
        at = pl.multiple_of(i * 8, 8)

        def tile(start):
            return local_ref[pl.ds(start + at, 8), :]

        low = pack_pair(tile(0), tile(half))
        high = pack_pair(tile(2 * count), tile(2 * count + half))
        to_a[pl.ds(at, 8), :] = jnp.where(even, high, low)
        to_b[pl.ds(at, 8), :] = jnp.where(even, low, high)
        return 0

    lax.fori_loop(0, tiles // 2, body, 0, unroll=11)


def gather_nodes(local_ref, from_a, from_b, free_ref, tiles, slab, nodes_ref):
    count = plane_rows(tiles)
    half = count // 2
    even = slab % 2 == 0
    nodes_ref[count : 2 * count] = free_ref[count : 2 * count] * local_ref[count : 2 * count]

    def body(i, _):
        at = pl.multiple_of(i * 8, 8)
        a = from_a[pl.ds(at, 8), :]
        b = from_b[pl.ds(at, 8), :]
        for start, packed in ((0, jnp.where(even, b, a)), (2 * count, jnp.where(even, a, b))):
            for part, tile in enumerate(unpack_pair(packed)):
                where = pl.ds(start + part * half + at, 8)
                nodes_ref[where, :] = free_ref[where, :] * (local_ref[where, :] + tile)
        return 0

    lax.fori_loop(0, tiles // 2, body, 0, unroll=11)


def filter_kernel(design_ref, da_ref, db_ref, strip_ref, sw_ref, factor_ref, density_ref, fine_ref, sum_ref):
    planes, fy, fz = design_ref.shape
    role, slab = where_am_i()
    slabs = lax.axis_size("gx") * lax.axis_size("gy")
    roles = lax.axis_size("role")
    half = fz // 2
    even = slab % 2 == 0

    at_lane = jnp.where(role == 0, 0, LANES - STRIP)
    put = jnp.where(iota((STRIP, LANES), 1) == iota((STRIP, LANES), 0) + at_lane, 1.0, 0.0).astype(BF16)
    for p in range(planes):
        a = da_ref[p]
        b = db_ref[p]
        fine_ref[p, :, :fz] = jnp.where(even, b, a)
        fine_ref[planes + p, :, :fz] = design_ref[p]
        fine_ref[2 * planes + p, :, :fz] = jnp.where(even, a, b)
    for p in range(planes):
        own = pick_right(strip_ref[p * fy : (p + 1) * fy], put)
        a = pick_right(strip_ref[(planes + p) * fy : (planes + p + 1) * fy], put)
        b = pick_right(strip_ref[(2 * planes + p) * fy : (2 * planes + p + 1) * fy], put)
        fine_ref[p, :, fz:] = jnp.where(even, b, a)
        fine_ref[planes + p, :, fz:] = own
        fine_ref[2 * planes + p, :, fz:] = jnp.where(even, a, b)

    width = 2 * fz
    lane = iota((1, width), 1)
    z_place = role * fz + jnp.where(lane < fz + fz // 2, lane, lane - width)
    inv_z = 1.0 / hat_count(z_place, roles * fz)
    inv_y = 1.0 / hat_count(iota((fy, 1), 0), fy)
    inv_yz = inv_y * inv_z
    sum_ref[...] = jnp.zeros((fy, width), F32)

    def filter_plane(p, _):
        x = fine_ref[p] + fine_ref[p + 4] + 2.0 * (fine_ref[p + 1] + fine_ref[p + 3]) + 3.0 * fine_ref[p + 2]
        x = smooth_y(smooth_z(x))
        place = jnp.full((1, 1), slab * planes + p - 2, jnp.int32)
        inv = inv_yz * (1.0 / hat_count(place, slabs * planes))
        bent = jnp.tanh(SHARPNESS * (x * inv - THRESHOLD))
        sw_ref[p] = (SHARPNESS / (2.0 * TANH2)) * (1.0 - bent * bent) * inv
        mine = jnp.logical_and(p >= 2, p < 2 + planes)
        sum_ref[...] += jnp.where(mine, (TANH2 + bent) * (1.0 / (2.0 * TANH2)), 0.0)
        return 0

    lax.fori_loop(0, planes + 4, filter_plane, 0)

    rows = factor_ref.shape[0]
    pool_y = jnp.where(iota((rows, fy), 1) // 4 == iota((rows, fy), 0), 1.0, 0.0).astype(BF16)
    pool_z = jnp.where(iota((width, LANES), 0) // 2 == iota((width, LANES), 1), 1.0, 0.0).astype(BF16)
    density = pick_right(pick_left(pool_y, sum_ref[...]), pool_z) * (1.0 / 32.0)
    inside = element_lanes((rows, LANES), role, half)
    density = jnp.where(inside, density, 0.0)
    density_ref[...] = density
    factor_ref[...] = jnp.where(inside, FLOOR_STIFF + (1.0 - FLOOR_STIFF) * density * density * density, 0.0)


def first_kernel(
    rf_ref, factor_ref, table_ref,
    nodes_ref, free_ref, local_ref, to_a, to_b, e00_ref,
    main_ref, shift_ref, shift32_ref,
):
    tiles = main_ref.shape[1]
    count = plane_rows(tiles)
    role, slab = where_am_i()
    half = LANES // 2
    parts = rf_ref.shape[0]
    deep = (2 * factor_ref.shape[0]) // parts
    tail = 18 * deep

    nodes_ref[...] = jnp.zeros(nodes_ref.shape, F32)
    free_ref[...] = jnp.zeros(free_ref.shape, F32)
    zi = iota((2 * LANES, 2 * LANES), 0)
    ci = iota((2 * LANES, 2 * LANES), 1)
    lane_of = ci & (LANES - 1)
    odd = ci // LANES
    first_lane = jnp.where(role == 0, half, LANES - STRIP // 2)
    own = zi == 2 * lane_of + odd
    edge = (zi & (STRIP - 1)) == 2 * (lane_of - first_lane) + odd
    table = jnp.where(zi < LANES, jnp.where(own, 1.0, 0.0), jnp.where(edge, 1.0, 0.0)).astype(BF16)
    own_y = (iota((deep, LANES), 1) // STRIP) == iota((deep, LANES), 0)
    for row in range(6):
        for a in range(3):
            at = row * 3 + a
            x = jnp.concatenate([rf_ref[j, at * deep : (at + 1) * deep] for j in range(parts)], axis=0)
            st = jnp.concatenate(
                [jnp.where(own_y, rf_ref[j, tail + at : tail + at + 1], 0.0) for j in range(parts)], axis=0
            )
            x = jnp.concatenate([x, st], axis=1)
            if row < 3:
                y = pick_right(x, table)
                dest = nodes_ref
            else:
                y = dot(x.astype(BF16), table)
                dest = free_ref
            q = row % 3
            dest[pl.ds(a * count + q, parts * deep, stride=8), :] = y[:, :LANES]
            dest[pl.ds(a * count + 4 + q, parts * deep, stride=8), :] = y[:, LANES:]

    make_tiles(nodes_ref, main_ref, shift_ref, shift32_ref)
    sweep(table_ref, main_ref, shift_ref, factor_ref, local_ref, [(nodes_ref, shift32_ref, e00_ref)])
    send_planes(local_ref, tiles, slab, to_a, to_b)


def second_kernel(
    prev_ref, free_ref, last_ref, from_a, from_b, factor_ref, table_ref,
    nodes_ref, local_ref, to_a, to_b, e01_ref, e11_ref,
    main_ref, shift_ref, shift32_ref, prev32_ref,
):
    tiles = main_ref.shape[1]
    _, slab = where_am_i()
    gather_nodes(last_ref, from_a, from_b, free_ref, tiles, slab, nodes_ref)
    for s in range(2):
        prev32_ref[s] = shifted_tiles(prev_ref, tiles, s)
    make_tiles(nodes_ref, main_ref, shift_ref, shift32_ref)
    sweep(
        table_ref, main_ref, shift_ref, factor_ref, local_ref,
        [(prev_ref, prev32_ref, e01_ref), (nodes_ref, shift32_ref, e11_ref)],
    )
    send_planes(local_ref, tiles, slab, to_a, to_b)


def third_kernel(
    v0_ref, v1_ref, free_ref, last_ref, from_a, from_b, factor_ref, table_ref, e00_ref, e01_ref, e11_ref,
    nodes_ref, e02_ref, e12_ref, e22_ref, moment_ref,
    main_ref, shift_ref, shift32_ref, s0_ref, s1_ref,
):
    tiles = main_ref.shape[1]
    count = plane_rows(tiles)
    _, slab = where_am_i()
    gather_nodes(last_ref, from_a, from_b, free_ref, tiles, slab, nodes_ref)
    for s in range(2):
        s0_ref[s] = shifted_tiles(v0_ref, tiles, s)
        s1_ref[s] = shifted_tiles(v1_ref, tiles, s)
    make_tiles(nodes_ref, main_ref, shift_ref, shift32_ref)
    sweep(
        table_ref, main_ref, shift_ref, factor_ref, None,
        [(v0_ref, s0_ref, e02_ref), (v1_ref, s1_ref, e12_ref), (nodes_ref, shift32_ref, e22_ref)],
    )
    half = LANES // 2
    own = iota((1, LANES), 1) < half
    v0 = v0_ref[0 : 2 * count]
    sums = [jnp.sum(v0 * v0, axis=0, keepdims=True)]
    for e_ref in (e00_ref, e01_ref, e11_ref, e12_ref, e22_ref):
        sums.append(jnp.sum(factor_ref[...] * e_ref[...], axis=0, keepdims=True))
    lane = iota((1, LANES), 1)
    out = jnp.zeros((1, LANES), F32)
    for k, s in enumerate(sums):
        total = jnp.sum(jnp.where(own, s, 0.0), axis=1, keepdims=True)
        out = jnp.where(lane == k, total, out)
    moment_ref[...] = jnp.broadcast_to(out, moment_ref.shape)


def combine_kernel(
    moment_ref, v0_ref, v1_ref, v2_ref, e00_ref, e01_ref, e11_ref, e02_ref, e12_ref, e22_ref, density_ref,
    grad_ref, u_ref, nodes_ref,
):
    role, _ = where_am_i()
    parts, _, _, deep, fz = u_ref.shape
    half = fz // 2
    count = v0_ref.shape[0] // 3
    total = jnp.sum(moment_ref[...], axis=0, keepdims=True)
    lane = iota((1, LANES), 1)
    m = [jnp.sum(jnp.where(lane == k, total, 0.0), axis=1, keepdims=True) for k in range(6)]
    s = m[1] / m[0]
    inv = 1.0 / s
    mu = [jnp.ones_like(s)]
    power = 1.0 / m[0]
    for k in range(1, 6):
        power = power * inv
        mu.append(m[k] * power)
    nu = list(mu)
    for depth in range(1, 6):
        for k in range(5, depth - 1, -1):
            nu[k] = nu[k] - nu[k - 1]
    g = [nu[k] + nu[k + 1] for k in range(5)]
    l10 = g[1] / g[0]
    l20 = g[2] / g[0]
    d1 = g[2] - l10 * g[1]
    x12 = g[3] - l10 * g[2]
    r1 = nu[1] - l10 * nu[0]
    r2 = nu[2] - l20 * nu[0]
    l21 = x12 / d1
    d2 = (g[4] - l20 * g[2]) - l21 * x12
    c2 = (r2 - l21 * r1) / d2
    c1 = (r1 - x12 * c2) / d1
    c0 = (nu[0] - g[1] * c1 - g[2] * c2) / g[0]
    w0 = (c0 - c1 + c2) * inv
    w1 = (c1 - 2.0 * c2) * inv * inv
    w2 = c2 * inv * inv * inv
    energy = (
        w0 * (w0 * e00_ref[...] + 2.0 * (w1 * e01_ref[...] + w2 * e02_ref[...]))
        + w1 * (w1 * e11_ref[...] + 2.0 * w2 * e12_ref[...])
        + w2 * w2 * e22_ref[...]
    )
    density = density_ref[...]
    grad = (-3.0 * (1.0 - FLOOR_STIFF) / 32.0) * density * density * energy
    grad_ref[...] = jnp.where(element_lanes(grad.shape, role, half), grad, 0.0)
    nodes_ref[...] = w0 * v0_ref[0 : 2 * count] + w1 * v1_ref[0 : 2 * count] + w2 * v2_ref[0 : 2 * count]
    gi = iota((LANES, fz), 0)
    zi = iota((LANES, fz), 1)
    even_table = jnp.where(zi == 2 * gi, 1.0, 0.0).astype(BF16)
    odd_table = jnp.where(zi == 2 * gi + 1, 1.0, 0.0).astype(BF16)
    for a in range(2):
        for q in range(3):
            even = nodes_ref[pl.ds(a * count + q, parts * deep, stride=8), :]
            odd = nodes_ref[pl.ds(a * count + 4 + q, parts * deep, stride=8), :]
            x = pick_right(even, even_table) + pick_right(odd, odd_table)
            for j in range(parts):
                u_ref[j, q, a] = x[j * deep : (j + 1) * deep]


def last_kernel(grad_ref, ga_ref, gb_ref, sw_ref, out_ref, work_ref):
    planes, fy, fz = out_ref.shape
    width = 2 * fz
    _, slab = where_am_i()
    even = slab % 2 == 0
    rows = grad_ref.shape[0]
    pool_y = jnp.where(iota((fy, rows), 0) // 4 == iota((fy, rows), 1), 1.0, 0.0).astype(BF16)
    pool_z = jnp.where(iota((LANES, width), 1) // 2 == iota((LANES, width), 0), 1.0, 0.0).astype(BF16)
    a = ga_ref[...]
    b = gb_ref[...]
    low = jnp.where(even, b, a)
    high = jnp.where(even, a, b)
    for grad, first, last in ((low, 0, 2), (grad_ref[...], 2, 2 + planes), (high, 2 + planes, 4 + planes)):
        wide = pick_right(pick_left(pool_y, grad), pool_z)
        for p in range(first, last):
            work_ref[p] = wide * sw_ref[p]

    def body(p, _):
        x = work_ref[p] + work_ref[p + 4] + 2.0 * (work_ref[p + 1] + work_ref[p + 3]) + 3.0 * work_ref[p + 2]
        out_ref[p] = smooth_y(smooth_z(x))[:, :fz]
        return 0

    lax.fori_loop(0, planes, body, 0)


def shape(*dims, dtype=F32):
    return jax.ShapeDtypeStruct(dims, dtype)


def on_device(design, force, clamped_dof_mask, stiffness):
    planes, fy, fz = design.shape
    _, bx, by, _ = force.shape
    gx = lax.axis_size("gx")
    gy = lax.axis_size("gy")
    roles = lax.axis_size("role")
    devices = gx * gy * roles
    slabs = gx * gy
    assert roles == 2 and planes == 4 and fz == LANES and bx == 2 * gy and slabs % 2 == 0
    columns = fy // 4
    nodes = fy // 2
    tiles = nodes + 2
    count = tiles * 8
    pairs_a = [(i, i ^ 1) for i in range(slabs)]
    pairs_b = [(i, i + 1 if i % 2 else i - 1) for i in range(1, slabs - 1)]

    def beside(to_a, to_b):
        b = lax.ppermute(to_b, LINE, pairs_b)
        a = lax.ppermute(to_a, LINE, pairs_a)
        return a, b

    plane0, strips, corner = pl.pallas_call(
        strip_rows_kernel,
        out_shape=(shape(6 * by, fz), shape(6 * bx, LANES), shape(8, LANES)),
        in_specs=[pl.BlockSpec(memory_space=pltpu.HBM)] * 2,
        scratch_shapes=[
            pltpu.VMEM(force.shape, F32), pltpu.VMEM(force.shape, jnp.int32), pltpu.SemaphoreType.DMA((2,)),
        ],
        name="rows",
        compiler_params=KEEP,
    )(force, clamped_dof_mask)
    plane0, strips, corner, design = lax.optimization_barrier((plane0, strips, corner, design))
    next_plane = lax.ppermute(plane0, "gx", [(i + 1, i) for i in range(gx - 1)])
    strips = lax.ppermute(strips, "role", [(0, 1), (1, 0)])
    corner = lax.ppermute(
        corner, ("role", "gx"), [((1 - r) * gx + i + 1, r * gx + i) for r in range(2) for i in range(gx - 1)]
    )
    design_a, design_b = beside(design, design)
    pack, table = pl.pallas_call(
        pack_kernel,
        out_shape=(shape(gy, 18 * by + 24, fz), shape(2 * ROWS, 2 * ROWS, dtype=BF16)),
        name="pack",
        compiler_params=KEEP,
    )(force, clamped_dof_mask, next_plane, strips, corner, stiffness, jnp.asarray(place_table()))
    rf = lax.all_to_all(pack, "gy", 0, 0)

    role = lax.axis_index("role")

    def strip(x):
        return jnp.where(role == 0, x[..., fz - STRIP :], x[..., :STRIP]).reshape(-1, STRIP)

    fine_strips = jnp.concatenate([strip(design), strip(design_a), strip(design_b)], axis=0)
    fine_strips = lax.ppermute(fine_strips, "role", [(0, 1), (1, 0)])

    node_set = shape(3 * count, LANES)
    plane = shape(count // 2, LANES)
    element = shape(columns, LANES)
    tile_scratch = [
        pltpu.VMEM((3, tiles, 16, LANES), BF16),
        pltpu.VMEM((2, tiles, 16, LANES), BF16),
        pltpu.VMEM((2, count, LANES), F32),
    ]
    shift32 = pltpu.VMEM((2, count, LANES), F32)
    sw, factor, density = pl.pallas_call(
        filter_kernel,
        out_shape=(shape(planes + 4, fy, 2 * fz), element, element),
        scratch_shapes=[pltpu.VMEM((3 * planes, fy, 2 * fz), F32), pltpu.VMEM((fy, 2 * fz), F32)],
        name="filter",
        compiler_params=KEEP,
        cost_estimate=pl.CostEstimate(flops=30_000_000, transcendentals=0, bytes_accessed=4_000_000),
    )(design, design_a, design_b, fine_strips)
    v0, free, local, to_a, to_b, e00 = pl.pallas_call(
        first_kernel,
        out_shape=(node_set, node_set, node_set, plane, plane, element),
        scratch_shapes=tile_scratch,
        name="first",
        compiler_params=KEEP,
    )(rf, factor, table)
    from_a, from_b = beside(to_a, to_b)
    v1, local, to_a, to_b, e01, e11 = pl.pallas_call(
        second_kernel,
        out_shape=(node_set, node_set, plane, plane, element, element),
        scratch_shapes=tile_scratch + [shift32],
        name="second",
        compiler_params=KEEP,
    )(v0, free, local, from_a, from_b, factor, table)
    from_a, from_b = beside(to_a, to_b)
    v2, e02, e12, e22, moments = pl.pallas_call(
        third_kernel,
        out_shape=(node_set, element, element, element, shape(devices, LANES)),
        scratch_shapes=tile_scratch + [shift32, shift32],
        name="third",
        compiler_params=KEEP,
    )(v0, v1, free, local, from_a, from_b, factor, table, e00, e01, e11)
    moments = lax.all_to_all(moments, ("role", "gx", "gy"), 0, 0, tiled=True)
    grad, u = pl.pallas_call(
        combine_kernel,
        out_shape=(element, shape(gy, 3, 2, by, fz)),
        scratch_shapes=[pltpu.VMEM((2 * count, LANES), F32)],
        name="combine",
        compiler_params=KEEP,
    )(moments, v0, v1, v2, e00, e01, e11, e02, e12, e22, density)
    grad_a, grad_b = beside(grad, grad)
    sensitivity = pl.pallas_call(
        last_kernel,
        out_shape=shape(planes, fy, fz),
        scratch_shapes=[pltpu.VMEM((planes + 4, fy, 2 * fz), F32)],
        name="last",
        compiler_params=KEEP,
    )(grad, grad_a, grad_b, sw)
    u = lax.all_to_all(u, "gy", 0, 0)
    displacement = jnp.transpose(u, (1, 0, 2, 3, 4)).reshape(3, bx, by, fz)
    return sensitivity, displacement


def solution(mesh):
    placed = (
        P(("gx", "gy"), None, "role"),
        P(None, "gx", "gy", "role"),
        P(None, "gx", "gy", "role"),
        P(),
    )

    return jax.shard_map(
        on_device,
        mesh=mesh,
        in_specs=placed,
        out_specs=(P(("gx", "gy"), None, "role"), P(None, "gx", "gy", "role")),
        check_vma=False,
    )
```

```python
import jax
import jax.numpy as jnp
import numpy as np
from jax import lax
from jax.experimental import pallas as pl
from jax.experimental.pallas import tpu as pltpu
from jax.sharding import PartitionSpec as P


SHARPNESS = 4.0
THRESHOLD = 0.5
FLOOR_STIFF = 0.001
TANH2 = float(np.tanh(2.0))
LANES = 128
HALO = 3
STRIP = 8
ROWS = 120
LINE = ("gx", "gy")
KEEP = pltpu.CompilerParams(vmem_limit_bytes=12 << 20)
F32 = jnp.float32
BF16 = jnp.bfloat16


def iota(shape, dim):
    return lax.broadcasted_iota(jnp.int32, shape, dim)


def place_table():
    table = np.zeros((ROWS, 81), np.float32)
    for c in range(3):
        for b in range(3):
            for a in range(3):
                for q in range(3):
                    dof = ((c * 3 + b) * 3 + a) * 3 + q
                    if c < 2:
                        row = 8 * (3 * a + b) + 4 * c + q
                    else:
                        row = 72 + 8 * (2 * b + (a == 2)) + 4 * (a == 1) + q
                    table[row, dof] = 1.0
    return table


def split2(x):
    hi = x.astype(BF16)
    return hi, (x - hi.astype(F32)).astype(BF16)


def split3(x):
    hi = x.astype(BF16)
    rest = x - hi.astype(F32)
    mid = rest.astype(BF16)
    return hi, mid, (rest - mid.astype(F32)).astype(BF16)


def dot(a, b):
    return jnp.dot(a, b, preferred_element_type=F32)


def pick_right(x, table):
    hi, mid, lo = split3(x)
    return (dot(hi, table) + dot(mid, table)) + dot(lo, table)


def pick_left(table, x):
    hi, mid, lo = split3(x)
    return (dot(table, hi) + dot(table, mid)) + dot(table, lo)


def where_am_i():
    role = lax.axis_index("role")
    slab = lax.axis_index("gx") * lax.axis_size("gy") + lax.axis_index("gy")
    return role, slab


def element_lanes(shape, role, half):
    lane = iota(shape, len(shape) - 1)
    above = jnp.logical_and(lane >= half, lane < half + HALO)
    below = lane >= LANES - HALO
    roles = lax.axis_size("role")
    return (lane < half) | (above & (role < roles - 1)) | (below & (role > 0))


def hat_count(place, extent):
    low = jnp.where(place == 0, 3.0, jnp.where(place == 1, 1.0, 0.0))
    high = jnp.where(place == extent - 1, 3.0, jnp.where(place == extent - 2, 1.0, 0.0))
    return 9.0 - low - high


def smooth_z(x):
    width = x.shape[1]
    for _ in range(2):
        x = x + pltpu.roll(x, 1, 1) + pltpu.roll(x, width - 1, 1)
    return x


def smooth_y(x):
    rows = x.shape[0]
    x = jnp.concatenate([x, jnp.zeros((8, x.shape[1]), F32)], axis=0)
    for _ in range(2):
        x = x + pltpu.roll(x, 1, 0) + pltpu.roll(x, rows + 7, 0)
    return x[:rows]


def strip_rows_kernel(force_hbm, mask_hbm, plane_ref, strip_ref, corner_ref, force_ref, mask_ref, sems):
    copies = (
        pltpu.make_async_copy(force_hbm, force_ref, sems.at[0]),
        pltpu.make_async_copy(mask_hbm, mask_ref, sems.at[1]),
    )
    for copy in copies:
        copy.start()
    for copy in copies:
        copy.wait()
    _, bx, by, fz = force_ref.shape
    role, _ = where_am_i()
    first = jnp.where(role == 0, fz - STRIP, 0)
    take = jnp.where(iota((fz, LANES), 0) == first + (iota((fz, LANES), 1) & (STRIP - 1)), 1.0, 0.0).astype(BF16)
    own_y = (iota((bx, by, LANES), 2) // STRIP) == iota((bx, by, LANES), 1)
    corner_ref[...] = jnp.zeros(corner_ref.shape, F32)
    for q in range(3):
        free = 1.0 - mask_ref[q].astype(F32)
        rhs = free * force_ref[q]
        plane_ref[q * by : (q + 1) * by] = rhs[0]
        plane_ref[(q + 3) * by : (q + 4) * by] = free[0]
        edge = pick_right(rhs.reshape(bx * by, fz), take), dot(free.reshape(bx * by, fz).astype(BF16), take)
        for row, x in ((q, edge[0]), (q + 3, edge[1])):
            x = jnp.sum(jnp.where(own_y, x.reshape(bx, by, LANES), 0.0), axis=1)
            strip_ref[row * bx : (row + 1) * bx] = x
            corner_ref[row : row + 1] = x[0:1]


def pack_kernel(force_ref, mask_ref, plane_ref, strip_ref, corner_ref, pack_ref):
    _, bx, by, _ = force_ref.shape
    parts = pack_ref.shape[0]
    tail = 18 * by
    for j in range(parts):
        pack_ref[j, tail + 18 :] = jnp.zeros((pack_ref.shape[1] - tail - 18, LANES), F32)
    for q in range(3):
        free = 1.0 - mask_ref[q].astype(F32)
        rhs = free * force_ref[q]
        for row, val in ((q, rhs), (q + 3, free)):
            for j in range(parts):
                for a in range(3):
                    x = 2 * j + a
                    at = row * 3 + a
                    inner = x < bx
                    pack_ref[j, at * by : (at + 1) * by] = val[x] if inner else plane_ref[row * by : (row + 1) * by]
                    edge = strip_ref[row * bx + x : row * bx + x + 1] if inner else corner_ref[row : row + 1]
                    pack_ref[j, tail + at : tail + at + 1] = edge


def table_kernel(stiff_ref, place_ref, table_ref):
    place = place_ref[...]
    half_way = jnp.dot(place, stiff_ref[...], precision=lax.Precision.HIGHEST, preferred_element_type=F32)
    spread = lax.dot_general(
        half_way, place, (((1,), (1,)), ((), ())), precision=lax.Precision.HIGHEST, preferred_element_type=F32
    )
    hi, lo = split2(spread)
    row = iota((ROWS, 2 * ROWS), 0)
    col = iota((ROWS, 2 * ROWS), 1)
    twice = jnp.where(row == 8 * (col // 16) + col % 8, 1.0, 0.0).astype(BF16)
    table_ref[:ROWS] = dot(hi, twice).astype(BF16)
    table_ref[ROWS:] = dot(lo, twice).astype(BF16)


def plane_rows(tiles):
    return tiles * 8


def shifted_tiles(nodes_ref, tiles, s):
    count = plane_rows(tiles)
    upper = (iota((count, LANES), 0) & 4) == 0
    if s == 0:
        first = nodes_ref[0:count]
        second = nodes_ref[count : 2 * count]
        x = jnp.where(upper, first, pltpu.roll(second, 4, 0))
    else:
        x = jnp.where(upper, nodes_ref[2 * count : 3 * count], 0.0)
    return pltpu.roll(x, LANES - 1, 1)


def pair_tiles(x):
    tiles = x.shape[0] // 8
    hi = x.astype(BF16).astype(F32)
    lo = x - hi
    both = jnp.concatenate([hi.reshape(tiles, 8, LANES), lo.reshape(tiles, 8, LANES)], axis=1)
    return both.astype(BF16)


def make_tiles(nodes_ref, main_ref, shift_ref, shift32_ref):
    tiles = main_ref.shape[1]
    count = plane_rows(tiles)
    for a in range(3):
        main_ref[a] = pair_tiles(nodes_ref[a * count : (a + 1) * count])
    for s in range(2):
        x = shifted_tiles(nodes_ref, tiles, s)
        if shift32_ref is not None:
            shift32_ref[s] = x
        shift_ref[s] = pair_tiles(x)


def sweep(table_ref, main_ref, shift_ref, factor_ref, out_ref, energies):
    tiles = main_ref.shape[1]
    columns = factor_ref.shape[0]
    upper = iota((8, LANES), 0) < 4

    def finish(node, parts):
        t0, t1, t2, s0, s1 = parts
        r0 = pltpu.roll(s0, 1, 1)
        r1 = pltpu.roll(s1, 1, 1)
        done = (
            t0 + jnp.where(upper, r0, 0.0),
            t1 + jnp.where(upper, pltpu.roll(r0, 4, 0), 0.0),
            t2 + jnp.where(upper, r1, 0.0),
        )
        for a in range(3):
            out_ref[pl.ds(pl.multiple_of((a * tiles + node) * 8, 8), 8), :] = done[a]

    def body(i, carry):
        cols = []
        for k in range(2):
            base = 4 * i + 2 * k
            pieces = [main_ref[a, base + b] for a in range(3) for b in range(3)]
            pieces += [shift_ref[s, base + b] for b in range(3) for s in range(2)]
            cols.append(jnp.concatenate(pieces, axis=0))
        product = dot(table_ref[...], jnp.concatenate(cols, axis=1))
        product = product[:ROWS] + product[ROWS:]
        parts = []
        for k in range(2):
            y = product[:, k * LANES : (k + 1) * LANES]
            base = 4 * i + 2 * k
            for nodes_ref, shift32_ref, e_ref in energies:
                total = None
                for a in range(3):
                    for b in range(3):
                        at = pl.multiple_of((a * tiles + base + b) * 8, 8)
                        term = nodes_ref[pl.ds(at, 8), :] * y[8 * (3 * a + b) : 8 * (3 * a + b) + 8]
                        total = term if total is None else total + term
                for b in range(3):
                    for s in range(2):
                        at = pl.multiple_of((base + b) * 8, 8)
                        lo = 72 + 8 * (2 * b + s)
                        total = total + shift32_ref[s, pl.ds(at, 8), :] * y[lo : lo + 8]
                e_ref[pl.ds(2 * i + k, 1), :] = jnp.sum(total, axis=0, keepdims=True)
            if out_ref is not None:
                z = y * factor_ref[pl.ds(2 * i + k, 1), :]
                parts.append(
                    [
                        [z[8 * (3 * a + b) : 8 * (3 * a + b) + 8] for a in range(3)]
                        + [z[72 + 8 * (2 * b + s) : 80 + 8 * (2 * b + s)] for s in range(2)]
                        for b in range(3)
                    ]
                )
        if out_ref is None:
            return carry
        left, right = parts
        finish(4 * i, [c + v for c, v in zip(carry, left[0])])
        finish(4 * i + 1, left[1])
        finish(4 * i + 2, [c + v for c, v in zip(left[2], right[0])])
        finish(4 * i + 3, right[1])
        return tuple(right[2])

    if out_ref is None:
        lax.fori_loop(0, columns // 2, lambda i, c: body(i, c), 0, unroll=min(16, columns // 2))
    else:
        zero = jnp.zeros((8, LANES), F32)
        lax.fori_loop(0, columns // 2, body, (zero,) * 5, unroll=min(16, columns // 2))
        for a in range(3):
            for node in range(2 * columns, tiles):
                at = (a * tiles + node) * 8
                out_ref[at : at + 8, :] = zero


def pack_pair(x, y):
    lane = iota((8, LANES), 1)
    row = iota((8, LANES), 0)
    half = LANES // 2
    even = jnp.where(row < 4, x, pltpu.roll(y, 4, 0))
    odd = jnp.where(row < 4, pltpu.roll(x, 4, 0), y)
    main = jnp.where(lane < half, even, pltpu.roll(odd, half, 1))
    edge = jnp.zeros((8, LANES), F32)
    for tile, first in ((x, 0), (y, 28)):
        moved = pltpu.roll(tile, half + first, 1, stride=4, stride_axis=0)
        at = lane - first - 4 * row
        edge = jnp.where(((at >= 0) & (at < 4)) | ((at >= 60) & (at < 64)), moved, edge)
    for shift in (4, 2, 1):
        edge = edge + pltpu.roll(edge, shift, 0)
    return jnp.where(row == 3, edge, main)


def unpack_pair(x):
    lane = iota((8, LANES), 1)
    row = iota((8, LANES), 0)
    half = LANES // 2
    own_even = (lane < half) & (row < 3)
    live = (row & 3) < 3
    own_odd = (lane < half) & (row >= 4) & live
    rim = live & ((lane // 4 == half // 4) | (lane // 4 == LANES // 4 - 1))
    swapped = pltpu.roll(x, half, 1)
    first = jnp.where(own_even, x, jnp.where(own_odd, pltpu.roll(swapped, 4, 0), 0.0))
    second = jnp.where(own_even, pltpu.roll(x, 4, 0), jnp.where(own_odd, swapped, 0.0))
    edge = jnp.broadcast_to(x[3:4], (8, LANES))
    out = []
    for tile, start in ((first, 0), (second, 28)):
        moved = jnp.take_along_axis(edge, (lane - half + start + 4 * row) & (LANES - 1), axis=1)
        out.append(jnp.where(rim, moved, tile))
    return out


def send_planes(local_ref, tiles, slab, to_a, to_b):
    count = plane_rows(tiles)
    half = count // 2
    even = slab % 2 == 0

    def body(i, _):
        at = pl.multiple_of(i * 8, 8)

        def tile(start):
            return local_ref[pl.ds(start + at, 8), :]

        low = pack_pair(tile(0), tile(half))
        high = pack_pair(tile(2 * count), tile(2 * count + half))
        to_a[pl.ds(at, 8), :] = jnp.where(even, high, low)
        to_b[pl.ds(at, 8), :] = jnp.where(even, low, high)
        return 0

    lax.fori_loop(0, tiles // 2, body, 0, unroll=11)


def gather_nodes(local_ref, from_a, from_b, free_ref, tiles, slab, nodes_ref):
    count = plane_rows(tiles)
    half = count // 2
    even = slab % 2 == 0
    nodes_ref[count : 2 * count] = free_ref[count : 2 * count] * local_ref[count : 2 * count]

    def body(i, _):
        at = pl.multiple_of(i * 8, 8)
        a = from_a[pl.ds(at, 8), :]
        b = from_b[pl.ds(at, 8), :]
        for start, packed in ((0, jnp.where(even, b, a)), (2 * count, jnp.where(even, a, b))):
            for part, tile in enumerate(unpack_pair(packed)):
                where = pl.ds(start + part * half + at, 8)
                nodes_ref[where, :] = free_ref[where, :] * (local_ref[where, :] + tile)
        return 0

    lax.fori_loop(0, tiles // 2, body, 0, unroll=11)


def filter_kernel(design_ref, da_ref, db_ref, strip_ref, sw_ref, factor_ref, density_ref, fine_ref, sum_ref):
    planes, fy, fz = design_ref.shape
    role, slab = where_am_i()
    slabs = lax.axis_size("gx") * lax.axis_size("gy")
    roles = lax.axis_size("role")
    half = fz // 2
    even = slab % 2 == 0

    at_lane = jnp.where(role == 0, 0, LANES - STRIP)
    put = jnp.where(iota((STRIP, LANES), 1) == iota((STRIP, LANES), 0) + at_lane, 1.0, 0.0).astype(BF16)
    for p in range(planes):
        a = da_ref[p]
        b = db_ref[p]
        fine_ref[p, :, :fz] = jnp.where(even, b, a)
        fine_ref[planes + p, :, :fz] = design_ref[p]
        fine_ref[2 * planes + p, :, :fz] = jnp.where(even, a, b)
    for p in range(planes):
        own = pick_right(strip_ref[p * fy : (p + 1) * fy], put)
        a = pick_right(strip_ref[(planes + p) * fy : (planes + p + 1) * fy], put)
        b = pick_right(strip_ref[(2 * planes + p) * fy : (2 * planes + p + 1) * fy], put)
        fine_ref[p, :, fz:] = jnp.where(even, b, a)
        fine_ref[planes + p, :, fz:] = own
        fine_ref[2 * planes + p, :, fz:] = jnp.where(even, a, b)

    width = 2 * fz
    lane = iota((1, width), 1)
    z_place = role * fz + jnp.where(lane < fz + fz // 2, lane, lane - width)
    inv_z = 1.0 / hat_count(z_place, roles * fz)
    inv_y = 1.0 / hat_count(iota((fy, 1), 0), fy)
    inv_yz = inv_y * inv_z
    sum_ref[...] = jnp.zeros((fy, width), F32)

    def filter_plane(p, _):
        x = fine_ref[p] + fine_ref[p + 4] + 2.0 * (fine_ref[p + 1] + fine_ref[p + 3]) + 3.0 * fine_ref[p + 2]
        x = smooth_y(smooth_z(x))
        place = jnp.full((1, 1), slab * planes + p - 2, jnp.int32)
        inv = inv_yz * (1.0 / hat_count(place, slabs * planes))
        bent = jnp.tanh(SHARPNESS * (x * inv - THRESHOLD))
        sw_ref[p] = (SHARPNESS / (2.0 * TANH2)) * (1.0 - bent * bent) * inv
        mine = jnp.logical_and(p >= 2, p < 2 + planes)
        sum_ref[...] += jnp.where(mine, (TANH2 + bent) * (1.0 / (2.0 * TANH2)), 0.0)
        return 0

    lax.fori_loop(0, planes + 4, filter_plane, 0)

    rows = factor_ref.shape[0]
    pool_y = jnp.where(iota((rows, fy), 1) // 4 == iota((rows, fy), 0), 1.0, 0.0).astype(BF16)
    pool_z = jnp.where(iota((width, LANES), 0) // 2 == iota((width, LANES), 1), 1.0, 0.0).astype(BF16)
    density = pick_right(pick_left(pool_y, sum_ref[...]), pool_z) * (1.0 / 32.0)
    inside = element_lanes((rows, LANES), role, half)
    density = jnp.where(inside, density, 0.0)
    density_ref[...] = density
    factor_ref[...] = jnp.where(inside, FLOOR_STIFF + (1.0 - FLOOR_STIFF) * density * density * density, 0.0)


def first_kernel(
    rf_ref, factor_ref, table_ref,
    nodes_ref, free_ref, local_ref, to_a, to_b, e00_ref,
    main_ref, shift_ref, shift32_ref,
):
    tiles = main_ref.shape[1]
    count = plane_rows(tiles)
    role, slab = where_am_i()
    half = LANES // 2
    parts = rf_ref.shape[0]
    deep = (2 * factor_ref.shape[0]) // parts
    tail = 18 * deep

    nodes_ref[...] = jnp.zeros(nodes_ref.shape, F32)
    free_ref[...] = jnp.zeros(free_ref.shape, F32)
    zi = iota((2 * LANES, 2 * LANES), 0)
    ci = iota((2 * LANES, 2 * LANES), 1)
    lane_of = ci & (LANES - 1)
    odd = ci // LANES
    first_lane = jnp.where(role == 0, half, LANES - STRIP // 2)
    own = zi == 2 * lane_of + odd
    edge = (zi & (STRIP - 1)) == 2 * (lane_of - first_lane) + odd
    table = jnp.where(zi < LANES, jnp.where(own, 1.0, 0.0), jnp.where(edge, 1.0, 0.0)).astype(BF16)
    own_y = (iota((deep, LANES), 1) // STRIP) == iota((deep, LANES), 0)
    for row in range(6):
        for a in range(3):
            at = row * 3 + a
            x = jnp.concatenate([rf_ref[j, at * deep : (at + 1) * deep] for j in range(parts)], axis=0)
            st = jnp.concatenate(
                [jnp.where(own_y, rf_ref[j, tail + at : tail + at + 1], 0.0) for j in range(parts)], axis=0
            )
            x = jnp.concatenate([x, st], axis=1)
            if row < 3:
                y = pick_right(x, table)
                dest = nodes_ref
            else:
                y = dot(x.astype(BF16), table)
                dest = free_ref
            q = row % 3
            dest[pl.ds(a * count + q, parts * deep, stride=8), :] = y[:, :LANES]
            dest[pl.ds(a * count + 4 + q, parts * deep, stride=8), :] = y[:, LANES:]

    make_tiles(nodes_ref, main_ref, shift_ref, shift32_ref)
    sweep(table_ref, main_ref, shift_ref, factor_ref, local_ref, [(nodes_ref, shift32_ref, e00_ref)])
    send_planes(local_ref, tiles, slab, to_a, to_b)


def second_kernel(
    prev_ref, free_ref, last_ref, from_a, from_b, factor_ref, table_ref,
    nodes_ref, local_ref, to_a, to_b, e01_ref, e11_ref,
    main_ref, shift_ref, shift32_ref, prev32_ref,
):
    tiles = main_ref.shape[1]
    _, slab = where_am_i()
    gather_nodes(last_ref, from_a, from_b, free_ref, tiles, slab, nodes_ref)
    for s in range(2):
        prev32_ref[s] = shifted_tiles(prev_ref, tiles, s)
    make_tiles(nodes_ref, main_ref, shift_ref, shift32_ref)
    sweep(
        table_ref, main_ref, shift_ref, factor_ref, local_ref,
        [(prev_ref, prev32_ref, e01_ref), (nodes_ref, shift32_ref, e11_ref)],
    )
    send_planes(local_ref, tiles, slab, to_a, to_b)


def third_kernel(
    v0_ref, v1_ref, free_ref, last_ref, from_a, from_b, factor_ref, table_ref, e00_ref, e01_ref, e11_ref,
    nodes_ref, e02_ref, e12_ref, e22_ref, moment_ref,
    main_ref, shift_ref, shift32_ref, s0_ref, s1_ref,
):
    tiles = main_ref.shape[1]
    count = plane_rows(tiles)
    _, slab = where_am_i()
    gather_nodes(last_ref, from_a, from_b, free_ref, tiles, slab, nodes_ref)
    for s in range(2):
        s0_ref[s] = shifted_tiles(v0_ref, tiles, s)
        s1_ref[s] = shifted_tiles(v1_ref, tiles, s)
    make_tiles(nodes_ref, main_ref, shift_ref, shift32_ref)
    sweep(
        table_ref, main_ref, shift_ref, factor_ref, None,
        [(v0_ref, s0_ref, e02_ref), (v1_ref, s1_ref, e12_ref), (nodes_ref, shift32_ref, e22_ref)],
    )
    half = LANES // 2
    own = iota((1, LANES), 1) < half
    v0 = v0_ref[0 : 2 * count]
    sums = [jnp.sum(v0 * v0, axis=0, keepdims=True)]
    for e_ref in (e00_ref, e01_ref, e11_ref, e12_ref, e22_ref):
        sums.append(jnp.sum(factor_ref[...] * e_ref[...], axis=0, keepdims=True))
    lane = iota((1, LANES), 1)
    out = jnp.zeros((1, LANES), F32)
    for k, s in enumerate(sums):
        total = jnp.sum(jnp.where(own, s, 0.0), axis=1, keepdims=True)
        out = jnp.where(lane == k, total, out)
    moment_ref[...] = jnp.broadcast_to(out, moment_ref.shape)


def combine_kernel(
    moment_ref, v0_ref, v1_ref, v2_ref, e00_ref, e01_ref, e11_ref, e02_ref, e12_ref, e22_ref, density_ref,
    grad_ref, u_ref, nodes_ref,
):
    role, _ = where_am_i()
    parts, _, _, deep, fz = u_ref.shape
    half = fz // 2
    count = v0_ref.shape[0] // 3
    total = jnp.sum(moment_ref[...], axis=0, keepdims=True)
    lane = iota((1, LANES), 1)
    m = [jnp.sum(jnp.where(lane == k, total, 0.0), axis=1, keepdims=True) for k in range(6)]
    s = m[1] / m[0]
    inv = 1.0 / s
    mu = [jnp.ones_like(s)]
    power = 1.0 / m[0]
    for k in range(1, 6):
        power = power * inv
        mu.append(m[k] * power)
    nu = list(mu)
    for depth in range(1, 6):
        for k in range(5, depth - 1, -1):
            nu[k] = nu[k] - nu[k - 1]
    g = [nu[k] + nu[k + 1] for k in range(5)]
    l10 = g[1] / g[0]
    l20 = g[2] / g[0]
    d1 = g[2] - l10 * g[1]
    x12 = g[3] - l10 * g[2]
    r1 = nu[1] - l10 * nu[0]
    r2 = nu[2] - l20 * nu[0]
    l21 = x12 / d1
    d2 = (g[4] - l20 * g[2]) - l21 * x12
    c2 = (r2 - l21 * r1) / d2
    c1 = (r1 - x12 * c2) / d1
    c0 = (nu[0] - g[1] * c1 - g[2] * c2) / g[0]
    w0 = (c0 - c1 + c2) * inv
    w1 = (c1 - 2.0 * c2) * inv * inv
    w2 = c2 * inv * inv * inv
    energy = (
        w0 * (w0 * e00_ref[...] + 2.0 * (w1 * e01_ref[...] + w2 * e02_ref[...]))
        + w1 * (w1 * e11_ref[...] + 2.0 * w2 * e12_ref[...])
        + w2 * w2 * e22_ref[...]
    )
    density = density_ref[...]
    grad = (-3.0 * (1.0 - FLOOR_STIFF) / 32.0) * density * density * energy
    grad_ref[...] = jnp.where(element_lanes(grad.shape, role, half), grad, 0.0)
    nodes_ref[...] = w0 * v0_ref[0 : 2 * count] + w1 * v1_ref[0 : 2 * count] + w2 * v2_ref[0 : 2 * count]
    gi = iota((LANES, fz), 0)
    zi = iota((LANES, fz), 1)
    even_table = jnp.where(zi == 2 * gi, 1.0, 0.0).astype(BF16)
    odd_table = jnp.where(zi == 2 * gi + 1, 1.0, 0.0).astype(BF16)
    for a in range(2):
        for q in range(3):
            even = nodes_ref[pl.ds(a * count + q, parts * deep, stride=8), :]
            odd = nodes_ref[pl.ds(a * count + 4 + q, parts * deep, stride=8), :]
            x = pick_right(even, even_table) + pick_right(odd, odd_table)
            for j in range(parts):
                u_ref[j, q, a] = x[j * deep : (j + 1) * deep]


def last_kernel(grad_ref, ga_ref, gb_ref, sw_ref, out_ref, work_ref):
    planes, fy, fz = out_ref.shape
    width = 2 * fz
    _, slab = where_am_i()
    even = slab % 2 == 0
    rows = grad_ref.shape[0]
    pool_y = jnp.where(iota((fy, rows), 0) // 4 == iota((fy, rows), 1), 1.0, 0.0).astype(BF16)
    pool_z = jnp.where(iota((LANES, width), 1) // 2 == iota((LANES, width), 0), 1.0, 0.0).astype(BF16)
    a = ga_ref[...]
    b = gb_ref[...]
    low = jnp.where(even, b, a)
    high = jnp.where(even, a, b)
    for grad, first, last in ((low, 0, 2), (grad_ref[...], 2, 2 + planes), (high, 2 + planes, 4 + planes)):
        wide = pick_right(pick_left(pool_y, grad), pool_z)
        for p in range(first, last):
            work_ref[p] = wide * sw_ref[p]

    def body(p, _):
        x = work_ref[p] + work_ref[p + 4] + 2.0 * (work_ref[p + 1] + work_ref[p + 3]) + 3.0 * work_ref[p + 2]
        out_ref[p] = smooth_y(smooth_z(x)[:, :fz])
        return 0

    lax.fori_loop(0, planes, body, 0, unroll=True)


def shape(*dims, dtype=F32):
    return jax.ShapeDtypeStruct(dims, dtype)


def on_device(design, force, clamped_dof_mask, stiffness):
    planes, fy, fz = design.shape
    _, bx, by, _ = force.shape
    gx = lax.axis_size("gx")
    gy = lax.axis_size("gy")
    roles = lax.axis_size("role")
    devices = gx * gy * roles
    slabs = gx * gy
    assert roles == 2 and planes == 4 and fz == LANES and bx == 2 * gy and slabs % 2 == 0
    columns = fy // 4
    nodes = fy // 2
    tiles = nodes + 2
    count = tiles * 8
    pairs_a = [(i, i ^ 1) for i in range(slabs)]
    pairs_b = [(i, i + 1 if i % 2 else i - 1) for i in range(1, slabs - 1)]

    def beside(to_a, to_b):
        b = lax.ppermute(to_b, LINE, pairs_b)
        a = lax.ppermute(to_a, LINE, pairs_a)
        return a, b

    plane0, strips, corner = pl.pallas_call(
        strip_rows_kernel,
        out_shape=(shape(6 * by, fz), shape(6 * bx, LANES), shape(8, LANES)),
        in_specs=[pl.BlockSpec(memory_space=pltpu.HBM)] * 2,
        scratch_shapes=[
            pltpu.VMEM(force.shape, F32), pltpu.VMEM(force.shape, jnp.int32), pltpu.SemaphoreType.DMA((2,)),
        ],
        name="rows",
        compiler_params=KEEP,
    )(pltpu.with_memory_space_constraint(force, pltpu.HBM), pltpu.with_memory_space_constraint(clamped_dof_mask, pltpu.HBM))
    plane0, strips, corner, design = lax.optimization_barrier((plane0, strips, corner, design))
    next_plane = lax.ppermute(plane0, "gx", [(i + 1, i) for i in range(gx - 1)])
    strips = lax.ppermute(strips, "role", [(0, 1), (1, 0)])
    corner = lax.ppermute(
        corner, ("role", "gx"), [((1 - r) * gx + i + 1, r * gx + i) for r in range(2) for i in range(gx - 1)]
    )
    design_a, design_b = beside(design, design)
    pack = pl.pallas_call(
        pack_kernel,
        out_shape=shape(gy, 18 * by + 24, fz),
        name="pack",
        compiler_params=KEEP,
    )(force, clamped_dof_mask, next_plane, strips, corner)
    table = pl.pallas_call(
        table_kernel,
        out_shape=shape(2 * ROWS, 2 * ROWS, dtype=BF16),
        name="table",
        compiler_params=KEEP,
    )(stiffness, jnp.asarray(place_table()))
    rf = lax.all_to_all(pack, "gy", 0, 0)

    role = lax.axis_index("role")

    def strip(x):
        return jnp.where(role == 0, x[..., fz - STRIP :], x[..., :STRIP]).reshape(-1, STRIP)

    fine_strips = jnp.concatenate([strip(design), strip(design_a), strip(design_b)], axis=0)
    fine_strips = lax.ppermute(fine_strips, "role", [(0, 1), (1, 0)])

    node_set = shape(3 * count, LANES)
    plane = shape(count // 2, LANES)
    element = shape(columns, LANES)
    tile_scratch = [
        pltpu.VMEM((3, tiles, 16, LANES), BF16),
        pltpu.VMEM((2, tiles, 16, LANES), BF16),
        pltpu.VMEM((2, count, LANES), F32),
    ]
    shift32 = pltpu.VMEM((2, count, LANES), F32)
    sw, factor, density = pl.pallas_call(
        filter_kernel,
        out_shape=(shape(planes + 4, fy, 2 * fz), element, element),
        scratch_shapes=[pltpu.VMEM((3 * planes, fy, 2 * fz), F32), pltpu.VMEM((fy, 2 * fz), F32)],
        name="filter",
        compiler_params=KEEP,
        cost_estimate=pl.CostEstimate(flops=30_000_000, transcendentals=0, bytes_accessed=4_000_000),
    )(design, design_a, design_b, fine_strips)
    v0, free, local, to_a, to_b, e00 = pl.pallas_call(
        first_kernel,
        out_shape=(node_set, node_set, node_set, plane, plane, element),
        scratch_shapes=tile_scratch,
        name="first",
        compiler_params=KEEP,
    )(rf, factor, table)
    from_a, from_b = beside(to_a, to_b)
    v1, local, to_a, to_b, e01, e11 = pl.pallas_call(
        second_kernel,
        out_shape=(node_set, node_set, plane, plane, element, element),
        scratch_shapes=tile_scratch + [shift32],
        name="second",
        compiler_params=KEEP,
    )(v0, free, local, from_a, from_b, factor, table)
    from_a, from_b = beside(to_a, to_b)
    v2, e02, e12, e22, moments = pl.pallas_call(
        third_kernel,
        out_shape=(node_set, element, element, element, shape(devices, LANES)),
        scratch_shapes=tile_scratch + [shift32, shift32],
        name="third",
        compiler_params=KEEP,
    )(v0, v1, free, local, from_a, from_b, factor, table, e00, e01, e11)
    moments = lax.all_to_all(moments, ("role", "gx", "gy"), 0, 0, tiled=True)
    grad, u = pl.pallas_call(
        combine_kernel,
        out_shape=(element, shape(gy, 3, 2, by, fz)),
        scratch_shapes=[pltpu.VMEM((2 * count, LANES), F32)],
        name="combine",
        compiler_params=KEEP,
    )(moments, v0, v1, v2, e00, e01, e11, e02, e12, e22, density)
    grad_a, grad_b = beside(grad, grad)
    sensitivity = pl.pallas_call(
        last_kernel,
        out_shape=shape(planes, fy, fz),
        scratch_shapes=[pltpu.VMEM((planes + 4, fy, 2 * fz), F32)],
        name="last",
        compiler_params=KEEP,
    )(grad, grad_a, grad_b, sw)
    u = lax.all_to_all(u, "gy", 0, 0)
    displacement = jnp.transpose(u, (1, 0, 2, 3, 4)).reshape(3, bx, by, fz)
    return sensitivity, displacement


def solution(mesh):
    placed = (
        P(("gx", "gy"), None, "role"),
        P(None, "gx", "gy", "role"),
        P(None, "gx", "gy", "role"),
        P(),
    )

    return jax.shard_map(
        on_device,
        mesh=mesh,
        in_specs=placed,
        out_specs=(P(("gx", "gy"), None, "role"), P(None, "gx", "gy", "role")),
        check_vma=False,
    )
```

```python
import jax
import jax.numpy as jnp
import numpy as np
from jax import lax
from jax.experimental import pallas as pl
from jax.experimental.pallas import tpu as pltpu
from jax.sharding import PartitionSpec as P


SHARPNESS = 4.0
THRESHOLD = 0.5
FLOOR_STIFF = 0.001
TANH2 = float(np.tanh(2.0))
LANES = 128
HALO = 3
STRIP = 8
ROWS = 120
LINE = ("gx", "gy")
KEEP = pltpu.CompilerParams(vmem_limit_bytes=12 << 20)
F32 = jnp.float32
BF16 = jnp.bfloat16


def iota(shape, dim):
    return lax.broadcasted_iota(jnp.int32, shape, dim)


def place_table():
    table = np.zeros((ROWS, 81), np.float32)
    for c in range(3):
        for b in range(3):
            for a in range(3):
                for q in range(3):
                    dof = ((c * 3 + b) * 3 + a) * 3 + q
                    if c < 2:
                        row = 8 * (3 * a + b) + 4 * c + q
                    else:
                        row = 72 + 8 * (2 * b + (a == 2)) + 4 * (a == 1) + q
                    table[row, dof] = 1.0
    return table


def split2(x):
    hi = x.astype(BF16)
    return hi, (x - hi.astype(F32)).astype(BF16)


def split3(x):
    hi = x.astype(BF16)
    rest = x - hi.astype(F32)
    mid = rest.astype(BF16)
    return hi, mid, (rest - mid.astype(F32)).astype(BF16)


def dot(a, b):
    return jnp.dot(a, b, preferred_element_type=F32)


def pick_right(x, table):
    hi, mid, lo = split3(x)
    return (dot(hi, table) + dot(mid, table)) + dot(lo, table)


def pick_left(table, x):
    hi, mid, lo = split3(x)
    return (dot(table, hi) + dot(table, mid)) + dot(table, lo)


def where_am_i():
    role = lax.axis_index("role")
    slab = lax.axis_index("gx") * lax.axis_size("gy") + lax.axis_index("gy")
    return role, slab


def element_lanes(shape, role, half):
    lane = iota(shape, len(shape) - 1)
    above = jnp.logical_and(lane >= half, lane < half + HALO)
    below = lane >= LANES - HALO
    roles = lax.axis_size("role")
    return (lane < half) | (above & (role < roles - 1)) | (below & (role > 0))


def hat_count(place, extent):
    low = jnp.where(place == 0, 3.0, jnp.where(place == 1, 1.0, 0.0))
    high = jnp.where(place == extent - 1, 3.0, jnp.where(place == extent - 2, 1.0, 0.0))
    return 9.0 - low - high


def smooth_z(x):
    width = x.shape[1]
    for _ in range(2):
        x = x + pltpu.roll(x, 1, 1) + pltpu.roll(x, width - 1, 1)
    return x


def smooth_y(x):
    rows = x.shape[0]
    x = jnp.concatenate([x, jnp.zeros((8, x.shape[1]), F32)], axis=0)
    for _ in range(2):
        x = x + pltpu.roll(x, 1, 0) + pltpu.roll(x, rows + 7, 0)
    return x[:rows]


def strip_rows_kernel(
    force_hbm, mask_hbm, own_ref, plane_ref, strip_ref, corner_ref, force_ref, mask_ref, sems
):
    copies = (
        pltpu.make_async_copy(force_hbm, force_ref, sems.at[0]),
        pltpu.make_async_copy(mask_hbm, mask_ref, sems.at[1]),
    )
    for copy in copies:
        copy.start()
    for copy in copies:
        copy.wait()
    _, bx, by, fz = force_ref.shape
    role, _ = where_am_i()
    first = jnp.where(role == 0, fz - STRIP, 0)
    take = jnp.where(iota((fz, LANES), 0) == first + (iota((fz, LANES), 1) & (STRIP - 1)), 1.0, 0.0).astype(BF16)
    own_y = (iota((bx, by, LANES), 2) // STRIP) == iota((bx, by, LANES), 1)
    corner_ref[...] = jnp.zeros(corner_ref.shape, F32)
    for q in range(3):
        free = 1.0 - mask_ref[q].astype(F32)
        rhs = free * force_ref[q]
        own_ref[q] = rhs
        own_ref[q + 3] = free
        plane_ref[q * by : (q + 1) * by] = rhs[0]
        plane_ref[(q + 3) * by : (q + 4) * by] = free[0]
        edge = pick_right(rhs.reshape(bx * by, fz), take), dot(free.reshape(bx * by, fz).astype(BF16), take)
        for row, x in ((q, edge[0]), (q + 3, edge[1])):
            x = jnp.sum(jnp.where(own_y, x.reshape(bx, by, LANES), 0.0), axis=1)
            strip_ref[row * bx : (row + 1) * bx] = x
            corner_ref[row : row + 1] = x[0:1]


def turned(k):
    gy = lax.axis_size("gy")
    j = lax.axis_index("gy")
    return jnp.where(j + k < gy, j + k, j + k - gy), jnp.where(j >= k, j - k, j - k + gy)


def pack_kernel(own_ref, plane_ref, strip_ref, corner_ref, *pack_refs):
    _, bx, by, _ = own_ref.shape
    tail = 18 * by
    for k, pack_ref in enumerate(pack_refs):
        dest, _ = turned(k)
        pack_ref[tail + 18 :] = jnp.zeros((pack_ref.shape[0] - tail - 18, LANES), F32)
        for a in range(3):
            x = 2 * dest + a
            inner = x < bx
            x = jnp.minimum(x, bx - 1)
            for row in range(6):
                at = row * 3 + a
                val = own_ref[row, x]
                edge = strip_ref[pl.ds(row * bx + x, 1), :]
                if a == 2:
                    val = jnp.where(inner, val, plane_ref[row * by : (row + 1) * by])
                    edge = jnp.where(inner, edge, corner_ref[row : row + 1])
                pack_ref[at * by : (at + 1) * by] = val
                pack_ref[tail + at : tail + at + 1] = edge


def table_kernel(stiff_ref, place_ref, table_ref):
    place = place_ref[...]
    half_way = jnp.dot(place, stiff_ref[...], precision=lax.Precision.HIGHEST, preferred_element_type=F32)
    spread = lax.dot_general(
        half_way, place, (((1,), (1,)), ((), ())), precision=lax.Precision.HIGHEST, preferred_element_type=F32
    )
    hi, lo = split2(spread)
    row = iota((ROWS, 2 * ROWS), 0)
    col = iota((ROWS, 2 * ROWS), 1)
    twice = jnp.where(row == 8 * (col // 16) + col % 8, 1.0, 0.0).astype(BF16)
    table_ref[:ROWS] = dot(hi, twice).astype(BF16)
    table_ref[ROWS:] = dot(lo, twice).astype(BF16)


def plane_rows(tiles):
    return tiles * 8


def shifted_tiles(nodes_ref, tiles, s):
    count = plane_rows(tiles)
    upper = (iota((count, LANES), 0) & 4) == 0
    if s == 0:
        first = nodes_ref[0:count]
        second = nodes_ref[count : 2 * count]
        x = jnp.where(upper, first, pltpu.roll(second, 4, 0))
    else:
        x = jnp.where(upper, nodes_ref[2 * count : 3 * count], 0.0)
    return pltpu.roll(x, LANES - 1, 1)


def pair_tiles(x):
    tiles = x.shape[0] // 8
    hi = x.astype(BF16).astype(F32)
    lo = x - hi
    both = jnp.concatenate([hi.reshape(tiles, 8, LANES), lo.reshape(tiles, 8, LANES)], axis=1)
    return both.astype(BF16)


def make_tiles(nodes_ref, main_ref, shift_ref, shift32_ref):
    tiles = main_ref.shape[1]
    count = plane_rows(tiles)
    for a in range(3):
        main_ref[a] = pair_tiles(nodes_ref[a * count : (a + 1) * count])
    for s in range(2):
        x = shifted_tiles(nodes_ref, tiles, s)
        if shift32_ref is not None:
            shift32_ref[s] = x
        shift_ref[s] = pair_tiles(x)


def sweep(table_ref, main_ref, shift_ref, factor_ref, out_ref, energies):
    tiles = main_ref.shape[1]
    columns = factor_ref.shape[0]
    upper = iota((8, LANES), 0) < 4

    def finish(node, parts):
        t0, t1, t2, s0, s1 = parts
        r0 = pltpu.roll(s0, 1, 1)
        r1 = pltpu.roll(s1, 1, 1)
        done = (
            t0 + jnp.where(upper, r0, 0.0),
            t1 + jnp.where(upper, pltpu.roll(r0, 4, 0), 0.0),
            t2 + jnp.where(upper, r1, 0.0),
        )
        for a in range(3):
            out_ref[pl.ds(pl.multiple_of((a * tiles + node) * 8, 8), 8), :] = done[a]

    def body(i, carry):
        cols = []
        for k in range(2):
            base = 4 * i + 2 * k
            pieces = [main_ref[a, base + b] for a in range(3) for b in range(3)]
            pieces += [shift_ref[s, base + b] for b in range(3) for s in range(2)]
            cols.append(jnp.concatenate(pieces, axis=0))
        product = dot(table_ref[...], jnp.concatenate(cols, axis=1))
        product = product[:ROWS] + product[ROWS:]
        parts = []
        for k in range(2):
            y = product[:, k * LANES : (k + 1) * LANES]
            base = 4 * i + 2 * k
            for nodes_ref, shift32_ref, e_ref in energies:
                total = None
                for a in range(3):
                    for b in range(3):
                        at = pl.multiple_of((a * tiles + base + b) * 8, 8)
                        term = nodes_ref[pl.ds(at, 8), :] * y[8 * (3 * a + b) : 8 * (3 * a + b) + 8]
                        total = term if total is None else total + term
                for b in range(3):
                    for s in range(2):
                        at = pl.multiple_of((base + b) * 8, 8)
                        lo = 72 + 8 * (2 * b + s)
                        total = total + shift32_ref[s, pl.ds(at, 8), :] * y[lo : lo + 8]
                e_ref[pl.ds(2 * i + k, 1), :] = jnp.sum(total, axis=0, keepdims=True)
            if out_ref is not None:
                z = y * factor_ref[pl.ds(2 * i + k, 1), :]
                parts.append(
                    [
                        [z[8 * (3 * a + b) : 8 * (3 * a + b) + 8] for a in range(3)]
                        + [z[72 + 8 * (2 * b + s) : 80 + 8 * (2 * b + s)] for s in range(2)]
                        for b in range(3)
                    ]
                )
        if out_ref is None:
            return carry
        left, right = parts
        finish(4 * i, [c + v for c, v in zip(carry, left[0])])
        finish(4 * i + 1, left[1])
        finish(4 * i + 2, [c + v for c, v in zip(left[2], right[0])])
        finish(4 * i + 3, right[1])
        return tuple(right[2])

    if out_ref is None:
        lax.fori_loop(0, columns // 2, lambda i, c: body(i, c), 0, unroll=min(16, columns // 2))
    else:
        zero = jnp.zeros((8, LANES), F32)
        lax.fori_loop(0, columns // 2, body, (zero,) * 5, unroll=min(16, columns // 2))
        for a in range(3):
            for node in range(2 * columns, tiles):
                at = (a * tiles + node) * 8
                out_ref[at : at + 8, :] = zero


def pack_pair(x, y):
    lane = iota((8, LANES), 1)
    row = iota((8, LANES), 0)
    half = LANES // 2
    even = jnp.where(row < 4, x, pltpu.roll(y, 4, 0))
    odd = jnp.where(row < 4, pltpu.roll(x, 4, 0), y)
    main = jnp.where(lane < half, even, pltpu.roll(odd, half, 1))
    edge = jnp.zeros((8, LANES), F32)
    for tile, first in ((x, 0), (y, 28)):
        moved = pltpu.roll(tile, half + first, 1, stride=4, stride_axis=0)
        at = lane - first - 4 * row
        edge = jnp.where(((at >= 0) & (at < 4)) | ((at >= 60) & (at < 64)), moved, edge)
    for shift in (4, 2, 1):
        edge = edge + pltpu.roll(edge, shift, 0)
    return jnp.where(row == 3, edge, main)


def unpack_pair(x):
    lane = iota((8, LANES), 1)
    row = iota((8, LANES), 0)
    half = LANES // 2
    own_even = (lane < half) & (row < 3)
    live = (row & 3) < 3
    own_odd = (lane < half) & (row >= 4) & live
    rim = live & ((lane // 4 == half // 4) | (lane // 4 == LANES // 4 - 1))
    swapped = pltpu.roll(x, half, 1)
    first = jnp.where(own_even, x, jnp.where(own_odd, pltpu.roll(swapped, 4, 0), 0.0))
    second = jnp.where(own_even, pltpu.roll(x, 4, 0), jnp.where(own_odd, swapped, 0.0))
    edge = jnp.broadcast_to(x[3:4], (8, LANES))
    out = []
    for tile, start in ((first, 0), (second, 28)):
        moved = jnp.take_along_axis(edge, (lane - half + start + 4 * row) & (LANES - 1), axis=1)
        out.append(jnp.where(rim, moved, tile))
    return out


def send_planes(local_ref, tiles, slab, to_a, to_b):
    count = plane_rows(tiles)
    half = count // 2
    even = slab % 2 == 0

    def body(i, _):
        at = pl.multiple_of(i * 8, 8)

        def tile(start):
            return local_ref[pl.ds(start + at, 8), :]

        low = pack_pair(tile(0), tile(half))
        high = pack_pair(tile(2 * count), tile(2 * count + half))
        to_a[pl.ds(at, 8), :] = jnp.where(even, high, low)
        to_b[pl.ds(at, 8), :] = jnp.where(even, low, high)
        return 0

    lax.fori_loop(0, tiles // 2, body, 0, unroll=min(33, tiles // 2))


def gather_nodes(local_ref, from_a, from_b, free_ref, tiles, slab, nodes_ref):
    count = plane_rows(tiles)
    half = count // 2
    even = slab % 2 == 0
    nodes_ref[count : 2 * count] = free_ref[count : 2 * count] * local_ref[count : 2 * count]

    def body(i, _):
        at = pl.multiple_of(i * 8, 8)
        a = from_a[pl.ds(at, 8), :]
        b = from_b[pl.ds(at, 8), :]
        for start, packed in ((0, jnp.where(even, b, a)), (2 * count, jnp.where(even, a, b))):
            for part, tile in enumerate(unpack_pair(packed)):
                where = pl.ds(start + part * half + at, 8)
                nodes_ref[where, :] = free_ref[where, :] * (local_ref[where, :] + tile)
        return 0

    lax.fori_loop(0, tiles // 2, body, 0, unroll=min(33, tiles // 2))


def filter_kernel(design_ref, da_ref, db_ref, strip_ref, sw_ref, factor_ref, density_ref, fine_ref, sum_ref):
    planes, fy, fz = design_ref.shape
    role, slab = where_am_i()
    slabs = lax.axis_size("gx") * lax.axis_size("gy")
    roles = lax.axis_size("role")
    half = fz // 2
    even = slab % 2 == 0

    at_lane = jnp.where(role == 0, 0, LANES - STRIP)
    put = jnp.where(iota((STRIP, LANES), 1) == iota((STRIP, LANES), 0) + at_lane, 1.0, 0.0).astype(BF16)
    for p in range(planes):
        a = da_ref[p]
        b = db_ref[p]
        fine_ref[p, :, :fz] = jnp.where(even, b, a)
        fine_ref[planes + p, :, :fz] = design_ref[p]
        fine_ref[2 * planes + p, :, :fz] = jnp.where(even, a, b)
    for p in range(planes):
        own = pick_right(strip_ref[p * fy : (p + 1) * fy], put)
        a = pick_right(strip_ref[(planes + p) * fy : (planes + p + 1) * fy], put)
        b = pick_right(strip_ref[(2 * planes + p) * fy : (2 * planes + p + 1) * fy], put)
        fine_ref[p, :, fz:] = jnp.where(even, b, a)
        fine_ref[planes + p, :, fz:] = own
        fine_ref[2 * planes + p, :, fz:] = jnp.where(even, a, b)

    width = 2 * fz
    lane = iota((1, width), 1)
    z_place = role * fz + jnp.where(lane < fz + fz // 2, lane, lane - width)
    inv_z = 1.0 / hat_count(z_place, roles * fz)
    inv_y = 1.0 / hat_count(iota((fy, 1), 0), fy)
    inv_yz = inv_y * inv_z
    sum_ref[...] = jnp.zeros((fy, width), F32)

    def filter_plane(p, _):
        x = fine_ref[p] + fine_ref[p + 4] + 2.0 * (fine_ref[p + 1] + fine_ref[p + 3]) + 3.0 * fine_ref[p + 2]
        x = smooth_y(smooth_z(x))
        place = jnp.full((1, 1), slab * planes + p - 2, jnp.int32)
        inv = inv_yz * (1.0 / hat_count(place, slabs * planes))
        bent = jnp.tanh(SHARPNESS * (x * inv - THRESHOLD))
        sw_ref[p] = (SHARPNESS / (2.0 * TANH2)) * (1.0 - bent * bent) * inv
        mine = jnp.logical_and(p >= 2, p < 2 + planes)
        sum_ref[...] += jnp.where(mine, (TANH2 + bent) * (1.0 / (2.0 * TANH2)), 0.0)
        return 0

    lax.fori_loop(0, planes + 4, filter_plane, 0, unroll=True)

    rows = factor_ref.shape[0]
    pool_y = jnp.where(iota((rows, fy), 1) // 4 == iota((rows, fy), 0), 1.0, 0.0).astype(BF16)
    pool_z = jnp.where(iota((width, LANES), 0) // 2 == iota((width, LANES), 1), 1.0, 0.0).astype(BF16)
    density = pick_right(pick_left(pool_y, sum_ref[...]), pool_z) * (1.0 / 32.0)
    inside = element_lanes((rows, LANES), role, half)
    density = jnp.where(inside, density, 0.0)
    density_ref[...] = density
    factor_ref[...] = jnp.where(inside, FLOOR_STIFF + (1.0 - FLOOR_STIFF) * density * density * density, 0.0)


def first_kernel(*refs):
    parts = len(refs) - 11
    rf_refs = refs[:parts]
    (factor_ref, table_ref, nodes_ref, free_ref, local_ref, to_a, to_b, e00_ref,
     main_ref, shift_ref, shift32_ref) = refs[parts:]
    tiles = main_ref.shape[1]
    count = plane_rows(tiles)
    role, slab = where_am_i()
    half = LANES // 2
    deep = (2 * factor_ref.shape[0]) // parts
    starts = [pl.multiple_of(turned(k)[1] * (deep * 8), 8) for k in range(parts)]
    tail = 18 * deep

    nodes_ref[...] = jnp.zeros(nodes_ref.shape, F32)
    free_ref[...] = jnp.zeros(free_ref.shape, F32)
    zi = iota((2 * LANES, 2 * LANES), 0)
    ci = iota((2 * LANES, 2 * LANES), 1)
    lane_of = ci & (LANES - 1)
    odd = ci // LANES
    first_lane = jnp.where(role == 0, half, LANES - STRIP // 2)
    own = zi == 2 * lane_of + odd
    edge = (zi & (STRIP - 1)) == 2 * (lane_of - first_lane) + odd
    table = jnp.where(zi < LANES, jnp.where(own, 1.0, 0.0), jnp.where(edge, 1.0, 0.0)).astype(BF16)
    own_y = (iota((deep, LANES), 1) // STRIP) == iota((deep, LANES), 0)
    for row in range(6):
        for a in range(3):
            at = row * 3 + a
            x = jnp.concatenate([rf_ref[at * deep : (at + 1) * deep] for rf_ref in rf_refs], axis=0)
            st = jnp.concatenate(
                [jnp.where(own_y, rf_ref[tail + at : tail + at + 1], 0.0) for rf_ref in rf_refs], axis=0
            )
            x = jnp.concatenate([x, st], axis=1)
            if row < 3:
                y = pick_right(x, table)
                dest = nodes_ref
            else:
                y = dot(x.astype(BF16), table)
                dest = free_ref
            q = row % 3
            for k in range(parts):
                part = y[k * deep : (k + 1) * deep]
                dest[pl.ds(a * count + q + starts[k], deep, stride=8), :] = part[:, :LANES]
                dest[pl.ds(a * count + 4 + q + starts[k], deep, stride=8), :] = part[:, LANES:]

    make_tiles(nodes_ref, main_ref, shift_ref, shift32_ref)
    sweep(table_ref, main_ref, shift_ref, factor_ref, local_ref, [(nodes_ref, shift32_ref, e00_ref)])
    send_planes(local_ref, tiles, slab, to_a, to_b)


def second_kernel(
    prev_ref, free_ref, last_ref, from_a, from_b, factor_ref, table_ref,
    nodes_ref, local_ref, to_a, to_b, e01_ref, e11_ref,
    main_ref, shift_ref, shift32_ref, prev32_ref,
):
    tiles = main_ref.shape[1]
    _, slab = where_am_i()
    gather_nodes(last_ref, from_a, from_b, free_ref, tiles, slab, nodes_ref)
    for s in range(2):
        prev32_ref[s] = shifted_tiles(prev_ref, tiles, s)
    make_tiles(nodes_ref, main_ref, shift_ref, shift32_ref)
    sweep(
        table_ref, main_ref, shift_ref, factor_ref, local_ref,
        [(prev_ref, prev32_ref, e01_ref), (nodes_ref, shift32_ref, e11_ref)],
    )
    send_planes(local_ref, tiles, slab, to_a, to_b)


def third_kernel(
    v0_ref, v1_ref, free_ref, last_ref, from_a, from_b, factor_ref, table_ref, e00_ref, e01_ref, e11_ref,
    nodes_ref, e02_ref, e12_ref, e22_ref, moment_ref,
    main_ref, shift_ref, shift32_ref, s0_ref, s1_ref,
):
    tiles = main_ref.shape[1]
    count = plane_rows(tiles)
    _, slab = where_am_i()
    gather_nodes(last_ref, from_a, from_b, free_ref, tiles, slab, nodes_ref)
    for s in range(2):
        s0_ref[s] = shifted_tiles(v0_ref, tiles, s)
        s1_ref[s] = shifted_tiles(v1_ref, tiles, s)
    make_tiles(nodes_ref, main_ref, shift_ref, shift32_ref)
    sweep(
        table_ref, main_ref, shift_ref, factor_ref, None,
        [(v0_ref, s0_ref, e02_ref), (v1_ref, s1_ref, e12_ref), (nodes_ref, shift32_ref, e22_ref)],
    )
    half = LANES // 2
    own = iota((1, LANES), 1) < half
    v0 = v0_ref[0 : 2 * count]
    sums = [jnp.sum(v0 * v0, axis=0, keepdims=True)]
    for e_ref in (e00_ref, e01_ref, e11_ref, e12_ref, e22_ref):
        sums.append(jnp.sum(factor_ref[...] * e_ref[...], axis=0, keepdims=True))
    lane = iota((1, LANES), 1)
    out = jnp.zeros((1, LANES), F32)
    for k, s in enumerate(sums):
        total = jnp.sum(jnp.where(own, s, 0.0), axis=1, keepdims=True)
        out = jnp.where(lane == k, total, out)
    moment_ref[...] = jnp.broadcast_to(out, moment_ref.shape)


def combine_kernel(
    moment_ref, v0_ref, v1_ref, v2_ref, e00_ref, e01_ref, e11_ref, e02_ref, e12_ref, e22_ref, density_ref,
    grad_ref, *rest,
):
    *u_refs, nodes_ref, u_ref = rest
    role, _ = where_am_i()
    parts = len(u_refs)
    _, _, deep, fz = u_refs[0].shape
    half = fz // 2
    count = v0_ref.shape[0] // 3
    total = jnp.sum(moment_ref[...], axis=0, keepdims=True)
    lane = iota((1, LANES), 1)
    m = [jnp.sum(jnp.where(lane == k, total, 0.0), axis=1, keepdims=True) for k in range(6)]
    s = m[1] / m[0]
    inv = 1.0 / s
    mu = [jnp.ones_like(s)]
    power = 1.0 / m[0]
    for k in range(1, 6):
        power = power * inv
        mu.append(m[k] * power)
    nu = list(mu)
    for depth in range(1, 6):
        for k in range(5, depth - 1, -1):
            nu[k] = nu[k] - nu[k - 1]
    g = [nu[k] + nu[k + 1] for k in range(5)]
    l10 = g[1] / g[0]
    l20 = g[2] / g[0]
    d1 = g[2] - l10 * g[1]
    x12 = g[3] - l10 * g[2]
    r1 = nu[1] - l10 * nu[0]
    r2 = nu[2] - l20 * nu[0]
    l21 = x12 / d1
    d2 = (g[4] - l20 * g[2]) - l21 * x12
    c2 = (r2 - l21 * r1) / d2
    c1 = (r1 - x12 * c2) / d1
    c0 = (nu[0] - g[1] * c1 - g[2] * c2) / g[0]
    w0 = (c0 - c1 + c2) * inv
    w1 = (c1 - 2.0 * c2) * inv * inv
    w2 = c2 * inv * inv * inv
    energy = (
        w0 * (w0 * e00_ref[...] + 2.0 * (w1 * e01_ref[...] + w2 * e02_ref[...]))
        + w1 * (w1 * e11_ref[...] + 2.0 * w2 * e12_ref[...])
        + w2 * w2 * e22_ref[...]
    )
    density = density_ref[...]
    grad = (-3.0 * (1.0 - FLOOR_STIFF) / 32.0) * density * density * energy
    grad_ref[...] = jnp.where(element_lanes(grad.shape, role, half), grad, 0.0)
    nodes_ref[...] = w0 * v0_ref[0 : 2 * count] + w1 * v1_ref[0 : 2 * count] + w2 * v2_ref[0 : 2 * count]
    gi = iota((LANES, fz), 0)
    zi = iota((LANES, fz), 1)
    even_table = jnp.where(zi == 2 * gi, 1.0, 0.0).astype(BF16)
    odd_table = jnp.where(zi == 2 * gi + 1, 1.0, 0.0).astype(BF16)
    for a in range(2):
        for q in range(3):
            even = nodes_ref[pl.ds(a * count + q, parts * deep, stride=8), :]
            odd = nodes_ref[pl.ds(a * count + 4 + q, parts * deep, stride=8), :]
            x = pick_right(even, even_table) + pick_right(odd, odd_table)
            u_ref[q, a] = x
    for k in range(parts):
        at = pl.multiple_of(turned(k)[0] * deep, 8)
        for q in range(3):
            for a in range(2):
                u_refs[k][q, a] = u_ref[q, a, pl.ds(at, deep), :]


def place_kernel(*refs):
    *u_refs, out_ref = refs
    for k, u_ref in enumerate(u_refs):
        source = turned(k)[1]
        for q in range(3):
            for a in range(2):
                out_ref[q, 2 * source + a] = u_ref[q, a]


def last_kernel(grad_ref, ga_ref, gb_ref, sw_ref, out_ref, work_ref):
    planes, fy, fz = out_ref.shape
    width = 2 * fz
    _, slab = where_am_i()
    even = slab % 2 == 0
    rows = grad_ref.shape[0]
    pool_y = jnp.where(iota((fy, rows), 0) // 4 == iota((fy, rows), 1), 1.0, 0.0).astype(BF16)
    pool_z = jnp.where(iota((LANES, width), 1) // 2 == iota((LANES, width), 0), 1.0, 0.0).astype(BF16)
    a = ga_ref[...]
    b = gb_ref[...]
    low = jnp.where(even, b, a)
    high = jnp.where(even, a, b)
    for grad, first, last in ((low, 0, 2), (grad_ref[...], 2, 2 + planes), (high, 2 + planes, 4 + planes)):
        wide = pick_right(pick_left(pool_y, grad), pool_z)
        for p in range(first, last):
            work_ref[p] = wide * sw_ref[p]

    def body(p, _):
        x = work_ref[p] + work_ref[p + 4] + 2.0 * (work_ref[p + 1] + work_ref[p + 3]) + 3.0 * work_ref[p + 2]
        out_ref[p] = smooth_y(smooth_z(x)[:, :fz])
        return 0

    lax.fori_loop(0, planes, body, 0, unroll=True)


def shape(*dims, dtype=F32):
    return jax.ShapeDtypeStruct(dims, dtype)


def on_device(design, force, clamped_dof_mask, stiffness):
    planes, fy, fz = design.shape
    _, bx, by, _ = force.shape
    gx = lax.axis_size("gx")
    gy = lax.axis_size("gy")
    roles = lax.axis_size("role")
    devices = gx * gy * roles
    slabs = gx * gy
    assert roles == 2 and planes == 4 and fz == LANES and bx == 2 * gy and slabs % 2 == 0
    columns = fy // 4
    nodes = fy // 2
    tiles = nodes + 2
    count = tiles * 8
    pairs_a = [(i, i ^ 1) for i in range(slabs)]
    pairs_b = [(i, i + 1 if i % 2 else i - 1) for i in range(1, slabs - 1)]

    def beside(to_a, to_b):
        b = lax.ppermute(to_b, LINE, pairs_b)
        a = lax.ppermute(to_a, LINE, pairs_a)
        return a, b

    own, plane0, strips, corner = pl.pallas_call(
        strip_rows_kernel,
        out_shape=(shape(6, bx, by, fz), shape(6 * by, fz), shape(6 * bx, LANES), shape(8, LANES)),
        in_specs=[pl.BlockSpec(memory_space=pltpu.HBM)] * 2,
        scratch_shapes=[
            pltpu.VMEM(force.shape, F32), pltpu.VMEM(force.shape, jnp.int32), pltpu.SemaphoreType.DMA((2,)),
        ],
        name="rows",
        compiler_params=KEEP,
    )(pltpu.with_memory_space_constraint(force, pltpu.HBM), pltpu.with_memory_space_constraint(clamped_dof_mask, pltpu.HBM))
    plane0, strips, corner, design = lax.optimization_barrier((plane0, strips, corner, design))
    next_plane = lax.ppermute(plane0, "gx", [(i + 1, i) for i in range(gx - 1)])
    strips = lax.ppermute(strips, "role", [(0, 1), (1, 0)])
    corner = lax.ppermute(
        corner, ("role", "gx"), [((1 - r) * gx + i + 1, r * gx + i) for r in range(2) for i in range(gx - 1)]
    )
    design_a, design_b = beside(design, design)
    pack = pl.pallas_call(
        pack_kernel,
        out_shape=(shape(18 * by + 24, fz),) * gy,
        name="pack",
        compiler_params=KEEP,
    )(own, next_plane, strips, corner)
    table = pl.pallas_call(
        table_kernel,
        out_shape=shape(2 * ROWS, 2 * ROWS, dtype=BF16),
        name="table",
        compiler_params=KEEP,
    )(stiffness, jnp.asarray(place_table()))
    rf = [pack[0]]
    for k in range(1, gy):
        rf.append(lax.ppermute(pack[k], "gy", [(j, (j + k) % gy) for j in range(gy)]))

    role = lax.axis_index("role")

    def strip(x):
        return jnp.where(role == 0, x[..., fz - STRIP :], x[..., :STRIP]).reshape(-1, STRIP)

    fine_strips = jnp.concatenate([strip(design), strip(design_a), strip(design_b)], axis=0)
    fine_strips = lax.ppermute(fine_strips, "role", [(0, 1), (1, 0)])

    node_set = shape(3 * count, LANES)
    plane = shape(count // 2, LANES)
    element = shape(columns, LANES)
    tile_scratch = [
        pltpu.VMEM((3, tiles, 16, LANES), BF16),
        pltpu.VMEM((2, tiles, 16, LANES), BF16),
        pltpu.VMEM((2, count, LANES), F32),
    ]
    shift32 = pltpu.VMEM((2, count, LANES), F32)
    sw, factor, density = pl.pallas_call(
        filter_kernel,
        out_shape=(shape(planes + 4, fy, 2 * fz), element, element),
        scratch_shapes=[pltpu.VMEM((3 * planes, fy, 2 * fz), F32), pltpu.VMEM((fy, 2 * fz), F32)],
        name="filter",
        compiler_params=KEEP,
        cost_estimate=pl.CostEstimate(flops=30_000_000, transcendentals=0, bytes_accessed=4_000_000),
    )(design, design_a, design_b, fine_strips)
    v0, free, local, to_a, to_b, e00 = pl.pallas_call(
        first_kernel,
        out_shape=(node_set, node_set, node_set, plane, plane, element),
        scratch_shapes=tile_scratch,
        name="first",
        compiler_params=KEEP,
    )(*rf, factor, table)
    from_a, from_b = beside(to_a, to_b)
    v1, local, to_a, to_b, e01, e11 = pl.pallas_call(
        second_kernel,
        out_shape=(node_set, node_set, plane, plane, element, element),
        scratch_shapes=tile_scratch + [shift32],
        name="second",
        compiler_params=KEEP,
    )(v0, free, local, from_a, from_b, factor, table)
    from_a, from_b = beside(to_a, to_b)
    v2, e02, e12, e22, moments = pl.pallas_call(
        third_kernel,
        out_shape=(node_set, element, element, element, shape(devices, LANES)),
        scratch_shapes=tile_scratch + [shift32, shift32],
        name="third",
        compiler_params=KEEP,
    )(v0, v1, free, local, from_a, from_b, factor, table, e00, e01, e11)
    moments = lax.all_to_all(moments, ("role", "gx", "gy"), 0, 0, tiled=True)
    grad, *u = pl.pallas_call(
        combine_kernel,
        out_shape=(element,) + (shape(3, 2, by, fz),) * gy,
        scratch_shapes=[pltpu.VMEM((2 * count, LANES), F32), pltpu.VMEM((3, 2, nodes, LANES), F32)],
        name="combine",
        compiler_params=KEEP,
    )(moments, v0, v1, v2, e00, e01, e11, e02, e12, e22, density)
    grad_a, grad_b = beside(grad, grad)
    sensitivity = pl.pallas_call(
        last_kernel,
        out_shape=shape(planes, fy, fz),
        scratch_shapes=[pltpu.VMEM((planes + 4, fy, 2 * fz), F32)],
        name="last",
        compiler_params=KEEP,
    )(grad, grad_a, grad_b, sw)
    for k in range(1, gy):
        u[k] = lax.ppermute(u[k], "gy", [(j, (j + k) % gy) for j in range(gy)])
    displacement = pl.pallas_call(
        place_kernel,
        out_shape=shape(3, bx, by, fz),
        name="place",
        compiler_params=KEEP,
    )(*u)
    return sensitivity, displacement


def solution(mesh):
    placed = (
        P(("gx", "gy"), None, "role"),
        P(None, "gx", "gy", "role"),
        P(None, "gx", "gy", "role"),
        P(),
    )

    return jax.shard_map(
        on_device,
        mesh=mesh,
        in_specs=placed,
        out_specs=(P(("gx", "gy"), None, "role"), P(None, "gx", "gy", "role")),
        check_vma=False,
    )
```
